16 devices in a mesh: dp: 4 (over z, y), tp: 4 (over x, core).
Axes of the slice: x: 2, y: 2, z: 2, core: 2. Of those that a mesh axis runs over, the one named last changes fastest.
Arguments:
- hidden: bfloat16 [8, 1024, 2048], P('dp', 'tp'), parts along dimension 0
- positions: int32 [8, 1024], P('dp'), parts along dimension 0
- norm_w: float32 [2048], replicated
- w_query: bfloat16 [2048, 2048], P(None, 'tp')
- w_key: bfloat16 [2048, 128], replicated
- w_value: bfloat16 [2048, 128], replicated
- w_out: bfloat16 [2048, 2048], P('tp')
- grad_out: bfloat16 [8, 1024, 2048], P('dp', 'tp'), parts along dimension 0
Outputs:
- output 1: bfloat16 [8, 1024, 2048], P('dp', 'tp'), parts along dimension 0
- output 2: bfloat16 [8, 1024, 2048], P('dp', 'tp'), parts along dimension 0
- output 3: float32 [8192, 2048], P('dp', 'tp'), parts along dimension 0
- output 4: float32 [8192, 2048], P(('dp', 'tp')), parts along dimension 0
- output 5: float32 [8192, 128], P('dp'), parts along dimension 0
- output 6: float32 [8192, 128], P('dp'), parts along dimension 0
- output 7: float32 [8192], P('dp'), parts along dimension 0
There are 4 independent parts. The reference program is written for one: setup_inputs(seed, part) draws one part's arguments, and reference() takes and returns one part's arrays. A program takes and returns all parts, laid end to end along the dimension named above; an argument that names none is the same for every part.
All inputs are finite; a program needn't handle non-finite values.
Results may differ from the reference program's by a relative error of at most 0.02.
Values are sent between devices in bfloat16 or wider.
A program may use at most 1 GiB of HBM per device.

```python
import jax
import jax.numpy as jnp
from jax import lax

BATCH = 2
SEQ = 1024
D_MODEL = 2048
HEADS = 16
HEAD = 128


def setup_inputs(seed: int = 0, part: int = 0) -> dict:
    part_key = jax.random.fold_in(jax.random.key(seed), part)
    part_keys = jax.random.split(part_key, 4)
    shared_keys = jax.random.split(jax.random.key(seed + 1), 5)
    width = HEADS * HEAD
    hidden = jax.random.normal(part_keys[0], (BATCH, SEQ, D_MODEL), jnp.float32)
    increments = jax.random.randint(part_keys[1], (BATCH, SEQ), 1, 4, dtype=jnp.int32)
    starts = jax.random.randint(part_keys[2], (BATCH, 1), 0, 64, dtype=jnp.int32)
    positions = jnp.cumsum(increments, axis=1) - increments[:, :1] + starts
    grad_out = jax.random.normal(part_keys[3], (BATCH, SEQ, D_MODEL), jnp.float32)
    norm_w = 0.5 * jax.random.normal(shared_keys[0], (D_MODEL,), jnp.float32)
    w_query = jax.random.normal(shared_keys[1], (D_MODEL, width), jnp.float32) * D_MODEL ** -0.5
    w_key = jax.random.normal(shared_keys[2], (D_MODEL, HEAD), jnp.float32) * D_MODEL ** -0.5
    w_value = jax.random.normal(shared_keys[3], (D_MODEL, HEAD), jnp.float32) * D_MODEL ** -0.5
    out_gain = (SEQ ** 0.5) / 8.0 * width ** -0.5
    w_out = jax.random.normal(shared_keys[4], (width, D_MODEL), jnp.float32) * out_gain
    return {'hidden': hidden.astype(jnp.bfloat16), 'positions': positions.astype(jnp.int32), 'norm_w': norm_w, 'w_query': w_query.astype(jnp.bfloat16), 'w_key': w_key.astype(jnp.bfloat16), 'w_value': w_value.astype(jnp.bfloat16), 'w_out': w_out.astype(jnp.bfloat16), 'grad_out': grad_out.astype(jnp.bfloat16)}


def rope_tables(positions):
    half = HEAD // 2
    inv_freq = 10000.0 ** (-2.0 * jnp.arange(half, dtype=jnp.float32) / HEAD)
    angle = positions.astype(jnp.float32)[..., None] * inv_freq
    return jnp.cos(angle), jnp.sin(angle)


def apply_rope(vector, cos_t, sin_t):
    half = HEAD // 2
    first = vector[..., :half]
    second = vector[..., half:]
    return jnp.concatenate([first * cos_t - second * sin_t, second * cos_t + first * sin_t], axis=-1)


def block_forward(hidden, positions, norm_w, w_query, w_key, w_value, w_out):
    hidden_f = hidden.astype(jnp.float32)
    inv_rms = lax.rsqrt(jnp.mean(hidden_f * hidden_f, axis=-1, keepdims=True) + 1e-6)
    normed_act = (hidden_f * inv_rms * (1.0 + norm_w)).astype(jnp.bfloat16)
    tokens = normed_act.reshape(BATCH * SEQ, D_MODEL)
    query = jnp.dot(tokens, w_query, preferred_element_type=jnp.float32).astype(jnp.bfloat16).reshape(BATCH, SEQ, HEADS, HEAD)
    key_proj = jnp.dot(tokens, w_key, preferred_element_type=jnp.float32).astype(jnp.bfloat16).reshape(BATCH, SEQ, HEAD)
    value_proj = jnp.dot(tokens, w_value, preferred_element_type=jnp.float32).astype(jnp.bfloat16).reshape(BATCH, SEQ, HEAD)
    cos_t, sin_t = rope_tables(positions)
    q_rot = (apply_rope(query.astype(jnp.float32), cos_t[:, :, None], sin_t[:, :, None]) * HEAD ** -0.5).astype(jnp.bfloat16)
    k_rot = apply_rope(key_proj.astype(jnp.float32), cos_t, sin_t).astype(jnp.bfloat16)
    scores = jnp.einsum('bqhd,bkd->bhqk', q_rot.astype(jnp.float32), k_rot.astype(jnp.float32))
    causal = jnp.arange(SEQ)[:, None] >= jnp.arange(SEQ)[None, :]
    attn_probs = jax.nn.softmax(jnp.where(causal, scores, -1e30), axis=-1)
    attended = jnp.einsum('bhqk,bkd->bqhd', attn_probs.astype(jnp.bfloat16).astype(jnp.float32), value_proj.astype(jnp.float32)).astype(jnp.bfloat16)
    projected = jnp.dot(attended.reshape(BATCH * SEQ, HEADS * HEAD), w_out, preferred_element_type=jnp.float32).reshape(BATCH, SEQ, D_MODEL)
    return (hidden_f + projected).astype(jnp.bfloat16)


def reference(hidden, positions, norm_w, w_query, w_key, w_value, w_out, grad_out):
    def bound_forward(hidden_in, norm_in, query_in, key_in, value_in, out_in):
        return block_forward(hidden_in, positions, norm_in, query_in, key_in, value_in, out_in)
    output, pullback = jax.vjp(bound_forward, hidden, norm_w, w_query, w_key, w_value, w_out)
    grad_hidden, grad_norm_w, grad_w_query, grad_w_key, grad_w_value, grad_w_out = pullback(grad_out)
    return (output, grad_hidden.astype(jnp.bfloat16), grad_w_query.astype(jnp.float32), grad_w_out.astype(jnp.float32), grad_w_key.astype(jnp.float32), grad_w_value.astype(jnp.float32), grad_norm_w.astype(jnp.float32))
```

```python
import jax
import jax.numpy as jnp
from jax import lax
from jax.experimental import pallas as pl
from jax.experimental.pallas import tpu as pltpu
from jax.sharding import PartitionSpec as P

F32 = jnp.float32
BF16 = jnp.bfloat16
MESH = pl.DeviceIdType.MESH

TB = 256
NB = 2
TOK = TB * NB
SEQ = 1024
D = 2048
HD = 128
HL = 4
HW = HD * HL
SCALE = HD ** -0.5

W_SIB, W_X, W_Y, W_Z, W_YZ = 0, 1, 2, 3, 4
W_REL = 5
KV_SIB, KV_X, KV_REL = 9, 10, 11
BULK_X = 12
BULK_SIB = 16
BULK_REL = 20
RS_SIB, RS_SIB2, RS_X = 24, 25, 26
DKV_SIB, DKV_X, DKV_REL = 27, 28, 29
DW_SIB, DW_X, DW_XS = 30, 31, 32
OQ_SIB = 33
N_SEM = 34


def dot_nn(a, b):
    return jnp.dot(a, b, preferred_element_type=F32)


def dot_nt(a, b):
    return lax.dot_general(a, b, (((1,), (1,)), ((), ())), preferred_element_type=F32)


def dot_tn(a, b):
    return lax.dot_general(a, b, (((0,), (0,)), ((), ())), preferred_element_type=F32)


def rope(u, cos_t, sin_t):
    return u * cos_t + pltpu.roll(u, HD // 2, 1) * sin_t


def rope_back(u, cos_t, sin_t):
    return u * cos_t - pltpu.roll(u, HD // 2, 1) * sin_t


def attend(n, q, do, k_ref, b, kt_ref):
    keys = n * TB
    k = k_ref[b, 0:keys, 0:HD]
    v = k_ref[b, 0:keys, HD:2 * HD]
    s = dot_nt(k, q)
    row = lax.broadcasted_iota(jnp.int32, (TB, TB), 0)
    col = lax.broadcasted_iota(jnp.int32, (TB, TB), 1)
    last = jnp.where(row <= col, s[keys - TB:], -1e30)
    s = last if n == 1 else jnp.concatenate([s[:keys - TB], last], axis=0)
    e = jnp.exp(s - jnp.max(s, axis=0, keepdims=True))
    p = e * (1.0 / jnp.sum(e, axis=0, keepdims=True))
    p_low = p.astype(BF16)
    dp = dot_nt(v, do)
    ds = (p * (dp - jnp.sum(p * dp, axis=0, keepdims=True))).astype(BF16)
    o = dot_nn(kt_ref[b, HD:2 * HD, 0:keys], p_low).T
    dq = dot_nn(kt_ref[b, 0:HD, 0:keys], ds).T
    return o, dq, p_low, ds


def transpose_kv(kv_ref, kt_ref):
    for b in range(NB):
        for j in range(4):
            kt_ref[b, :, j * TB:(j + 1) * TB] = kv_ref[b, j * TB:(j + 1) * TB, :].astype(F32).T.astype(BF16)


def main_kernel(x_ref, act_ref, dout_ref, w_own, wkv_ref, gain_ref, cos_ref, sin_ref,
                out_ref, dx_ref, dw_ref, w_all, act_all, dout_all, kv_ref, dkv_ref, oq_ref,
                wbuf, q_s, do_s, o_s, dq_s, out_acc, da_acc, kt_ref, dkv_acc, rs_a, rs_b, rs_c, dw_parts,
                send, recv, lsem):
    dp = lax.axis_index('dp')
    tp = lax.axis_index('tp')
    sib = (dp, tp ^ 1)
    xp = (dp, tp ^ 2)
    xs = (dp, tp ^ 3)
    yp = (dp ^ 1, tp)
    zp = (dp ^ 2, tp)
    yzp = (dp ^ 3, tp)

    def rc(i, src, dst, dev):
        return pltpu.make_async_remote_copy(src_ref=src, dst_ref=dst, send_sem=send.at[i], recv_sem=recv.at[i],
                                            device_id=dev, device_id_type=MESH)

    def quarter(j):
        return pl.ds(pl.multiple_of((dp ^ j) * 128, 128), 128)

    def rows(blk):
        return pl.ds(pl.multiple_of(blk * TB, TB), TB)

    barrier = pltpu.get_barrier_semaphore()
    for dev in (sib, xp, xs, yp, zp, yzp):
        pl.semaphore_signal(barrier, inc=1, device_id=dev, device_id_type=MESH)
    pl.semaphore_wait(barrier, 6)

    copies = {}

    def start(i, src, dst, dev):
        copies[i] = rc(i, src, dst, dev)
        copies[i].start()

    start(W_X, w_own.at[:, quarter(0), :], w_all.at[2, :, quarter(0), :], xp)
    start(W_SIB, w_own, w_all.at[1], sib)
    start(BULK_SIB, dout_ref, dout_all.at[1], sib)
    start(BULK_SIB + 1, act_ref, act_all.at[1], sib)
    own_a = pltpu.make_async_copy(act_ref, act_all.at[0], lsem.at[1])
    own_a.start()
    own_d = pltpu.make_async_copy(dout_ref, dout_all.at[0], lsem.at[2])
    own_d.start()

    kv = dot_nn(act_ref[...], wkv_ref[...])
    k_rot = rope(kv[:, 0:HD].astype(BF16).astype(F32), cos_ref[...], sin_ref[...]).astype(BF16)
    v_own = kv[:, HD:2 * HD].astype(BF16)
    for b in range(NB):
        kv_ref[b, rows(tp), 0:HD] = k_rot[b * TB:(b + 1) * TB]
        kv_ref[b, rows(tp), HD:2 * HD] = v_own[b * TB:(b + 1) * TB]
    start(KV_X, kv_ref.at[:, rows(tp), :], kv_ref.at[:, rows(tp), :], xp)
    start(KV_SIB, kv_ref.at[:, rows(tp), :], kv_ref.at[:, rows(tp), :], sib)

    out_acc[...] = jnp.zeros_like(out_acc)
    da_acc[...] = jnp.zeros_like(da_acc)
    dkv_acc[...] = jnp.zeros_like(dkv_acc)

    def project():
        def pair(j, carry):
            cols = pl.ds(pl.multiple_of(j * 2 * HD, 2 * HD), 2 * HD)
            q = dot_nt(act_ref[...], wbuf[0, cols, :]).astype(BF16).astype(F32)
            for h in range(2):
                piece = rope(q[:, h * HD:(h + 1) * HD], cos_ref[...], sin_ref[...]) * SCALE
                q_s[:, pl.ds(pl.multiple_of((2 * j + h) * HD, HD), HD)] = piece.astype(BF16)
            do_s[:, cols] = dot_nt(dout_ref[...], wbuf[1, cols, :]).astype(BF16)
            return carry
        lax.fori_loop(0, HL // 2, pair, 0)

    def attend_group():
        for n in range(1, 5):
            @pl.when(tp == n - 1)
            def _():
                def step(t, carry):
                    b = t // 2
                    r = pl.ds(pl.multiple_of(b * TB, TB), TB)
                    cos_t = cos_ref[r, :]
                    sin_t = sin_ref[r, :]
                    for j in range(2):
                        c = pl.ds(pl.multiple_of(((t % 2) * 2 + j) * HD, HD), HD)
                        q = q_s[r, c]
                        do = do_s[r, c]
                        o, dq, p_low, ds = attend(n, q, do, kv_ref, b, kt_ref)
                        o_s[r, c] = o.astype(BF16)
                        dq_s[r, c] = rope_back(dq * SCALE, cos_t, sin_t).astype(BF16)
                        dkv_acc[b, 0:n * TB, 0:HD] += dot_nn(ds, q)
                        dkv_acc[b, 0:n * TB, HD:2 * HD] += dot_nn(p_low, do)
                    return carry
                lax.fori_loop(0, 4, step, 0)

    def accumulate():
        def tile(j, carry):
            cols = pl.ds(pl.multiple_of(j * 512, 512), 512)
            out_acc[:, cols] += dot_nn(o_s[...], wbuf[1, :, cols])
            da_acc[:, cols] += dot_nn(dq_s[...], wbuf[0, :, cols])
            return carry
        lax.fori_loop(0, 4, tile, 0)

    def load_w(src):
        cp = pltpu.make_async_copy(src, wbuf, lsem.at[0])
        cp.start()
        cp.wait()

    def exchange_kv():
        copies[KV_X].wait_recv()
        start(KV_REL, kv_ref.at[:, rows(tp ^ 2), :], kv_ref.at[:, rows(tp ^ 2), :], sib)
        copies[KV_SIB].wait_recv()
        copies[KV_REL].wait_recv()
        transpose_kv(kv_ref, kt_ref)

    def spread_w():
        copies[W_X].wait_recv()
        mine = w_all.at[2, :, quarter(0), :]
        start(W_Y, mine, mine, yp)
        start(W_Z, mine, mine, zp)
        start(W_YZ, mine, mine, yzp)
        start(W_REL, mine, w_all.at[3, :, quarter(0), :], sib)
        for b in range(NB):
            r = pl.ds(b * TB, TB)
            start(BULK_X + 2 * b, dout_ref.at[r, :], dout_all.at[2, r, :], xp)
            start(BULK_X + 2 * b + 1, act_ref.at[r, :], act_all.at[2, r, :], xp)

    load_w(w_own)
    project()
    spread_w()
    exchange_kv()

    def group(i, carry):
        @pl.when(i == 1)
        def _():
            rc(W_SIB, w_own, w_all.at[1], sib).wait_recv()

        @pl.when(i == 2)
        def _():
            for j, w in ((1, W_Y), (2, W_Z), (3, W_YZ)):
                piece = w_all.at[2, :, quarter(j), :]
                rc(w, piece, piece, sib).wait_recv()
                rc(W_REL + j, piece, w_all.at[3, :, quarter(j), :], sib).start()

        @pl.when(i == 3)
        def _():
            for j in range(4):
                rc(W_REL + j, w_all.at[2, :, quarter(j), :], w_all.at[3, :, quarter(j), :], sib).wait_recv()

        @pl.when(i > 0)
        def _():
            load_w(w_all.at[i])
            project()

        attend_group()
        accumulate()

        @pl.when(i == 0)
        def _():
            oq_ref[0, 0] = o_s[...]
            oq_ref[0, 1] = dq_s[...]

        @pl.when(i == 1)
        def _():
            rs_c[0] = o_s[...]
            rs_c[1] = dq_s[...]
        return carry

    lax.fori_loop(0, 4, group, 0)
    start(OQ_SIB, rs_c, oq_ref.at[1], sib)

    start(RS_SIB, dkv_acc.at[:, rows(tp ^ 1), :], rs_a.at[0], sib)
    start(RS_SIB2, dkv_acc.at[:, rows(tp ^ 3), :], rs_a.at[1], sib)
    for r in range(8):
        cols = slice(r * 256, (r + 1) * 256)
        out_ref[:, cols] = (x_ref[:, cols].astype(F32) + out_acc[:, cols]).astype(BF16)
    copies[RS_SIB].wait_recv()
    copies[RS_SIB2].wait_recv()
    rs_b[0] = dkv_acc[:, rows(tp ^ 2), :] + rs_a[1]
    start(RS_X, rs_b.at[0], rs_b.at[1], xp)

    for c in range(4):
        copies[BULK_X + c].wait_recv()
        r = pl.ds((c // 2) * TB, TB)
        whole = act_all if c % 2 else dout_all
        start(BULK_REL + c, whole.at[2, r, :], whole.at[3, r, :], sib)

    copies[RS_X].wait_recv()
    total = dkv_acc[:, rows(tp), :] + rs_a[0] + rs_b[1]
    for b in range(NB):
        r = slice(b * TB, (b + 1) * TB)
        dkv_ref[b, rows(tp), 0:HD] = rope_back(total[b, :, 0:HD], cos_ref[r], sin_ref[r]).astype(BF16)
        dkv_ref[b, rows(tp), HD:2 * HD] = total[b, :, HD:2 * HD].astype(BF16)
    start(DKV_X, dkv_ref.at[:, rows(tp), :], dkv_ref.at[:, rows(tp), :], xp)
    start(DKV_SIB, dkv_ref.at[:, rows(tp), :], dkv_ref.at[:, rows(tp), :], sib)

    dw_parts[0] = jnp.zeros((8, D), F32)

    def dx_rows(j, carry):
        b = j // 2
        r = pl.ds(pl.multiple_of(j * 128, 128), 128)
        d_own = dkv_ref[b, pl.ds(pl.multiple_of(tp * TB + (j % 2) * 128, 128), 128), :]
        da = da_acc[r, :] + dot_nt(d_own, wkv_ref[...])
        xf = x_ref[r, :].astype(F32)
        inv = lax.rsqrt(jnp.mean(xf * xf, axis=-1, keepdims=True) + 1e-6)
        normed = xf * inv
        prod = da * normed
        dw_parts[0] += jnp.sum(prod.reshape(16, 8, D), axis=0)
        gain = gain_ref[...]
        corr = jnp.mean(prod * gain, axis=-1, keepdims=True)
        dx_ref[r, :] = (dout_ref[r, :].astype(F32) + inv * (da * gain - normed * corr)).astype(BF16)
        return carry

    lax.fori_loop(0, 4, dx_rows, 0)
    start(DW_SIB, dw_parts.at[0], dw_parts.at[1], sib)
    start(DW_X, dw_parts.at[0], dw_parts.at[2], xp)
    start(DW_XS, dw_parts.at[0], dw_parts.at[3], xs)

    copies[DKV_X].wait_recv()
    start(DKV_REL, dkv_ref.at[:, rows(tp ^ 2), :], dkv_ref.at[:, rows(tp ^ 2), :], sib)
    for i in (DW_SIB, DW_X, DW_XS):
        copies[i].wait_recv()
    parts = [dw_parts[jnp.bitwise_xor(tp, t)] for t in range(4)]
    dw_ref[...] = jnp.sum(parts[0] + parts[1] + parts[2] + parts[3], axis=0, keepdims=True)

    copies[DKV_SIB].wait_recv()
    copies[DKV_REL].wait_recv()
    copies[OQ_SIB].wait_recv()
    for i in (BULK_SIB, BULK_SIB + 1, BULK_REL, BULK_REL + 1, BULK_REL + 2, BULK_REL + 3):
        copies[i].wait_recv()
    own_a.wait()
    own_d.wait()
    for i in copies:
        copies[i].wait_send()
    for j in (1, 2, 3):
        rc(W_REL + j, w_all.at[2, :, quarter(j), :], w_all.at[3, :, quarter(j), :], sib).wait_send()


def grad_kernel(act_ref, dout_ref, w_ref, kv_ref, dkv_ref, oq_ref, cos_ref, sin_ref,
                dwq_ref, dwo_ref, dwkv_ref, q_s, do_s, o_s, dq_s, kt_ref, dwkv_s):
    i = pl.program_id(0)
    tp = lax.axis_index('tp')
    blk = tp ^ i
    own_rows = pl.ds(pl.multiple_of(blk * TB, TB), TB)

    @pl.when(i == 0)
    def _():
        transpose_kv(kv_ref, kt_ref)
        dwq_ref[...] = jnp.zeros_like(dwq_ref)
        dwo_ref[...] = jnp.zeros_like(dwo_ref)

    @pl.when(i < 2)
    def _():
        o_s[...] = oq_ref[jnp.minimum(i, 1), 0]
        dq_s[...] = oq_ref[jnp.minimum(i, 1), 1]

    @pl.when(i >= 2)
    def _():
        def pair(j, carry):
            cols = pl.ds(pl.multiple_of(j * 2 * HD, 2 * HD), 2 * HD)
            q = dot_nt(act_ref[0], w_ref[0, cols, :]).astype(BF16).astype(F32)
            for b in range(NB):
                r = slice(b * TB, (b + 1) * TB)
                for h in range(2):
                    piece = rope(q[r, h * HD:(h + 1) * HD], cos_ref[b, own_rows, :], sin_ref[b, own_rows, :]) * SCALE
                    q_s[r, pl.ds(pl.multiple_of((2 * j + h) * HD, HD), HD)] = piece.astype(BF16)
            do_s[:, cols] = dot_nt(dout_ref[0], w_ref[1, cols, :]).astype(BF16)
            return carry
        lax.fori_loop(0, HL // 2, pair, 0)
        for n in range(1, 5):
            @pl.when(blk == n - 1)
            def _():
                def step(t, carry):
                    b = t // 2
                    r = pl.ds(pl.multiple_of(b * TB, TB), TB)
                    for j in range(2):
                        c = pl.ds(pl.multiple_of(((t % 2) * 2 + j) * HD, HD), HD)
                        o, dq, _, _ = attend(n, q_s[r, c], do_s[r, c], kv_ref, b, kt_ref)
                        o_s[r, c] = o.astype(BF16)
                        dq = rope_back(dq * SCALE, cos_ref[b, own_rows, :], sin_ref[b, own_rows, :])
                        dq_s[r, c] = dq.astype(BF16)
                    return carry
                lax.fori_loop(0, 4, step, 0)

    ot = o_s[...].astype(F32).T.astype(BF16)
    dqt = dq_s[...].astype(F32).T.astype(BF16)
    dkvt = jnp.concatenate([dkv_ref[b, own_rows, :].astype(F32).T for b in range(NB)], axis=1).astype(BF16)

    def tile(j, carry):
        cols = pl.ds(pl.multiple_of(j * 512, 512), 512)
        a = act_ref[0, :, cols]
        dwo_ref[:, cols] += dot_nn(ot, dout_ref[0, :, cols])
        dwq_ref[:, cols] += dot_nn(dqt, a)
        kv_part = dot_nn(dkvt, a)

        @pl.when(i % 2 == 0)
        def _():
            dwkv_s[i // 2, :, cols] = kv_part

        @pl.when(i % 2 == 1)
        def _():
            dwkv_s[i // 2, :, cols] += kv_part
        return carry

    lax.fori_loop(0, 4, tile, 0)

    @pl.when(i == 3)
    def _():
        dwkv_ref[...] = dwkv_s[0] + dwkv_s[1]


def local_block(hidden, positions, norm_w, w_query, w_key, w_value, w_out, grad_out):
    tp = lax.axis_index('tp')
    x = hidden.reshape(TOK, D)
    dout = grad_out.reshape(TOK, D)
    xf = x.astype(F32)
    inv_rms = lax.rsqrt(jnp.mean(xf * xf, axis=-1, keepdims=True) + 1e-6)
    gain = (1.0 + norm_w)[None, :]
    act = (xf * inv_rms * gain).astype(BF16)
    w_own = jnp.stack([w_query.T, w_out])
    wkv = jnp.concatenate([w_key, w_value], axis=1)
    half = HD // 2
    inv_freq = 10000.0 ** (-2.0 * jnp.arange(half, dtype=F32) / HD)
    angle = positions.astype(F32)[..., None] * inv_freq
    cos_t, sin_t = jnp.cos(angle), jnp.sin(angle)
    cos_all = jnp.concatenate([cos_t, cos_t], axis=-1)
    sin_all = jnp.concatenate([-sin_t, sin_t], axis=-1)
    cos_own = lax.dynamic_slice_in_dim(cos_all, tp * TB, TB, axis=1).reshape(TOK, HD)
    sin_own = lax.dynamic_slice_in_dim(sin_all, tp * TB, TB, axis=1).reshape(TOK, HD)

    vmem = pl.BlockSpec(memory_space=pltpu.VMEM)
    anym = pl.BlockSpec(memory_space=pl.ANY)
    sds = jax.ShapeDtypeStruct
    out, dx, dw, _, act_all, dout_all, kv, dkv, oq = pl.pallas_call(
        main_kernel,
        out_shape=[sds((TOK, D), BF16), sds((TOK, D), BF16), sds((1, D), F32), sds((4, 2, HW, D), BF16),
                   sds((4, TOK, D), BF16), sds((4, TOK, D), BF16), sds((NB, SEQ, 2 * HD), BF16),
                   sds((NB, SEQ, 2 * HD), BF16), sds((2, 2, TOK, HW), BF16)],
        in_specs=[vmem, vmem, vmem, anym, vmem, vmem, vmem, vmem],
        out_specs=[vmem, vmem, vmem, anym, anym, anym, vmem, vmem, vmem],
        scratch_shapes=[
            pltpu.VMEM((2, HW, D), BF16),
            pltpu.VMEM((TOK, HW), BF16), pltpu.VMEM((TOK, HW), BF16),
            pltpu.VMEM((TOK, HW), BF16), pltpu.VMEM((TOK, HW), BF16),
            pltpu.VMEM((TOK, D), F32), pltpu.VMEM((TOK, D), F32),
            pltpu.VMEM((NB, 2 * HD, SEQ), BF16),
            pltpu.VMEM((NB, SEQ, 2 * HD), F32),
            pltpu.VMEM((2, NB, TB, 2 * HD), F32), pltpu.VMEM((2, NB, TB, 2 * HD), F32),
            pltpu.VMEM((2, TOK, HW), BF16),
            pltpu.VMEM((4, 8, D), F32),
            pltpu.SemaphoreType.DMA((N_SEM,)), pltpu.SemaphoreType.DMA((N_SEM,)), pltpu.SemaphoreType.DMA((3,)),
        ],
        compiler_params=pltpu.CompilerParams(collective_id=0, has_side_effects=True, vmem_limit_bytes=64_000_000),
        name='main',
    )(x, act, dout, w_own, wkv, gain, cos_own, sin_own)

    whole = lambda s: pl.BlockSpec(s, lambda t: (0,) * len(s))
    chunk = pl.BlockSpec((1, TOK, D), lambda t: (t, 0, 0))
    dwq, dwo, dwkv = pl.pallas_call(
        grad_kernel,
        grid=(4,),
        out_shape=[sds((HW, D), F32), sds((HW, D), F32), sds((2 * HD, D), F32)],
        in_specs=[chunk, chunk, whole((2, HW, D)), whole((NB, SEQ, 2 * HD)), whole((NB, SEQ, 2 * HD)),
                  whole((2, 2, TOK, HW)), whole((NB, SEQ, HD)), whole((NB, SEQ, HD))],
        out_specs=[whole((HW, D)), whole((HW, D)), whole((2 * HD, D))],
        scratch_shapes=[pltpu.VMEM((TOK, HW), BF16)] * 4 + [pltpu.VMEM((NB, 2 * HD, SEQ), BF16), pltpu.VMEM((2, 2 * HD, D), F32)],
        compiler_params=pltpu.CompilerParams(vmem_limit_bytes=64_000_000),
        name='grads',
    )(act_all, dout_all, w_own, kv, dkv, oq, cos_all, sin_all)

    return (out.reshape(NB, TB, D), dx.reshape(NB, TB, D), dwq.T, dwo, dwkv[:HD].T, dwkv[HD:].T, dw.reshape(D))


def solution(mesh):
    specs_in = (P('dp', 'tp', None), P('dp', None), P(None), P(None, 'tp'), P(None, None), P(None, None), P('tp', None), P('dp', 'tp', None))
    specs_out = (P('dp', 'tp', None), P('dp', 'tp', None), P('dp', 'tp'), P(('dp', 'tp'), None), P('dp', None), P('dp', None), P('dp'))
    return jax.shard_map(local_block, mesh=mesh, in_specs=specs_in, out_specs=specs_out, check_vma=False)
```

```python
import jax
import jax.numpy as jnp
from jax import lax
from jax.experimental import pallas as pl
from jax.experimental.pallas import tpu as pltpu
from jax.sharding import PartitionSpec as P

F32 = jnp.float32
BF16 = jnp.bfloat16
MESH = pl.DeviceIdType.MESH

TB = 256
NB = 2
TOK = TB * NB
SEQ = 1024
D = 2048
HD = 128
HL = 4
HW = HD * HL
SCALE = HD ** -0.5

WQ_X, WQ_Y, WQ_Z, WQ_YZ, WQ_REL, WQ_SIB = 0, 1, 2, 3, 4, 8
WO_X, WO_Y, WO_Z, WO_YZ, WO_REL, WO_SIB = 9, 10, 11, 12, 13, 17
KV_X, KV_SIB, KV_REL = 18, 19, 20
BULK_X, BULK_REL = 21, 25
DOUT_SIB, ACT_SIB = 29, 30
RS_SIB, RS_SIB2, RS_X = 31, 32, 33
DKV_X, DKV_SIB, DKV_REL = 35, 37, 39
DW_SIB, DW_X, DW_XS = 41, 42, 43
OQ_SIB = 44
N_SEM = 45


def dot_nn(a, b):
    return jnp.dot(a, b, preferred_element_type=F32)


def dot_nt(a, b):
    return lax.dot_general(a, b, (((1,), (1,)), ((), ())), preferred_element_type=F32)


def dot_tn(a, b):
    return lax.dot_general(a, b, (((0,), (0,)), ((), ())), preferred_element_type=F32)


def rope(u, cos_t, sin_t):
    return u * cos_t + pltpu.roll(u, HD // 2, 1) * sin_t


def rope_back(u, cos_t, sin_t):
    return u * cos_t - pltpu.roll(u, HD // 2, 1) * sin_t


def rope_back_t(u, cos_t, sin_t):
    swapped = jnp.concatenate([u[HD // 2:], u[:HD // 2]], axis=0)
    return u * cos_t - swapped * sin_t


def attend(n, q, do, k_ref, b, kt_ref):
    keys = n * TB
    k = k_ref[b, 0:keys, 0:HD]
    v = k_ref[b, 0:keys, HD:2 * HD]
    s = dot_nt(k, q)
    row = lax.broadcasted_iota(jnp.int32, (TB, TB), 0)
    col = lax.broadcasted_iota(jnp.int32, (TB, TB), 1)
    last = jnp.where(row <= col, s[keys - TB:], -1e30)
    s = last if n == 1 else jnp.concatenate([s[:keys - TB], last], axis=0)
    e = jnp.exp(s - jnp.max(s, axis=0, keepdims=True))
    p = e * (1.0 / jnp.sum(e, axis=0, keepdims=True))
    p_low = p.astype(BF16)
    dp = dot_nt(v, do)
    ds = (p * (dp - jnp.sum(p * dp, axis=0, keepdims=True))).astype(BF16)
    o_t = dot_nn(kt_ref[b, HD:2 * HD, 0:keys], p_low)
    dq_t = dot_nn(kt_ref[b, 0:HD, 0:keys], ds)
    return o_t, dq_t, p_low, ds


def transpose_kv(kv_ref, kt_ref):
    for b in range(NB):
        for j in range(4):
            kt_ref[b, :, j * TB:(j + 1) * TB] = kv_ref[b, j * TB:(j + 1) * TB, :].astype(F32).T.astype(BF16)


def main_kernel(x_hbm, dout_hbm, wq_own, wo_own, wk_own, wv_own, normw_ref, angle_hbm,
                out_hbm, dx_hbm, dw_ref, wq_all, wo_all, act_all, dout_all, dkv_hbm, oqt_hbm,
                x_ref, dout_ref, angle_ref, io_ref, dkv_ref, oqt, trig_t,
                act, kv_ref, wkv, cos_s, sin_s, wq_buf, wo_buf, q_s, do_s, o_s, dq_s, out_acc, da_acc, kt_ref,
                dkv_acc, rs_a, rs_b, rs_c, dw_parts, a_buf, d_buf, send, recv, lsem):
    dp = lax.axis_index('dp')
    tp = lax.axis_index('tp')
    sib = (dp, tp ^ 1)
    xp = (dp, tp ^ 2)
    xs = (dp, tp ^ 3)
    yp = (dp ^ 1, tp)
    zp = (dp ^ 2, tp)
    yzp = (dp ^ 3, tp)

    def rc(i, src, dst, dev):
        return pltpu.make_async_remote_copy(src_ref=src, dst_ref=dst, send_sem=send.at[i], recv_sem=recv.at[i],
                                            device_id=dev, device_id_type=MESH)

    def quarter(which, shard, j):
        size = 512 if which == 0 else 128
        r = pl.ds(pl.multiple_of((dp ^ j) * size, size), size)
        if shard is None:
            return (wq_own, wo_own)[which].at[r, :]
        return (wq_all, wo_all)[which].at[shard, r, :]

    def rows(blk):
        return pl.ds(pl.multiple_of(blk * TB, TB), TB)

    copies = {}

    def start(i, src, dst, dev):
        copies[i] = rc(i, src, dst, dev)
        copies[i].start()

    def local(i, src, dst):
        cp = pltpu.make_async_copy(src, dst, lsem.at[i])
        cp.start()
        return cp

    load_x = local(8, x_hbm, x_ref)
    load_a = local(9, angle_hbm, angle_ref)
    load_k = local(0, wk_own, wkv.at[:, 0:HD])
    load_v = local(1, wv_own, wkv.at[:, HD:2 * HD])
    load_q = local(2, wq_own, wq_buf.at[0])
    load_o = local(3, wo_own, wo_buf.at[0])
    load_d = local(4, dout_hbm, dout_ref)

    barrier = pltpu.get_barrier_semaphore()
    for dev in (sib, xp, xs, yp, zp, yzp):
        pl.semaphore_signal(barrier, inc=1, device_id=dev, device_id_type=MESH)
    pl.semaphore_wait(barrier, 6)

    start(WQ_X, quarter(0, None, 0), quarter(0, 2, 0), xp)
    start(WQ_SIB, wq_own, wq_all.at[1], sib)
    start(WO_SIB, wo_own, wo_all.at[1], sib)
    start(DOUT_SIB, dout_hbm, dout_all.at[1], sib)
    load_x.wait()
    load_a.wait()

    def norm_rows(j, carry):
        r = pl.ds(pl.multiple_of(j * 64, 64), 64)
        xf = x_ref[r, :].astype(F32)
        inv = lax.rsqrt(jnp.mean(xf * xf, axis=-1, keepdims=True) + 1e-6)
        act[r, :] = (xf * inv * (1.0 + normw_ref[...])).astype(BF16)
        return carry

    lax.fori_loop(0, TOK // 64, norm_rows, 0)
    lane = lax.broadcasted_iota(jnp.int32, (TB, HD), 1)

    def tables(blk):
        for b in range(NB):
            angle = angle_ref[b, rows(blk), :]
            sin_t = jnp.sin(angle)
            cos_s[b, rows(blk), :] = jnp.cos(angle)
            sin_s[b, rows(blk), :] = jnp.where(lane < HD // 2, -sin_t, sin_t)

    tables(tp)
    load_k.wait()
    load_v.wait()
    kv = dot_nn(act[...], wkv[...])
    for b in range(NB):
        r = slice(b * TB, (b + 1) * TB)
        k_rot = rope(kv[r, 0:HD].astype(BF16).astype(F32), cos_s[b, rows(tp), :], sin_s[b, rows(tp), :])
        kv_ref[b, rows(tp), 0:HD] = k_rot.astype(BF16)
        kv_ref[b, rows(tp), HD:2 * HD] = kv[r, HD:2 * HD].astype(BF16)
    own_kv = kv_ref.at[:, rows(tp), :]
    start(KV_X, own_kv, own_kv, xp)
    start(KV_SIB, own_kv, own_kv, sib)
    start(WO_X, quarter(1, None, 0), quarter(1, 2, 0), xp)
    start(BULK_X, dout_hbm.at[0:TB, :], dout_all.at[2, 0:TB, :], xp)
    start(ACT_SIB, act, act_all.at[1], sib)
    own_a = local(5, act, act_all.at[0])

    out_acc[...] = jnp.zeros_like(out_acc)
    da_acc[...] = jnp.zeros_like(da_acc)
    dkv_acc[...] = jnp.zeros_like(dkv_acc)

    def project(n_rows, a_src, d_src, slot, table):
        def pair(j, carry):
            cols = pl.ds(pl.multiple_of(j * 2 * HD, 2 * HD), 2 * HD)
            q = dot_nn(a_src[0:n_rows, :], wq_buf[slot, :, cols]).astype(BF16).astype(F32)
            for t in range(n_rows // TB):
                r = slice(t * TB, (t + 1) * TB)
                cos_t, sin_t = table(t)
                for h in range(2):
                    piece = rope(q[r, h * HD:(h + 1) * HD], cos_t, sin_t) * SCALE
                    q_s[r, pl.ds(pl.multiple_of((2 * j + h) * HD, HD), HD)] = piece.astype(BF16)
            do_s[0:n_rows, cols] = dot_nt(d_src[0:n_rows, :], wo_buf[slot, cols, :]).astype(BF16)
            return carry
        lax.fori_loop(0, HL // 2, pair, 0)

    def project_own(slot):
        project(TOK, act, dout_ref, slot, lambda b: (cos_s[b, rows(tp), :], sin_s[b, rows(tp), :]))

    def attend_group():
        for n in range(1, 5):
            @pl.when(tp == n - 1)
            def _():
                def step(t, carry):
                    b = t // 2
                    r = pl.ds(pl.multiple_of(b * TB, TB), TB)
                    cos_t = cos_s[b, rows(tp), :]
                    sin_t = sin_s[b, rows(tp), :]
                    for j in range(2):
                        c = pl.ds(pl.multiple_of(((t % 2) * 2 + j) * HD, HD), HD)
                        q = q_s[r, c]
                        do = do_s[r, c]
                        o_t, dq_t, p_low, ds = attend(n, q, do, kv_ref, b, kt_ref)
                        o_s[r, c] = o_t.T.astype(BF16)
                        dq_s[r, c] = rope_back(dq_t.T * SCALE, cos_t, sin_t).astype(BF16)
                        dkv_acc[b, 0:n * TB, 0:HD] += dot_nn(ds, q)
                        dkv_acc[b, 0:n * TB, HD:2 * HD] += dot_nn(p_low, do)
                    return carry
                lax.fori_loop(0, 4, step, 0)

    def accumulate(slot):
        def tile(j, carry):
            cols = pl.ds(pl.multiple_of(j * 512, 512), 512)
            out_acc[:, cols] += dot_nn(o_s[...], wo_buf[slot, :, cols])
            da_acc[:, cols] += dot_nt(dq_s[...], wq_buf[slot, cols, :])
            return carry
        lax.fori_loop(0, 4, tile, 0)

    def spread(which, ids):
        x_id, y_id, z_id, yz_id, rel_id = ids
        copies[x_id].wait_recv()
        mine = quarter(which, 2, 0)
        start(y_id, mine, mine, yp)
        start(z_id, mine, mine, zp)
        start(yz_id, mine, mine, yzp)
        start(rel_id, mine, quarter(which, 3, 0), sib)

    load_q.wait()
    load_o.wait()
    load_d.wait()
    own_d = local(4, dout_ref, dout_all.at[0])
    project_own(0)
    tables(tp ^ 2)
    tables(tp ^ 3)
    spread(0, (WQ_X, WQ_Y, WQ_Z, WQ_YZ, WQ_REL))
    copies[KV_X].wait_recv()
    other_kv = kv_ref.at[:, rows(tp ^ 2), :]
    start(KV_REL, other_kv, other_kv, sib)
    copies[KV_SIB].wait_recv()
    copies[KV_REL].wait_recv()
    transpose_kv(kv_ref, kt_ref)
    spread(1, (WO_X, WO_Y, WO_Z, WO_YZ, WO_REL))
    start(BULK_X + 1, act.at[0:TB, :], act_all.at[2, 0:TB, :], xp)
    start(BULK_X + 2, dout_hbm.at[TB:TOK, :], dout_all.at[2, TB:TOK, :], xp)
    start(BULK_X + 3, act.at[TB:TOK, :], act_all.at[2, TB:TOK, :], xp)

    def group(i, carry):
        slot = jnp.minimum(i, 1)

        @pl.when(i == 1)
        def _():
            rc(WQ_SIB, wq_own, wq_all.at[1], sib).wait_recv()
            rc(WO_SIB, wo_own, wo_all.at[1], sib).wait_recv()

        @pl.when(i == 2)
        def _():
            for which, first, rel in ((0, WQ_X, WQ_REL), (1, WO_X, WO_REL)):
                for j in (1, 2, 3):
                    piece = quarter(which, 2, j)
                    rc(first + j, piece, piece, sib).wait_recv()
                    rc(rel + j, piece, quarter(which, 3, j), sib).start()

        @pl.when(i == 3)
        def _():
            for which, rel in ((0, WQ_REL), (1, WO_REL)):
                for j in range(4):
                    rc(rel + j, quarter(which, 2, j), quarter(which, 3, j), sib).wait_recv()

        @pl.when(i > 0)
        def _():
            lq = local(2, wq_all.at[i], wq_buf.at[1])
            lo = local(3, wo_all.at[i], wo_buf.at[1])
            lq.wait()
            lo.wait()
            project_own(1)

        attend_group()
        accumulate(slot)

        @pl.when(i < 2)
        def _():
            for b in range(NB):
                r = slice(b * TB, (b + 1) * TB)
                o_t = o_s[r, :].astype(F32).T.astype(BF16)
                dq_t = dq_s[r, :].astype(F32).T.astype(BF16)

                @pl.when(i == 0)
                def _():
                    oqt[0, :, r] = o_t
                    oqt[1, :, r] = dq_t

                @pl.when(i == 1)
                def _():
                    rs_c[0, :, r] = o_t
                    rs_c[1, :, r] = dq_t
        return carry

    lax.fori_loop(0, 4, group, 0)

    start(RS_SIB, dkv_acc.at[:, rows(tp ^ 1), :], rs_a.at[0], sib)
    start(RS_SIB2, dkv_acc.at[:, rows(tp ^ 3), :], rs_a.at[1], sib)
    start(OQ_SIB, rs_c, oqt.at[:, :, TOK:2 * TOK], sib)
    for r in range(8):
        cols = slice(r * 256, (r + 1) * 256)
        io_ref[:, cols] = (x_ref[:, cols].astype(F32) + out_acc[:, cols]).astype(BF16)
    put_out = local(8, io_ref, out_hbm)
    copies[RS_SIB].wait_recv()
    copies[RS_SIB2].wait_recv()
    rs_b[0] = dkv_acc[:, rows(tp ^ 2), :] + rs_a[1]
    for b in range(NB):
        start(RS_X + b, rs_b.at[0, b], rs_b.at[1, b], xp)

    def head_part(t, carry):
        b = t // 2
        i = 2 + t % 2
        blk = tp ^ i
        r = pl.ds(pl.multiple_of(b * TB, TB), TB)

        def relay(c, whole):
            return rc(BULK_REL + 2 * b + c, whole.at[2, r, :], whole.at[3, r, :], sib)

        @pl.when(i == 2)
        def _():
            for c, whole in ((0, dout_all), (1, act_all)):
                rc(BULK_X + 2 * b + c, whole.at[2, r, :], whole.at[2, r, :], xp).wait_recv()
                relay(c, whole).start()

        @pl.when(i == 3)
        def _():
            relay(0, dout_all).wait_recv()
            relay(1, act_all).wait_recv()

        la = local(6, act_all.at[i, r, :], a_buf)
        ld = local(7, dout_all.at[i, r, :], d_buf)
        cos_t = cos_s.at[b, rows(blk), :]
        sin_t = sin_s.at[b, rows(blk), :]
        trig_t[0] = cos_t[...].T
        trig_t[1] = sin_t[...].T
        la.wait()
        ld.wait()
        project(TB, a_buf, d_buf, 0, lambda _: (cos_t[...], sin_t[...]))
        place = pl.ds(pl.multiple_of(i * TOK + b * TB, TB), TB)
        for n in range(1, 5):
            @pl.when(blk == n - 1)
            def _():
                def step(u, carry):
                    for j in range(2):
                        c = pl.ds(pl.multiple_of((u * 2 + j) * HD, HD), HD)
                        o_t, dq_t, _, _ = attend(n, q_s[0:TB, c], do_s[0:TB, c], kv_ref, b, kt_ref)
                        oqt[0, c, place] = o_t.astype(BF16)
                        oqt[1, c, place] = rope_back_t(dq_t * SCALE, trig_t[0], trig_t[1]).astype(BF16)
                    return carry
                lax.fori_loop(0, 2, step, 0)
        return carry

    lax.fori_loop(0, 4, head_part, 0)
    copies[OQ_SIB].wait_recv()
    put_oqt = local(9, oqt, oqt_hbm)
    put_out.wait()

    dw_parts[0] = jnp.zeros((8, D), F32)
    gain = 1.0 + normw_ref[...]

    def finish(b, carry):
        mine = pl.ds(pl.multiple_of(tp * TB, TB), TB)
        rc(RS_X + b, rs_b.at[0, b], rs_b.at[1, b], xp).wait_recv()
        total = dkv_acc[b, mine, :] + rs_a[0, b] + rs_b[1, b]
        dkv_ref[b, mine, 0:HD] = rope_back(total[:, 0:HD], cos_s[b, mine, :], sin_s[b, mine, :]).astype(BF16)
        dkv_ref[b, mine, HD:2 * HD] = total[:, HD:2 * HD].astype(BF16)
        piece = dkv_ref.at[b, mine, :]
        rc(DKV_X + b, piece, piece, xp).start()
        rc(DKV_SIB + b, piece, piece, sib).start()

        def dx_rows(j, carry):
            r = pl.ds(pl.multiple_of(b * TB + j * 128, 128), 128)
            d_own = dkv_ref[b, pl.ds(pl.multiple_of(tp * TB + j * 128, 128), 128), :]
            da = da_acc[r, :] + dot_nt(d_own, wkv[...])
            xf = x_ref[r, :].astype(F32)
            inv = lax.rsqrt(jnp.mean(xf * xf, axis=-1, keepdims=True) + 1e-6)
            normed = xf * inv
            prod = da * normed
            dw_parts[0] += jnp.sum(prod.reshape(16, 8, D), axis=0)
            corr = jnp.mean(prod * gain, axis=-1, keepdims=True)
            io_ref[r, :] = (dout_ref[r, :].astype(F32) + inv * (da * gain - normed * corr)).astype(BF16)
            return carry

        lax.fori_loop(0, 2, dx_rows, 0)
        return carry

    lax.fori_loop(0, NB, finish, 0)
    put_dx = local(8, io_ref, dx_hbm)
    start(DW_SIB, dw_parts.at[0], dw_parts.at[1], sib)
    start(DW_X, dw_parts.at[0], dw_parts.at[2], xp)
    start(DW_XS, dw_parts.at[0], dw_parts.at[3], xs)
    for b in range(NB):
        piece = dkv_ref.at[b, rows(tp ^ 2), :]
        rc(DKV_X + b, piece, piece, xp).wait_recv()
        start(DKV_REL + b, piece, piece, sib)
    for i in (DW_SIB, DW_X, DW_XS):
        copies[i].wait_recv()
    parts = [dw_parts[jnp.bitwise_xor(tp, t)] for t in range(4)]
    dw_ref[...] = jnp.sum(parts[0] + parts[1] + parts[2] + parts[3], axis=0, keepdims=True)

    for b in range(NB):
        piece = dkv_ref.at[b, rows(tp ^ 1), :]
        rc(DKV_SIB + b, piece, piece, sib).wait_recv()
        copies[DKV_REL + b].wait_recv()
    put_dkv = local(10, dkv_ref, dkv_hbm)
    copies[DOUT_SIB].wait_recv()
    copies[ACT_SIB].wait_recv()
    own_a.wait()
    own_d.wait()
    put_oqt.wait()
    put_dx.wait()
    put_dkv.wait()
    for i in copies:
        copies[i].wait_send()
    for which, rel in ((0, WQ_REL), (1, WO_REL)):
        for j in (1, 2, 3):
            rc(rel + j, quarter(which, 2, j), quarter(which, 3, j), sib).wait_send()
    for b in range(NB):
        piece = dkv_ref.at[b, rows(tp), :]
        rc(DKV_X + b, piece, piece, xp).wait_send()
        rc(DKV_SIB + b, piece, piece, sib).wait_send()
        r = slice(b * TB, (b + 1) * TB)
        rc(BULK_REL + 2 * b, dout_all.at[2, r, :], dout_all.at[3, r, :], sib).wait_send()
        rc(BULK_REL + 2 * b + 1, act_all.at[2, r, :], act_all.at[3, r, :], sib).wait_send()


def grad_kernel(act_ref, dout_ref, dkv_ref, oqt_ref, out_in, dx_in, dwq_ref, dwo_ref, dwk_ref, dwv_ref, out_ref, dx_ref, dkvt):
    tp = lax.axis_index('tp')
    out_ref[...] = out_in[...]
    dx_ref[...] = dx_in[...]

    @pl.when(pl.program_id(0) == 0)
    def _():
        for t in range(4):
            for b in range(NB):
                dkvt[t, :, b * TB:(b + 1) * TB] = dkv_ref[b, t * TB:(t + 1) * TB, :].astype(F32).T.astype(BF16)

    dwo_ref[...] = dot_nn(oqt_ref[0], dout_ref[...].reshape(4 * TOK, -1))
    dwq_ref[...] = dot_nn(oqt_ref[1], act_ref[...].reshape(4 * TOK, -1)).T
    total = dot_nn(dkvt[0], act_ref[jnp.bitwise_xor(tp, 0)])
    for t in range(1, 4):
        total += dot_nn(dkvt[t], act_ref[jnp.bitwise_xor(tp, t)])
    dwk_ref[...] = total[0:HD].T
    dwv_ref[...] = total[HD:2 * HD].T


def local_block(hidden, positions, norm_w, w_query, w_key, w_value, w_out, grad_out):
    x = hidden.reshape(TOK, D)
    dout = grad_out.reshape(TOK, D)
    half = HD // 2
    inv_freq = 10000.0 ** (-2.0 * (jnp.arange(HD) % half).astype(F32) / HD)
    angle = positions.astype(F32)[..., None] * inv_freq

    vmem = pl.BlockSpec(memory_space=pltpu.VMEM)
    anym = pl.BlockSpec(memory_space=pl.ANY)
    sds = jax.ShapeDtypeStruct
    out, dx, dw, _, _, act_all, dout_all, dkv, oqt = pl.pallas_call(
        main_kernel,
        out_shape=[sds((TOK, D), BF16), sds((TOK, D), BF16), sds((1, D), F32), sds((4, D, HW), BF16), sds((4, HW, D), BF16),
                   sds((4, TOK, D), BF16), sds((4, TOK, D), BF16), sds((NB, SEQ, 2 * HD), BF16), sds((2, HW, 4 * TOK), BF16)],
        in_specs=[anym, anym, anym, anym, anym, anym, vmem, anym],
        out_specs=[anym, anym, vmem, anym, anym, anym, anym, anym, anym],
        scratch_shapes=[
            pltpu.VMEM((TOK, D), BF16), pltpu.VMEM((TOK, D), BF16),
            pltpu.VMEM((NB, SEQ, HD), F32),
            pltpu.VMEM((TOK, D), BF16),
            pltpu.VMEM((NB, SEQ, 2 * HD), BF16),
            pltpu.VMEM((2, HW, 4 * TOK), BF16),
            pltpu.VMEM((2, HD, TB), F32),
            pltpu.VMEM((TOK, D), BF16),
            pltpu.VMEM((NB, SEQ, 2 * HD), BF16),
            pltpu.VMEM((D, 2 * HD), BF16),
            pltpu.VMEM((NB, SEQ, HD), F32), pltpu.VMEM((NB, SEQ, HD), F32),
            pltpu.VMEM((2, D, HW), BF16), pltpu.VMEM((2, HW, D), BF16),
            pltpu.VMEM((TOK, HW), BF16), pltpu.VMEM((TOK, HW), BF16),
            pltpu.VMEM((TOK, HW), BF16), pltpu.VMEM((TOK, HW), BF16),
            pltpu.VMEM((TOK, D), F32), pltpu.VMEM((TOK, D), F32),
            pltpu.VMEM((NB, 2 * HD, SEQ), BF16),
            pltpu.VMEM((NB, SEQ, 2 * HD), F32),
            pltpu.VMEM((2, NB, TB, 2 * HD), F32), pltpu.VMEM((2, NB, TB, 2 * HD), F32),
            pltpu.VMEM((2, TOK, HW), BF16),
            pltpu.VMEM((4, 8, D), F32),
            pltpu.VMEM((TB, D), BF16), pltpu.VMEM((TB, D), BF16),
            pltpu.SemaphoreType.DMA((N_SEM,)), pltpu.SemaphoreType.DMA((N_SEM,)), pltpu.SemaphoreType.DMA((11,)),
        ],
        compiler_params=pltpu.CompilerParams(collective_id=0, has_side_effects=True, vmem_limit_bytes=66_000_000),
        name='main',
    )(x, dout, w_query, w_out, w_key, w_value, norm_w[None, :], angle)

    whole = lambda s: pl.BlockSpec(s, lambda t: (0,) * len(s))
    cols = D // 8
    chunk = pl.BlockSpec((4, TOK, cols), lambda t: (0, 0, t))
    by_row = lambda r, c: pl.BlockSpec((r, c), lambda t: (t, 0))
    dwq, dwo, dwk, dwv, out, dx = pl.pallas_call(
        grad_kernel,
        grid=(8,),
        out_shape=[sds((D, HW), F32), sds((HW, D), F32), sds((D, HD), F32), sds((D, HD), F32), sds((TOK, D), BF16), sds((TOK, D), BF16)],
        in_specs=[chunk, chunk, whole((NB, SEQ, 2 * HD)), whole((2, HW, 4 * TOK)), by_row(TOK // 8, D), by_row(TOK // 8, D)],
        out_specs=[by_row(cols, HW), pl.BlockSpec((HW, cols), lambda t: (0, t)), by_row(cols, HD), by_row(cols, HD),
                   by_row(TOK // 8, D), by_row(TOK // 8, D)],
        scratch_shapes=[pltpu.VMEM((4, 2 * HD, TOK), BF16)],
        compiler_params=pltpu.CompilerParams(vmem_limit_bytes=64_000_000),
        name='grads',
    )(act_all, dout_all, dkv, oqt, out, dx)

    return out.reshape(NB, TB, D), dx.reshape(NB, TB, D), dwq, dwo, dwk, dwv, dw.reshape(D)


def solution(mesh):
    specs_in = (P('dp', 'tp', None), P('dp', None), P(None), P(None, 'tp'), P(None, None), P(None, None), P('tp', None), P('dp', 'tp', None))
    specs_out = (P('dp', 'tp', None), P('dp', 'tp', None), P('dp', 'tp'), P(('dp', 'tp'), None), P('dp', None), P('dp', None), P('dp'))
    return jax.shard_map(local_block, mesh=mesh, in_specs=specs_in, out_specs=specs_out, check_vma=False)
```

```python
import jax
import jax.numpy as jnp
import numpy as np
from jax import lax
from jax.experimental import pallas as pl
from jax.experimental.pallas import tpu as pltpu
from jax.sharding import PartitionSpec as P

F32 = jnp.float32
BF16 = jnp.bfloat16
MESH = pl.DeviceIdType.MESH

TB = 256
NB = 2
TOK = TB * NB
SEQ = 1024
D = 2048
HD = 128
HL = 4
HW = HD * HL
SCALE = HD ** -0.5

WQ_X, WQ_Y, WQ_Z, WQ_YZ, WQ_REL, WQ_SIB = 0, 1, 2, 3, 4, 8
WO_X, WO_Y, WO_Z, WO_YZ, WO_REL, WO_SIB = 9, 10, 11, 12, 13, 17
KV_X, KV_SIB, KV_REL = 18, 19, 20
BULK_X, BULK_REL = 21, 25
DOUT_SIB, ACT_SIB = 29, 30
RS_SIB, RS_SIB2, OQ_SIB = 31, 32, 33
DW_SIB, DW_X, DW_XS = 34, 35, 36
DKV_X, DKV_SIB, DKV_REL = 37, 41, 45
N_SEM = 49


def dot_nn(a, b):
    return jnp.dot(a, b, preferred_element_type=F32)


def dot_nt(a, b):
    return lax.dot_general(a, b, (((1,), (1,)), ((), ())), preferred_element_type=F32)


def dot_tn(a, b):
    return lax.dot_general(a, b, (((0,), (0,)), ((), ())), preferred_element_type=F32)


def rope(u, cos_t, sin_t):
    return u * cos_t + pltpu.roll(u, HD // 2, 1) * sin_t


def rope_back(u, cos_t, sin_t):
    return u * cos_t - pltpu.roll(u, HD // 2, 1) * sin_t


def rope_back_t(u, cos_t, sin_t):
    swapped = jnp.concatenate([u[HD // 2:], u[:HD // 2]], axis=0)
    return u * cos_t - swapped * sin_t


def attend(n, q, do, k_ref, b, kt_ref):
    keys = n * TB
    k = k_ref[b, 0:keys, 0:HD]
    v = k_ref[b, 0:keys, HD:2 * HD]
    s = dot_nt(k, q)
    row = lax.broadcasted_iota(jnp.int32, (TB, TB), 0)
    col = lax.broadcasted_iota(jnp.int32, (TB, TB), 1)
    last = jnp.where(row <= col, s[keys - TB:], -1e30)
    s = last if n == 1 else jnp.concatenate([s[:keys - TB], last], axis=0)
    e = jnp.exp(s - jnp.max(s, axis=0, keepdims=True))
    p = e * (1.0 / jnp.sum(e, axis=0, keepdims=True))
    p_low = p.astype(BF16)
    dp = dot_nt(v, do)
    ds = (p * (dp - jnp.sum(p * dp, axis=0, keepdims=True))).astype(BF16)
    o_t = dot_nn(kt_ref[b, HD:2 * HD, 0:keys], p_low)
    dq_t = dot_nn(kt_ref[b, 0:HD, 0:keys], ds)
    return o_t, dq_t, p_low, ds


def transpose_kv(kv_ref, kt_ref):
    for b in range(NB):
        for j in range(4):
            kt_ref[b, :, j * TB:(j + 1) * TB] = kv_ref[b, j * TB:(j + 1) * TB, :].astype(F32).T.astype(BF16)


def main_kernel(x_hbm, dout_hbm, wq_own, wo_own, wk_own, wv_own, normw_ref, pos_ref, freq_ref,
                out_hbm, dx_hbm, dw_ref, accq_hbm, acco_hbm, oqt_hbm, dkv_hbm, act_all, dout_all,
                x_ref, dout_ref, io_ref, dkv_ref, oqt, trig_t, dwq_acc,
                act, kv_ref, wkv, cos_s, sin_s, wq_buf, wo_buf, q_s, do_s, o_s, dq_s, out_acc, da_acc, kt_ref,
                dkv_acc, rs_a, rs_c, dw_parts, buf, send, recv, lsem):
    dp = lax.axis_index('dp')
    tp = lax.axis_index('tp')
    sib = (dp, tp ^ 1)
    xp = (dp, tp ^ 2)
    xs = (dp, tp ^ 3)
    yp = (dp ^ 1, tp)
    zp = (dp ^ 2, tp)
    yzp = (dp ^ 3, tp)

    def rc(i, src, dst, dev):
        return pltpu.make_async_remote_copy(src_ref=src, dst_ref=dst, send_sem=send.at[i], recv_sem=recv.at[i],
                                            device_id=dev, device_id_type=MESH)

    def quarter(which, shard, j):
        size = 512 if which == 0 else 128
        r = pl.ds(pl.multiple_of((dp ^ j) * size, size), size)
        if shard is None:
            return (wq_own, wo_own)[which].at[r, :]
        return (wq_buf, wo_buf)[which].at[shard, r, :]

    def rows(blk):
        return pl.ds(pl.multiple_of(blk * TB, TB), TB)

    copies = {}

    def start(i, src, dst, dev):
        copies[i] = rc(i, src, dst, dev)
        copies[i].start()

    def local(i, src, dst):
        cp = pltpu.make_async_copy(src, dst, lsem.at[i])
        cp.start()
        return cp

    def spread(which):
        first = (WQ_X, WO_X)[which]
        mine = quarter(which, 2, 0)
        rc(first, quarter(which, None, 0), mine, xp).wait_recv()
        for j, dev in ((1, yp), (2, zp), (3, yzp)):
            rc(first + j, mine, mine, dev).start()
        rc(first + 4, mine, quarter(which, 3, 0), sib).start()

    def bulk(c):
        r = pl.ds((c // 2) * TB, TB)
        src, dst = (act, act_all) if c % 2 else (dout_hbm, dout_all)
        return rc(BULK_X + c, src.at[r, :], dst.at[2, r, :], xp)

    load_x = local(8, x_hbm, x_ref)
    load_k = local(0, wk_own, wkv.at[:, 0:HD])
    load_v = local(1, wv_own, wkv.at[:, HD:2 * HD])
    load_q = local(2, wq_own, wq_buf.at[0])
    load_o = local(3, wo_own, wo_buf.at[0])
    load_d = local(4, dout_hbm, dout_ref)

    barrier = pltpu.get_barrier_semaphore()
    for dev in (sib, xp, xs, yp, zp, yzp):
        pl.semaphore_signal(barrier, inc=1, device_id=dev, device_id_type=MESH)
    pl.semaphore_wait(barrier, 6)

    start(WQ_X, quarter(0, None, 0), quarter(0, 2, 0), xp)
    start(WQ_SIB, wq_own, wq_buf.at[1], sib)
    start(WO_SIB, wo_own, wo_buf.at[1], sib)
    start(DOUT_SIB, dout_hbm, dout_all.at[1], sib)
    load_x.wait()

    def norm_rows(j, carry):
        r = pl.ds(pl.multiple_of(j * 64, 64), 64)
        xf = x_ref[r, :].astype(F32)
        inv = lax.rsqrt(jnp.mean(xf * xf, axis=-1, keepdims=True) + 1e-6)
        act[r, :] = (xf * inv * (1.0 + normw_ref[...])).astype(BF16)
        return carry

    lax.fori_loop(0, TOK // 64, norm_rows, 0)
    lane = lax.broadcasted_iota(jnp.int32, (HD, HD), 1)

    def tables(blk):
        for b in range(NB):
            for h in range(TB // HD):
                pos = pos_ref[b:b + 1, pl.ds(pl.multiple_of(blk * TB + h * HD, HD), HD)].astype(F32)
                angle = jnp.broadcast_to(pos, (HD, HD)).T * freq_ref[...]
                r = pl.ds(pl.multiple_of(blk * TB + h * HD, HD), HD)
                sin_t = jnp.sin(angle)
                cos_s[b, r, :] = jnp.cos(angle)
                sin_s[b, r, :] = jnp.where(lane < HD // 2, -sin_t, sin_t)

    tables(tp)
    load_k.wait()
    load_v.wait()
    kv = dot_nn(act[...], wkv[...])
    for b in range(NB):
        r = slice(b * TB, (b + 1) * TB)
        k_rot = rope(kv[r, 0:HD].astype(BF16).astype(F32), cos_s[b, rows(tp), :], sin_s[b, rows(tp), :])
        kv_ref[b, rows(tp), 0:HD] = k_rot.astype(BF16)
        kv_ref[b, rows(tp), HD:2 * HD] = kv[r, HD:2 * HD].astype(BF16)
    own_kv = kv_ref.at[:, rows(tp), :]
    start(KV_X, own_kv, own_kv, xp)
    start(KV_SIB, own_kv, own_kv, sib)
    start(WO_X, quarter(1, None, 0), quarter(1, 2, 0), xp)
    bulk(0).start()
    start(ACT_SIB, act, act_all.at[1], sib)
    own_a = local(5, act, act_all.at[0])

    out_acc[...] = jnp.zeros_like(out_acc)
    da_acc[...] = jnp.zeros_like(da_acc)
    dkv_acc[...] = jnp.zeros_like(dkv_acc)

    def project(n_rows, a_src, d_src, slot, table):
        def pair(j, carry):
            cols = pl.ds(pl.multiple_of(j * 2 * HD, 2 * HD), 2 * HD)
            q = dot_nn(a_src[0:n_rows, :], wq_buf[slot, :, cols]).astype(BF16).astype(F32)
            for t in range(n_rows // TB):
                r = slice(t * TB, (t + 1) * TB)
                cos_t, sin_t = table(t)
                for h in range(2):
                    piece = rope(q[r, h * HD:(h + 1) * HD], cos_t, sin_t) * SCALE
                    q_s[r, pl.ds(pl.multiple_of((2 * j + h) * HD, HD), HD)] = piece.astype(BF16)
            do_s[0:n_rows, cols] = dot_nt(d_src[0:n_rows, :], wo_buf[slot, cols, :]).astype(BF16)
            return carry
        lax.fori_loop(0, HL // 2, pair, 0)

    def project_own(slot):
        project(TOK, act, dout_ref, slot, lambda b: (cos_s[b, rows(tp), :], sin_s[b, rows(tp), :]))

    def attend_group():
        for n in range(1, 5):
            @pl.when(tp == n - 1)
            def _():
                def step(t, carry):
                    b = t // 2
                    r = pl.ds(pl.multiple_of(b * TB, TB), TB)
                    cos_t = cos_s[b, rows(tp), :]
                    sin_t = sin_s[b, rows(tp), :]
                    for j in range(2):
                        c = pl.ds(pl.multiple_of(((t % 2) * 2 + j) * HD, HD), HD)
                        q = q_s[r, c]
                        do = do_s[r, c]
                        o_t, dq_t, p_low, ds = attend(n, q, do, kv_ref, b, kt_ref)
                        o_s[r, c] = o_t.T.astype(BF16)
                        dq_s[r, c] = rope_back(dq_t.T * SCALE, cos_t, sin_t).astype(BF16)
                        dkv_acc[b, 0:n * TB, 0:HD] += dot_nn(ds, q)
                        dkv_acc[b, 0:n * TB, HD:2 * HD] += dot_nn(p_low, do)
                    return carry
                lax.fori_loop(0, 4, step, 0)

    def accumulate(slot):
        def tile(j, carry):
            cols = pl.ds(pl.multiple_of(j * 512, 512), 512)
            out_acc[:, cols] += dot_nn(o_s[...], wo_buf[slot, :, cols])
            da_acc[:, cols] += dot_nt(dq_s[...], wq_buf[slot, cols, :])
            return carry
        lax.fori_loop(0, 4, tile, 0)

    load_q.wait()
    load_o.wait()
    load_d.wait()
    own_d = local(4, dout_ref, dout_all.at[0])
    project_own(0)
    tables(tp ^ 2)
    tables(tp ^ 3)
    spread(0)
    copies[KV_X].wait_recv()
    other_kv = kv_ref.at[:, rows(tp ^ 2), :]
    start(KV_REL, other_kv, other_kv, sib)
    copies[KV_SIB].wait_recv()
    copies[KV_REL].wait_recv()
    transpose_kv(kv_ref, kt_ref)

    def group(i, carry):
        @pl.when(i == 1)
        def _():
            rc(WQ_SIB, wq_own, wq_buf.at[1], sib).wait_recv()
            rc(WO_SIB, wo_own, wo_buf.at[1], sib).wait_recv()

        @pl.when(i == 2)
        def _():
            for which, first in ((0, WQ_X), (1, WO_X)):
                for j in (1, 2, 3):
                    piece = quarter(which, 2, j)
                    rc(first + j, piece, piece, sib).wait_recv()
                    rc(first + 4 + j, piece, quarter(which, 3, j), sib).start()

        @pl.when(i == 3)
        def _():
            for which, rel in ((0, WQ_REL), (1, WO_REL)):
                for j in range(4):
                    rc(rel + j, quarter(which, 2, j), quarter(which, 3, j), sib).wait_recv()

        @pl.when(i > 0)
        def _():
            project_own(i)

        attend_group()

        @pl.when(i == 0)
        def _():
            spread(1)
            for c in (1, 2, 3):
                bulk(c).start()

        accumulate(i)

        @pl.when(i == 0)
        def _():
            oqt[0, 0] = o_s[...].astype(F32).T.astype(BF16)
            oqt[0, 1] = dq_s[...].astype(F32).T.astype(BF16)

        @pl.when(i == 1)
        def _():
            rs_c[0] = o_s[...].astype(F32).T.astype(BF16)
            rs_c[1] = dq_s[...].astype(F32).T.astype(BF16)
            rc(OQ_SIB, rs_c, oqt.at[1], sib).start()
        return carry

    lax.fori_loop(0, 4, group, 0)

    start(RS_SIB, dkv_acc.at[:, rows(tp ^ 1), :], rs_a.at[0], sib)
    start(RS_SIB2, dkv_acc.at[:, rows(tp ^ 3), :], rs_a.at[1], sib)
    for r in range(8):
        cols = slice(r * 256, (r + 1) * 256)
        io_ref[:, cols] = (x_ref[:, cols].astype(F32) + out_acc[:, cols]).astype(BF16)
    put_out = local(8, io_ref, out_hbm)
    copies[RS_SIB].wait_recv()
    copies[RS_SIB2].wait_recv()

    def dkv_piece(part, b, blk):
        return dkv_ref.at[part, b, rows(blk), :]

    for b in range(NB):
        for part, blk in ((0, tp), (1, tp ^ 2)):
            total = dkv_acc[b, rows(blk), :] + rs_a[part, b]
            d_k = rope_back(total[:, 0:HD], cos_s[b, rows(blk), :], sin_s[b, rows(blk), :])
            dkv_ref[part, b, rows(blk), 0:HD] = d_k.astype(BF16)
            dkv_ref[part, b, rows(blk), HD:2 * HD] = total[:, HD:2 * HD].astype(BF16)
    for b in range(NB):
        for part, blk in ((0, tp), (1, tp ^ 2)):
            piece = dkv_piece(part, b, blk)
            start(DKV_X + 2 * part + b, piece, piece, xp)
            start(DKV_SIB + 2 * part + b, piece, piece, sib)

    def weight_grads(first, o_t, dq_t, a_src, d_src):
        def tile(j, carry):
            cols = pl.ds(pl.multiple_of(j * 512, 512), 512)
            o_part = dot_nn(o_t[...], d_src[:, cols])
            q_part = dot_nn(dq_t[...], a_src[:, cols])
            if first:
                out_acc[:, cols] = o_part
                dwq_acc[:, cols] = q_part
            else:
                out_acc[:, cols] += o_part
                dwq_acc[:, cols] += q_part
            return carry
        lax.fori_loop(0, 4, tile, 0)

    copies[ACT_SIB].wait_recv()
    copies[DOUT_SIB].wait_recv()
    la = local(6, act_all.at[1], buf.at[0])
    ld = local(7, dout_all.at[1], buf.at[1])
    weight_grads(True, oqt.at[0, 0], oqt.at[0, 1], act, dout_ref)
    la.wait()
    ld.wait()
    rc(OQ_SIB, rs_c, oqt.at[1], sib).wait_recv()
    weight_grads(False, oqt.at[1, 0], oqt.at[1, 1], buf.at[0], buf.at[1])

    def head_part(t, carry):
        b = t // 2
        i = 2 + t % 2
        blk = tp ^ i
        r = pl.ds(pl.multiple_of(b * TB, TB), TB)

        def relay(c, whole):
            return rc(BULK_REL + 2 * b + c, whole.at[2, r, :], whole.at[3, r, :], sib)

        def load(k):
            half = pl.ds(k * TB, TB)
            return (pltpu.make_async_copy(act_all.at[2 + k, r, :], buf.at[0, half, :], lsem.at[6]),
                    pltpu.make_async_copy(dout_all.at[2 + k, r, :], buf.at[1, half, :], lsem.at[7]))

        @pl.when(i == 2)
        def _():
            for c, whole in ((0, dout_all), (1, act_all)):
                rc(BULK_X + 2 * b + c, whole.at[2, r, :], whole.at[2, r, :], xp).wait_recv()
                relay(c, whole).start()
            for cp in load(0):
                cp.start()

        cos_t = cos_s.at[b, rows(blk), :]
        sin_t = sin_s.at[b, rows(blk), :]
        trig_t[0] = cos_t[...].T
        trig_t[1] = sin_t[...].T
        half = pl.ds(pl.multiple_of((i - 2) * TB, TB), TB)
        for cp in load(0):
            cp.wait()
        project(TB, buf.at[0, half, :], buf.at[1, half, :], 0, lambda _: (cos_t[...], sin_t[...]))

        @pl.when(i == 2)
        def _():
            relay(0, dout_all).wait_recv()
            relay(1, act_all).wait_recv()
            for cp in load(1):
                cp.start()

        for n in range(1, 5):
            @pl.when(blk == n - 1)
            def _():
                def step(u, carry):
                    for j in range(2):
                        c = pl.ds(pl.multiple_of((u * 2 + j) * HD, HD), HD)
                        o_t, dq_t, _, _ = attend(n, q_s[0:TB, c], do_s[0:TB, c], kv_ref, b, kt_ref)
                        oqt[0, 0, c, half] = o_t.astype(BF16)
                        oqt[0, 1, c, half] = rope_back_t(dq_t * SCALE, trig_t[0], trig_t[1]).astype(BF16)
                    return carry
                lax.fori_loop(0, 2, step, 0)

        @pl.when(t == 1)
        def _():
            weight_grads(False, oqt.at[0, 0], oqt.at[0, 1], buf.at[0], buf.at[1])
            pltpu.make_async_copy(dwq_acc, accq_hbm, lsem.at[9]).start()
            pltpu.make_async_copy(out_acc, acco_hbm, lsem.at[10]).start()
        return carry

    lax.fori_loop(0, 4, head_part, 0)
    put_oqt = local(0, oqt.at[0], oqt_hbm)
    put_out.wait()

    dw_parts[0] = jnp.zeros((8, D), F32)
    gain = 1.0 + normw_ref[...]
    put_dkv = []

    for b in range(NB):
        for part, blk in ((0, tp ^ 2), (1, tp)):
            piece = dkv_piece(part, b, blk)
            rc(DKV_X + 2 * part + b, piece, piece, xp).wait_recv()
            start(DKV_REL + 2 * part + b, piece, piece, sib)

        def dx_rows(j, carry):
            r = pl.ds(pl.multiple_of(b * TB + j * 128, 128), 128)
            own = pl.ds(pl.multiple_of(tp * TB + j * 128, 128), 128)
            da = da_acc[r, :] + dot_nt(dkv_ref[0, b, own, :], wkv[...]) + dot_nt(dkv_ref[1, b, own, :], wkv[...])
            xf = x_ref[r, :].astype(F32)
            inv = lax.rsqrt(jnp.mean(xf * xf, axis=-1, keepdims=True) + 1e-6)
            normed = xf * inv
            prod = da * normed
            dw_parts[0] += jnp.sum(prod.reshape(16, 8, D), axis=0)
            corr = jnp.mean(prod * gain, axis=-1, keepdims=True)
            io_ref[r, :] = (dout_ref[r, :].astype(F32) + inv * (da * gain - normed * corr)).astype(BF16)
            return carry

        lax.fori_loop(0, 2, dx_rows, 0)
        if b == NB - 1:
            put_dx = local(8, io_ref, dx_hbm)
            start(DW_SIB, dw_parts.at[0], dw_parts.at[1], sib)
            start(DW_X, dw_parts.at[0], dw_parts.at[2], xp)
            start(DW_XS, dw_parts.at[0], dw_parts.at[3], xs)
        for part, blk, rel in ((0, tp ^ 1, tp ^ 3), (1, tp ^ 3, tp ^ 1)):
            piece = dkv_piece(part, b, blk)
            rc(DKV_SIB + 2 * part + b, piece, piece, sib).wait_recv()
            piece = dkv_piece(part, b, rel)
            rc(DKV_REL + 2 * part + b, piece, piece, sib).wait_recv()
        put_dkv.append(local(1 + b, dkv_ref.at[:, b], dkv_hbm.at[:, b]))

    for i in (DW_SIB, DW_X, DW_XS):
        copies[i].wait_recv()
    parts = [dw_parts[jnp.bitwise_xor(tp, t)] for t in range(4)]
    dw_ref[...] = jnp.sum(parts[0] + parts[1] + parts[2] + parts[3], axis=0, keepdims=True)

    own_a.wait()
    own_d.wait()
    for cp in (put_oqt, put_dx, *put_dkv):
        cp.wait()
    pltpu.make_async_copy(dwq_acc, accq_hbm, lsem.at[9]).wait()
    pltpu.make_async_copy(out_acc, acco_hbm, lsem.at[10]).wait()
    for i in copies:
        copies[i].wait_send()
    rc(OQ_SIB, rs_c, oqt.at[1], sib).wait_send()
    for c in range(4):
        bulk(c).wait_send()
        whole = act_all if c % 2 else dout_all
        r = slice((c // 2) * TB, (c // 2 + 1) * TB)
        rc(BULK_REL + c, whole.at[2, r, :], whole.at[3, r, :], sib).wait_send()
    for which, first in ((0, WQ_X), (1, WO_X)):
        for j in range(1, 8):
            rc(first + j, quarter(which, 2, j % 4), quarter(which, 2, j % 4), sib).wait_send()


def grad_kernel(accq_ref, acco_ref, act_ref, dout_ref, oqt_ref, dkv_ref, out_in, dx_in,
                dwq_ref, dwo_ref, dwk_ref, dwv_ref, out_ref, dx_ref, dkvt):
    tp = lax.axis_index('tp')
    out_ref[...] = out_in[...]
    dx_ref[...] = dx_in[...]

    @pl.when(pl.program_id(0) == 0)
    def _():
        for t in range(6):
            for b in range(NB):
                piece = dkv_ref[t // 4, b, (t % 4) * TB:(t % 4 + 1) * TB, :]
                dkvt[t, :, b * TB:(b + 1) * TB] = piece.astype(F32).T.astype(BF16)

    a = jnp.concatenate([act_ref[2, TB:TOK, :], act_ref[3, TB:TOK, :]], axis=0)
    d = dout_ref[...].reshape(TOK, -1)
    dwo_ref[...] = acco_ref[...] + dot_nn(oqt_ref[0], d)
    dwq_ref[...] = (accq_ref[...] + dot_nn(oqt_ref[1], a)).T
    total = dot_nn(dkvt[0], act_ref[jnp.bitwise_xor(tp, 0)])
    for t in range(1, 6):
        total += dot_nn(dkvt[t], act_ref[jnp.bitwise_xor(tp, t % 4)])
    dwk_ref[...] = total[0:HD].T
    dwv_ref[...] = total[HD:2 * HD].T


def local_block(hidden, positions, norm_w, w_query, w_key, w_value, w_out, grad_out):
    x = hidden.reshape(TOK, D)
    dout = grad_out.reshape(TOK, D)
    freq = 10000.0 ** (-2.0 * (np.arange(HD) % (HD // 2)) / HD)

    vmem = pl.BlockSpec(memory_space=pltpu.VMEM)
    anym = pl.BlockSpec(memory_space=pl.ANY)
    sds = jax.ShapeDtypeStruct
    out, dx, dw, accq, acco, oqt, dkv, act_all, dout_all = pl.pallas_call(
        main_kernel,
        out_shape=[sds((TOK, D), BF16), sds((TOK, D), BF16), sds((1, D), F32), sds((HW, D), F32), sds((HW, D), F32),
                   sds((2, HW, TOK), BF16), sds((2, NB, SEQ, 2 * HD), BF16), sds((4, TOK, D), BF16), sds((4, TOK, D), BF16)],
        in_specs=[anym, anym, anym, anym, anym, anym, vmem, vmem, vmem],
        out_specs=[anym, anym, vmem, anym, anym, anym, anym, anym, anym],
        scratch_shapes=[
            pltpu.VMEM((TOK, D), BF16), pltpu.VMEM((TOK, D), BF16), pltpu.VMEM((TOK, D), BF16),
            pltpu.VMEM((2, NB, SEQ, 2 * HD), BF16),
            pltpu.VMEM((2, 2, HW, TOK), BF16),
            pltpu.VMEM((2, HD, TB), F32),
            pltpu.VMEM((HW, D), F32),
            pltpu.VMEM((TOK, D), BF16),
            pltpu.VMEM((NB, SEQ, 2 * HD), BF16),
            pltpu.VMEM((D, 2 * HD), BF16),
            pltpu.VMEM((NB, SEQ, HD), F32), pltpu.VMEM((NB, SEQ, HD), F32),
            pltpu.VMEM((4, D, HW), BF16), pltpu.VMEM((4, HW, D), BF16),
            pltpu.VMEM((TOK, HW), BF16), pltpu.VMEM((TOK, HW), BF16),
            pltpu.VMEM((TOK, HW), BF16), pltpu.VMEM((TOK, HW), BF16),
            pltpu.VMEM((TOK, D), F32), pltpu.VMEM((TOK, D), F32),
            pltpu.VMEM((NB, 2 * HD, SEQ), BF16),
            pltpu.VMEM((NB, SEQ, 2 * HD), F32),
            pltpu.VMEM((2, NB, TB, 2 * HD), F32),
            pltpu.VMEM((2, HW, TOK), BF16),
            pltpu.VMEM((4, 8, D), F32),
            pltpu.VMEM((2, TOK, D), BF16),
            pltpu.SemaphoreType.DMA((N_SEM,)), pltpu.SemaphoreType.DMA((N_SEM,)), pltpu.SemaphoreType.DMA((11,)),
        ],
        compiler_params=pltpu.CompilerParams(collective_id=0, has_side_effects=True, vmem_limit_bytes=67_000_000),
        name='main',
    )(x, dout, w_query, w_out, w_key, w_value, norm_w[None, :], positions, jnp.asarray(freq[None, :], F32))

    whole = lambda s: pl.BlockSpec(s, lambda t: (0,) * len(s))
    cols = D // 8
    by_row = lambda r, c: pl.BlockSpec((r, c), lambda t: (t, 0))
    by_col = pl.BlockSpec((HW, cols), lambda t: (0, t))
    dwq, dwo, dwk, dwv, out, dx = pl.pallas_call(
        grad_kernel,
        grid=(8,),
        out_shape=[sds((D, HW), F32), sds((HW, D), F32), sds((D, HD), F32), sds((D, HD), F32), sds((TOK, D), BF16), sds((TOK, D), BF16)],
        in_specs=[by_col, by_col, pl.BlockSpec((4, TOK, cols), lambda t: (0, 0, t)), pl.BlockSpec((2, TB, cols), lambda t: (1, 1, t)),
                  whole((2, HW, TOK)), whole((2, NB, SEQ, 2 * HD)), by_row(TOK // 8, D), by_row(TOK // 8, D)],
        out_specs=[by_row(cols, HW), by_col, by_row(cols, HD), by_row(cols, HD), by_row(TOK // 8, D), by_row(TOK // 8, D)],
        scratch_shapes=[pltpu.VMEM((6, 2 * HD, TOK), BF16)],
        compiler_params=pltpu.CompilerParams(vmem_limit_bytes=64_000_000),
        name='grads',
    )(accq, acco, act_all, dout_all, oqt, dkv, out, dx)

    return out.reshape(NB, TB, D), dx.reshape(NB, TB, D), dwq, dwo, dwk, dwv, dw.reshape(D)


def solution(mesh):
    specs_in = (P('dp', 'tp', None), P('dp', None), P(None), P(None, 'tp'), P(None, None), P(None, None), P('tp', None), P('dp', 'tp', None))
    specs_out = (P('dp', 'tp', None), P('dp', 'tp', None), P('dp', 'tp'), P(('dp', 'tp'), None), P('dp', None), P('dp', None), P('dp'))
    return jax.shard_map(local_block, mesh=mesh, in_specs=specs_in, out_specs=specs_out, check_vma=False)
```

```python
import jax
import jax.numpy as jnp
import numpy as np
from jax import lax
from jax.experimental import pallas as pl
from jax.experimental.pallas import tpu as pltpu
from jax.sharding import PartitionSpec as P

F32 = jnp.float32
BF16 = jnp.bfloat16
MESH = pl.DeviceIdType.MESH

TB = 256
NB = 2
TOK = TB * NB
SEQ = 1024
D = 2048
HD = 128
HL = 4
HW = HD * HL
SCALE = HD ** -0.5

N_SEM = 51
(WQ_X, _, _, _, WQ_REL, _, _, _, WQ_SIB,
 WO_X, _, _, _, WO_REL, _, _, _, WO_SIB,
 KV_X, KV_SIB, KV_REL, KV_LATE, _,
 BULK_X, _, _, _, BULK_REL, _, _, _,
 DOUT_SIB, ACT_SIB, RS_SIB, RS_SIB2, OQ_SIB, DW_SIB, DW_X, DW_XS,
 DKV_X, _, _, _, DKV_SIB, _, _, _, DKV_REL, _, _, _) = range(N_SEM)
KEY = slice(HD)
VAL = slice(HD, 2 * HD)


def dot_nn(a, b):
    return jnp.dot(a, b, preferred_element_type=F32)


def dot_nt(a, b):
    return lax.dot_general(a, b, (((1,), (1,)), ((), ())), preferred_element_type=F32)


def dot_tn(a, b):
    return lax.dot_general(a, b, (((0,), (0,)), ((), ())), preferred_element_type=F32)


def rope(u, cos_t, sin_t):
    return u * cos_t + pltpu.roll(u, HD // 2, 1) * sin_t


def rope_back(u, cos_t, sin_t):
    return u * cos_t - pltpu.roll(u, HD // 2, 1) * sin_t


def rope_back_t(u, cos_t, sin_t):
    swapped = jnp.concatenate([u[HD // 2:], u[:HD // 2]], axis=0)
    return u * cos_t - swapped * sin_t


def attend(n, q, do, k_ref, b, kt_ref):
    keys = n * TB
    k = k_ref[b, 0:keys, KEY]
    v = k_ref[b, 0:keys, VAL]
    s = dot_nt(k, q)
    row = lax.broadcasted_iota(jnp.int32, (TB, TB), 0)
    col = lax.broadcasted_iota(jnp.int32, (TB, TB), 1)
    last = jnp.where(row <= col, s[keys - TB:], -1e30)
    s = last if n == 1 else jnp.concatenate([s[:keys - TB], last], axis=0)
    e = jnp.exp(s - jnp.max(s, axis=0, keepdims=True))
    p = e * (1.0 / jnp.sum(e, axis=0, keepdims=True))
    p_low = p.astype(BF16)
    dp = dot_nt(v, do)
    ds = (p * (dp - jnp.sum(p * dp, axis=0, keepdims=True))).astype(BF16)
    o_t = dot_nn(kt_ref[b, VAL, 0:keys], p_low)
    dq_t = dot_nn(kt_ref[b, KEY, 0:keys], ds)
    return o_t, dq_t, p_low, ds


def transpose_kv(kv_ref, kt_ref, b, later):
    for j in range(2):
        r = pl.ds(pl.multiple_of((2 * later + j) * TB, TB), TB)
        kt_ref[b, :, r] = kv_ref[b, r, :].astype(F32).T.astype(BF16)


def main_kernel(x_hbm, dout_hbm, wq_own, wo_own, wk_own, wv_own, normw_ref, pos_ref, freq_ref,
                out_hbm, dx_hbm, dw_ref, accq_hbm, acco_hbm, oqt_hbm, dkv_hbm, act_all, dout_all,
                x_ref, dout_ref, io_ref, dkv_ref, oqt, trig_t, dwq_acc,
                act, kv_ref, wkv, cos_s, sin_s, wq_buf, wo_buf, q_s, do_s, o_s, dq_s, out_acc, da_acc, kt_ref,
                dkv_acc, rs_a, rs_c, dw_parts, buf, send, recv, lsem):
    dp = lax.axis_index('dp')
    tp = lax.axis_index('tp')
    sib = (dp, tp ^ 1)
    xp = (dp, tp ^ 2)
    xs = (dp, tp ^ 3)
    yp = (dp ^ 1, tp)
    zp = (dp ^ 2, tp)
    yzp = (dp ^ 3, tp)

    def rc(i, src, dst, dev):
        return pltpu.make_async_remote_copy(src_ref=src, dst_ref=dst, send_sem=send.at[i], recv_sem=recv.at[i],
                                            device_id=dev, device_id_type=MESH)

    def quarter(which, shard, j):
        size = 512 if which == 0 else 128
        r = pl.ds(pl.multiple_of((dp ^ j) * size, size), size)
        if shard is None:
            return (wq_own, wo_own)[which].at[r, :]
        return (wq_buf, wo_buf)[which].at[shard, r, :]

    def rows(blk):
        return pl.ds(pl.multiple_of(blk * TB, TB), TB)

    copies = {}

    def start(i, src, dst, dev):
        copies[i] = rc(i, src, dst, dev)
        copies[i].start()

    def local(i, src, dst):
        cp = pltpu.make_async_copy(src, dst, lsem.at[i])
        cp.start()
        return cp

    def spread(which):
        first = (WQ_X, WO_X)[which]
        mine = quarter(which, 2, 0)
        rc(first, quarter(which, None, 0), mine, xp).wait_recv()
        for j, dev in ((1, yp), (2, zp), (3, yzp)):
            rc(first + j, mine, mine, dev).start()
        rc(first + 4, mine, quarter(which, 3, 0), sib).start()

    def bulk(c):
        r = pl.ds((c // 2) * TB, TB)
        src, dst = (act, act_all) if c % 2 else (dout_hbm, dout_all)
        return rc(BULK_X + c, src.at[r, :], dst.at[2, r, :], xp)

    load_x = local(8, x_hbm, x_ref)
    load_k = local(0, wk_own, wkv.at[:, KEY])
    load_v = local(1, wv_own, wkv.at[:, VAL])
    load_q = local(2, wq_own, wq_buf.at[0])
    load_o = local(3, wo_own, wo_buf.at[0])
    load_d = local(4, dout_hbm, dout_ref)

    barrier = pltpu.get_barrier_semaphore()
    for dev in (sib, xp, xs, yp, zp, yzp):
        pl.semaphore_signal(barrier, inc=1, device_id=dev, device_id_type=MESH)
    pl.semaphore_wait(barrier, 6)

    start(WQ_X, quarter(0, None, 0), quarter(0, 2, 0), xp)
    start(WQ_SIB, wq_own, wq_buf.at[1], sib)
    start(WO_SIB, wo_own, wo_buf.at[1], sib)
    start(DOUT_SIB, dout_hbm, dout_all.at[1], sib)
    load_x.wait()

    def norm_rows(j, carry):
        r = pl.ds(pl.multiple_of(j * 64, 64), 64)
        xf = x_ref[r, :].astype(F32)
        inv = lax.rsqrt(jnp.mean(xf * xf, axis=-1, keepdims=True) + 1e-6)
        act[r, :] = (xf * inv * (1.0 + normw_ref[...])).astype(BF16)
        return carry

    lax.fori_loop(0, TOK // 64, norm_rows, 0)
    lane = lax.broadcasted_iota(jnp.int32, (HD, HD), 1)

    def tables(blk):
        for b in range(NB):
            for h in range(TB // HD):
                pos = pos_ref[b:b + 1, pl.ds(pl.multiple_of(blk * TB + h * HD, HD), HD)].astype(F32)
                angle = jnp.broadcast_to(pos, (HD, HD)).T * freq_ref[...]
                r = pl.ds(pl.multiple_of(blk * TB + h * HD, HD), HD)
                sin_t = jnp.sin(angle)
                cos_s[b, r, :] = jnp.cos(angle)
                sin_s[b, r, :] = jnp.where(lane < HD // 2, -sin_t, sin_t)

    tables(tp)
    load_k.wait()
    load_v.wait()
    kv = dot_nn(act[...], wkv[...])
    for b in range(NB):
        r = slice(b * TB, (b + 1) * TB)
        k_rot = rope(kv[r, KEY].astype(BF16).astype(F32), cos_s[b, rows(tp), :], sin_s[b, rows(tp), :])
        kv_ref[b, rows(tp), KEY] = k_rot.astype(BF16)
        kv_ref[b, rows(tp), VAL] = kv[r, VAL].astype(BF16)
    own_kv = kv_ref.at[:, rows(tp), :]

    @pl.when(tp < 2)
    def _():
        rc(KV_X, own_kv, own_kv, xp).start()

    start(KV_SIB, own_kv, own_kv, sib)
    start(WO_X, quarter(1, None, 0), quarter(1, 2, 0), xp)
    bulk(0).start()
    start(ACT_SIB, act, act_all.at[1], sib)
    own_a = local(5, act, act_all.at[0])

    out_acc[...] = jnp.zeros_like(out_acc)
    da_acc[...] = jnp.zeros_like(da_acc)
    dkv_acc[...] = jnp.zeros_like(dkv_acc)

    def project(n_rows, a_src, d_src, slot, table):
        def pair(j, carry):
            cols = pl.ds(pl.multiple_of(j * 2 * HD, 2 * HD), 2 * HD)
            q = dot_nn(a_src[0:n_rows, :], wq_buf[slot, :, cols]).astype(BF16).astype(F32)
            for t in range(n_rows // TB):
                r = slice(t * TB, (t + 1) * TB)
                cos_t, sin_t = table(t)
                for h in range(2):
                    piece = rope(q[r, h * HD:(h + 1) * HD], cos_t, sin_t) * SCALE
                    q_s[r, pl.ds(pl.multiple_of((2 * j + h) * HD, HD), HD)] = piece.astype(BF16)
            do_s[0:n_rows, cols] = dot_nt(d_src[0:n_rows, :], wo_buf[slot, cols, :]).astype(BF16)
            return carry
        lax.fori_loop(0, HL // 2, pair, 0)

    def project_own(slot):
        project(TOK, act, dout_ref, slot, lambda b: (cos_s[b, rows(tp), :], sin_s[b, rows(tp), :]))

    def attend_group():
        for n in range(1, 5):
            @pl.when(tp == n - 1)
            def _():
                def step(t, carry):
                    b = t // 2
                    r = pl.ds(pl.multiple_of(b * TB, TB), TB)
                    cos_t = cos_s[b, rows(tp), :]
                    sin_t = sin_s[b, rows(tp), :]
                    for j in range(2):
                        c = pl.ds(pl.multiple_of(((t % 2) * 2 + j) * HD, HD), HD)
                        q = q_s[r, c]
                        do = do_s[r, c]
                        o_t, dq_t, p_low, ds = attend(n, q, do, kv_ref, b, kt_ref)
                        o_s[r, c] = o_t.T.astype(BF16)
                        dq_s[r, c] = rope_back(dq_t.T * SCALE, cos_t, sin_t).astype(BF16)
                        dkv_acc[b, 0:n * TB, KEY] += dot_nn(ds, q)
                        dkv_acc[b, 0:n * TB, VAL] += dot_nn(p_low, do)
                    return carry
                lax.fori_loop(0, 4, step, 0)

    def accumulate(slot):
        def tile(j, carry):
            cols = pl.ds(pl.multiple_of(j * 512, 512), 512)
            out_acc[:, cols] += dot_nn(o_s[...], wo_buf[slot, :, cols])
            da_acc[:, cols] += dot_nt(dq_s[...], wq_buf[slot, cols, :])
            return carry
        lax.fori_loop(0, 4, tile, 0)

    load_q.wait()
    load_o.wait()
    load_d.wait()
    own_d = local(4, dout_ref, dout_all.at[0])
    project_own(0)
    tables(tp ^ 2)
    tables(tp ^ 3)
    spread(0)
    other_kv = kv_ref.at[:, rows(tp ^ 2), :]

    @pl.when(tp >= 2)
    def _():
        rc(KV_X, other_kv, other_kv, xp).wait_recv()
        rc(KV_REL, other_kv, other_kv, sib).start()

    copies[KV_SIB].wait_recv()
    for b in range(NB):
        transpose_kv(kv_ref, kt_ref, b, tp // 2)

    @pl.when(tp >= 2)
    def _():
        sib_kv = kv_ref.at[:, rows(tp ^ 3), :]
        rc(KV_REL, sib_kv, sib_kv, sib).wait_recv()
        for b in range(NB):
            transpose_kv(kv_ref, kt_ref, b, False)

    def group(i, carry):
        @pl.when(i == 1)
        def _():
            rc(WQ_SIB, wq_own, wq_buf.at[1], sib).wait_recv()
            rc(WO_SIB, wo_own, wo_buf.at[1], sib).wait_recv()

        @pl.when(i == 2)
        def _():
            for which, first in ((0, WQ_X), (1, WO_X)):
                for j in (1, 2, 3):
                    piece = quarter(which, 2, j)
                    rc(first + j, piece, piece, sib).wait_recv()
                    rc(first + 4 + j, piece, quarter(which, 3, j), sib).start()

        @pl.when(i == 3)
        def _():
            for which, rel in ((0, WQ_REL), (1, WO_REL)):
                for j in range(4):
                    rc(rel + j, quarter(which, 2, j), quarter(which, 3, j), sib).wait_recv()

        @pl.when(i > 0)
        def _():
            project_own(i)

        attend_group()

        @pl.when(i == 0)
        def _():
            spread(1)
            for c in (1, 2, 3):
                bulk(c).start()

        accumulate(i)

        @pl.when(i == 0)
        def _():
            oqt[0, 0] = o_s[...].astype(F32).T.astype(BF16)
            oqt[0, 1] = dq_s[...].astype(F32).T.astype(BF16)

        @pl.when(i == 1)
        def _():
            rs_c[0] = o_s[...].astype(F32).T.astype(BF16)
            rs_c[1] = dq_s[...].astype(F32).T.astype(BF16)
            rc(OQ_SIB, rs_c, oqt.at[1], sib).start()
        return carry

    lax.fori_loop(0, 4, group, 0)

    start(RS_SIB, dkv_acc.at[:, rows(tp ^ 1), :], rs_a.at[0], sib)
    start(RS_SIB2, dkv_acc.at[:, rows(tp ^ 3), :], rs_a.at[1], sib)
    for r in range(8):
        cols = slice(r * 256, (r + 1) * 256)
        io_ref[:, cols] = (x_ref[:, cols].astype(F32) + out_acc[:, cols]).astype(BF16)
    put_out = local(8, io_ref, out_hbm)
    copies[RS_SIB].wait_recv()
    copies[RS_SIB2].wait_recv()

    def dkv_piece(part, b, blk):
        return dkv_ref.at[part, b, rows(blk), :]

    def reduce_kv(part, blk):
        for b in range(NB):
            total = dkv_acc[b, rows(blk), :] + rs_a[part, b]
            d_k = rope_back(total[:, KEY], cos_s[b, rows(blk), :], sin_s[b, rows(blk), :])
            dkv_ref[part, b, rows(blk), KEY] = d_k.astype(BF16)
            dkv_ref[part, b, rows(blk), VAL] = total[:, VAL].astype(BF16)
        for b in range(NB):
            piece = dkv_piece(part, b, blk)
            rc(DKV_X + 2 * part + b, piece, piece, xp).start()
            rc(DKV_SIB + 2 * part + b, piece, piece, sib).start()

    reduce_kv(0, tp)

    @pl.when(tp >= 2)
    def _():
        reduce_kv(1, tp ^ 2)
        dkv_ref[1, :, rows(tp), :] = jnp.zeros((NB, TB, 2 * HD), BF16)

    def weight_grads(first, o_t, dq_t, a_src, d_src):
        def tile(j, carry):
            cols = pl.ds(pl.multiple_of(j * 512, 512), 512)
            o_part = dot_nn(o_t[...], d_src[:, cols])
            q_part = dot_nn(dq_t[...], a_src[:, cols])
            if first:
                out_acc[:, cols] = o_part
                dwq_acc[:, cols] = q_part
            else:
                out_acc[:, cols] += o_part
                dwq_acc[:, cols] += q_part
            return carry
        lax.fori_loop(0, 4, tile, 0)

    copies[ACT_SIB].wait_recv()
    copies[DOUT_SIB].wait_recv()
    la = local(6, act_all.at[1], buf.at[0])
    ld = local(7, dout_all.at[1], buf.at[1])
    weight_grads(True, oqt.at[0, 0], oqt.at[0, 1], act, dout_ref)
    la.wait()
    ld.wait()
    rc(OQ_SIB, rs_c, oqt.at[1], sib).wait_recv()
    weight_grads(False, oqt.at[1, 0], oqt.at[1, 1], buf.at[0], buf.at[1])

    def head_part(t, carry):
        b = t // 2
        i = 2 + t % 2
        blk = tp ^ i
        r = pl.ds(pl.multiple_of(b * TB, TB), TB)

        def relay(c, whole):
            return rc(BULK_REL + 2 * b + c, whole.at[2, r, :], whole.at[3, r, :], sib)

        def load(k):
            half = pl.ds(k * TB, TB)
            return (pltpu.make_async_copy(act_all.at[2 + k, r, :], buf.at[0, half, :], lsem.at[6]),
                    pltpu.make_async_copy(dout_all.at[2 + k, r, :], buf.at[1, half, :], lsem.at[7]))

        @pl.when(i == 2)
        def _():
            for c, whole in ((0, dout_all), (1, act_all)):
                rc(BULK_X + 2 * b + c, whole.at[2, r, :], whole.at[2, r, :], xp).wait_recv()
                relay(c, whole).start()
            for cp in load(0):
                cp.start()

        cos_t = cos_s.at[b, rows(blk), :]
        sin_t = sin_s.at[b, rows(blk), :]
        trig_t[0] = cos_t[...].T
        trig_t[1] = sin_t[...].T
        half = pl.ds(pl.multiple_of((i - 2) * TB, TB), TB)
        for cp in load(0):
            cp.wait()

        def late_kv(blk):
            piece = kv_ref.at[b, rows(blk), :]
            return rc(KV_LATE + b, piece, piece, sib)

        @pl.when((i == 2) & (tp < 2))
        def _():
            kv = dot_nn(buf[0, 0:TB, :], wkv[...])
            kv_ref[b, rows(blk), KEY] = rope(kv[:, KEY].astype(BF16).astype(F32), cos_t[...], sin_t[...]).astype(BF16)
            kv_ref[b, rows(blk), VAL] = kv[:, VAL].astype(BF16)
            late_kv(tp ^ 2).start()

        project(TB, buf.at[0, half, :], buf.at[1, half, :], 0, lambda _: (cos_t[...], sin_t[...]))

        @pl.when(i == 2)
        def _():
            relay(0, dout_all).wait_recv()
            relay(1, act_all).wait_recv()
            for cp in load(1):
                cp.start()

        @pl.when((i == 2) & (tp < 2))
        def _():
            late_kv(tp ^ 3).wait_recv()
            transpose_kv(kv_ref, kt_ref, b, True)

        for n in range(1, 5):
            @pl.when(blk == n - 1)
            def _():
                def step(u, carry):
                    for j in range(2):
                        c = pl.ds(pl.multiple_of((u * 2 + j) * HD, HD), HD)
                        o_t, dq_t, _, _ = attend(n, q_s[0:TB, c], do_s[0:TB, c], kv_ref, b, kt_ref)
                        oqt[0, 0, c, half] = o_t.astype(BF16)
                        oqt[0, 1, c, half] = rope_back_t(dq_t * SCALE, trig_t[0], trig_t[1]).astype(BF16)
                    return carry
                lax.fori_loop(0, 2, step, 0)

        @pl.when(t == 1)
        def _():
            weight_grads(False, oqt.at[0, 0], oqt.at[0, 1], buf.at[0], buf.at[1])
            pltpu.make_async_copy(dwq_acc, accq_hbm, lsem.at[9]).start()
            pltpu.make_async_copy(out_acc, acco_hbm, lsem.at[10]).start()
        return carry

    lax.fori_loop(0, 4, head_part, 0)
    put_oqt = local(0, oqt.at[0], oqt_hbm)
    put_out.wait()

    dw_parts[0] = jnp.zeros((8, D), F32)
    gain = 1.0 + normw_ref[...]
    put_dkv = []

    for b in range(NB):
        def take(part, blk):
            piece = dkv_piece(part, b, blk)
            rc(DKV_X + 2 * part + b, piece, piece, xp).wait_recv()
            rc(DKV_REL + 2 * part + b, piece, piece, sib).start()

        take(0, tp ^ 2)

        @pl.when(tp < 2)
        def _():
            take(1, tp)

        def dx_rows(j, carry):
            r = pl.ds(pl.multiple_of(b * TB + j * 128, 128), 128)
            own = pl.ds(pl.multiple_of(tp * TB + j * 128, 128), 128)
            da = da_acc[r, :] + dot_nt(dkv_ref[0, b, own, :], wkv[...]) + dot_nt(dkv_ref[1, b, own, :], wkv[...])
            xf = x_ref[r, :].astype(F32)
            inv = lax.rsqrt(jnp.mean(xf * xf, axis=-1, keepdims=True) + 1e-6)
            normed = xf * inv
            prod = da * normed
            dw_parts[0] += jnp.sum(prod.reshape(16, 8, D), axis=0)
            corr = jnp.mean(prod * gain, axis=-1, keepdims=True)
            io_ref[r, :] = (dout_ref[r, :].astype(F32) + inv * (da * gain - normed * corr)).astype(BF16)
            return carry

        lax.fori_loop(0, 2, dx_rows, 0)
        if b == NB - 1:
            put_dx = local(8, io_ref, dx_hbm)
            start(DW_SIB, dw_parts.at[0], dw_parts.at[1], sib)
            start(DW_X, dw_parts.at[0], dw_parts.at[2], xp)
            start(DW_XS, dw_parts.at[0], dw_parts.at[3], xs)
        def arrived(first, part, blk):
            piece = dkv_piece(part, b, blk)
            rc(first + 2 * part + b, piece, piece, sib).wait_recv()

        arrived(DKV_SIB, 0, tp ^ 1)
        arrived(DKV_REL, 0, tp ^ 3)

        @pl.when(tp < 2)
        def _():
            arrived(DKV_REL, 1, tp ^ 1)

        @pl.when(tp >= 2)
        def _():
            arrived(DKV_SIB, 1, tp ^ 3)

        put_dkv.append(local(1 + b, dkv_ref.at[0, b], dkv_hbm.at[0, b]))
        put_dkv.append(local(3 + b, dkv_ref.at[1, b, 0:TOK, :], dkv_hbm.at[1, b, 0:TOK, :]))

    for i in (DW_SIB, DW_X, DW_XS):
        copies[i].wait_recv()
    parts = [dw_parts[jnp.bitwise_xor(tp, t)] for t in range(4)]
    dw_ref[...] = jnp.sum(sum(parts[1:], parts[0]), axis=0, keepdims=True)

    own_a.wait()
    own_d.wait()
    for cp in (put_oqt, put_dx, *put_dkv):
        cp.wait()
    pltpu.make_async_copy(dwq_acc, accq_hbm, lsem.at[9]).wait()
    pltpu.make_async_copy(out_acc, acco_hbm, lsem.at[10]).wait()
    for i in copies:
        copies[i].wait_send()
    rc(OQ_SIB, rs_c, oqt.at[1], sib).wait_send()
    for b in range(NB):
        piece = dkv_piece(0, b, tp)
        for i in (DKV_X, DKV_SIB, DKV_REL):
            rc(i + b, piece, piece, sib).wait_send()

        @pl.when(tp < 2)
        def _():
            rc(DKV_REL + 2 + b, piece, piece, sib).wait_send()
            rc(KV_LATE + b, piece, piece, sib).wait_send()

        @pl.when(tp >= 2)
        def _():
            rc(DKV_X + 2 + b, piece, piece, sib).wait_send()
            rc(DKV_SIB + 2 + b, piece, piece, sib).wait_send()

    @pl.when(tp < 2)
    def _():
        rc(KV_X, own_kv, own_kv, xp).wait_send()

    @pl.when(tp >= 2)
    def _():
        rc(KV_REL, own_kv, own_kv, sib).wait_send()

    for c in range(4):
        bulk(c).wait_send()
        whole = act_all if c % 2 else dout_all
        r = slice((c // 2) * TB, (c // 2 + 1) * TB)
        rc(BULK_REL + c, whole.at[2, r, :], whole.at[3, r, :], sib).wait_send()
    for which, first in ((0, WQ_X), (1, WO_X)):
        for j in range(1, 8):
            rc(first + j, quarter(which, 2, j % 4), quarter(which, 2, j % 4), sib).wait_send()


def grad_kernel(accq_ref, acco_ref, act_ref, dout_ref, oqt_ref, dkv_ref, out_in, dx_in,
                dwq_ref, dwo_ref, dwk_ref, dwv_ref, out_ref, dx_ref, dkvt):
    tp = lax.axis_index('tp')
    out_ref[...] = out_in[...]
    dx_ref[...] = dx_in[...]

    @pl.when(pl.program_id(0) == 0)
    def _():
        for t in range(6):
            for b in range(NB):
                piece = dkv_ref[t // 4, b, (t % 4) * TB:(t % 4 + 1) * TB, :]
                dkvt[t, :, b * TB:(b + 1) * TB] = piece.astype(F32).T.astype(BF16)

    a = jnp.concatenate([act_ref[2, TB:TOK, :], act_ref[3, TB:TOK, :]], axis=0)
    d = dout_ref[...].reshape(TOK, -1)
    dwo_ref[...] = acco_ref[...] + dot_nn(oqt_ref[0], d)
    dwq_ref[...] = (accq_ref[...] + dot_nn(oqt_ref[1], a)).T
    total = dot_nn(dkvt[0], act_ref[jnp.bitwise_xor(tp, 0)])
    for t in range(1, 6):
        total += dot_nn(dkvt[t], act_ref[jnp.bitwise_xor(tp, t % 4)])
    dwk_ref[...] = total[KEY].T
    dwv_ref[...] = total[VAL].T


def local_block(hidden, positions, norm_w, w_query, w_key, w_value, w_out, grad_out):
    x = hidden.reshape(TOK, D)
    dout = grad_out.reshape(TOK, D)
    freq = 10000.0 ** (-2.0 * (np.arange(HD) % (HD // 2)) / HD)

    vmem = pl.BlockSpec(memory_space=pltpu.VMEM)
    anym = pl.BlockSpec(memory_space=pl.ANY)
    sds = jax.ShapeDtypeStruct
    out, dx, dw, accq, acco, oqt, dkv, act_all, dout_all = pl.pallas_call(
        main_kernel,
        out_shape=[sds((TOK, D), BF16), sds((TOK, D), BF16), sds((1, D), F32), sds((HW, D), F32), sds((HW, D), F32),
                   sds((2, HW, TOK), BF16), sds((2, NB, SEQ, 2 * HD), BF16), sds((4, TOK, D), BF16), sds((4, TOK, D), BF16)],
        in_specs=[anym, anym, anym, anym, anym, anym, vmem, vmem, vmem],
        out_specs=[anym, anym, vmem, anym, anym, anym, anym, anym, anym],
        scratch_shapes=[
            pltpu.VMEM((TOK, D), BF16), pltpu.VMEM((TOK, D), BF16), pltpu.VMEM((TOK, D), BF16),
            pltpu.VMEM((2, NB, SEQ, 2 * HD), BF16),
            pltpu.VMEM((2, 2, HW, TOK), BF16),
            pltpu.VMEM((2, HD, TB), F32),
            pltpu.VMEM((HW, D), F32),
            pltpu.VMEM((TOK, D), BF16),
            pltpu.VMEM((NB, SEQ, 2 * HD), BF16),
            pltpu.VMEM((D, 2 * HD), BF16),
            pltpu.VMEM((NB, SEQ, HD), F32), pltpu.VMEM((NB, SEQ, HD), F32),
            pltpu.VMEM((4, D, HW), BF16), pltpu.VMEM((4, HW, D), BF16),
            pltpu.VMEM((TOK, HW), BF16), pltpu.VMEM((TOK, HW), BF16),
            pltpu.VMEM((TOK, HW), BF16), pltpu.VMEM((TOK, HW), BF16),
            pltpu.VMEM((TOK, D), F32), pltpu.VMEM((TOK, D), F32),
            pltpu.VMEM((NB, 2 * HD, SEQ), BF16),
            pltpu.VMEM((NB, SEQ, 2 * HD), F32),
            pltpu.VMEM((2, NB, TB, 2 * HD), F32),
            pltpu.VMEM((2, HW, TOK), BF16),
            pltpu.VMEM((4, 8, D), F32),
            pltpu.VMEM((2, TOK, D), BF16),
            pltpu.SemaphoreType.DMA((N_SEM,)), pltpu.SemaphoreType.DMA((N_SEM,)), pltpu.SemaphoreType.DMA((11,)),
        ],
        compiler_params=pltpu.CompilerParams(collective_id=0, has_side_effects=True, vmem_limit_bytes=67_000_000),
        name='main',
    )(x, dout, w_query, w_out, w_key, w_value, norm_w[None, :], positions, jnp.asarray(freq[None, :], F32))

    whole = lambda s: pl.BlockSpec(s, lambda t: (0,) * len(s))
    steps = 4
    cols = D // steps
    by_row = lambda r, c: pl.BlockSpec((r, c), lambda t: (t, 0))
    by_col = pl.BlockSpec((HW, cols), lambda t: (0, t))
    dwq, dwo, dwk, dwv, out, dx = pl.pallas_call(
        grad_kernel,
        grid=(steps,),
        out_shape=[sds((D, HW), F32), sds((HW, D), F32), sds((D, HD), F32), sds((D, HD), F32), sds((TOK, D), BF16), sds((TOK, D), BF16)],
        in_specs=[by_col, by_col, pl.BlockSpec((4, TOK, cols), lambda t: (0, 0, t)), pl.BlockSpec((2, TB, cols), lambda t: (1, 1, t)),
                  whole((2, HW, TOK)), whole((2, NB, SEQ, 2 * HD)), by_row(TOK // steps, D), by_row(TOK // steps, D)],
        out_specs=[by_row(cols, HW), by_col, by_row(cols, HD), by_row(cols, HD), by_row(TOK // steps, D), by_row(TOK // steps, D)],
        scratch_shapes=[pltpu.VMEM((6, 2 * HD, TOK), BF16)],
        compiler_params=pltpu.CompilerParams(vmem_limit_bytes=64_000_000),
        name='grads',
    )(accq, acco, act_all, dout_all, oqt, dkv, out, dx)

    return out.reshape(NB, TB, D), dx.reshape(NB, TB, D), dwq, dwo, dwk, dwv, dw.reshape(D)


def solution(mesh):
    specs_in = (P('dp', 'tp'), P('dp'), P(), P(None, 'tp'), P(), P(), P('tp'), P('dp', 'tp'))
    specs_out = (P('dp', 'tp'), P('dp', 'tp'), P('dp', 'tp'), P(('dp', 'tp')), P('dp'), P('dp'), P('dp'))
    return jax.shard_map(local_block, mesh=mesh, in_specs=specs_in, out_specs=specs_out, check_vma=False)
```

```python
import jax
import jax.numpy as jnp
import numpy as np
from jax import lax
from jax.experimental import pallas as pl
from jax.experimental.pallas import tpu as pltpu
from jax.sharding import PartitionSpec as P

F32 = jnp.float32
BF16 = jnp.bfloat16
MESH = pl.DeviceIdType.MESH

TB = 256
NB = 2
TOK = TB * NB
SEQ = 1024
D = 2048
HD = 128
HL = 4
HW = HD * HL
SCALE = HD ** -0.5

N_SEM = 51
(WQ_X, _, _, _, WQ_REL, _, _, _, WQ_SIB,
 WO_X, _, _, _, WO_REL, _, _, _, WO_SIB,
 KV_X, KV_SIB, KV_REL, KV_LATE, _,
 BULK_X, _, _, _, BULK_REL, _, _, _,
 DOUT_SIB, ACT_SIB, RS_SIB, RS_SIB2, OQ_SIB, DW_SIB, DW_X, DW_XS,
 DKV_X, _, _, _, DKV_SIB, _, _, _, DKV_REL, _, _, _) = range(N_SEM)
KEY = slice(HD)
VAL = slice(HD, 2 * HD)


def dot_nn(a, b):
    return jnp.dot(a, b, preferred_element_type=F32)


def dot_nt(a, b):
    return lax.dot_general(a, b, (((1,), (1,)), ((), ())), preferred_element_type=F32)


def dot_tn(a, b):
    return lax.dot_general(a, b, (((0,), (0,)), ((), ())), preferred_element_type=F32)


def rope(u, cos_t, sin_t):
    return u * cos_t + pltpu.roll(u, HD // 2, 1) * sin_t


def rope_back(u, cos_t, sin_t):
    return u * cos_t - pltpu.roll(u, HD // 2, 1) * sin_t


def rope_back_t(u, cos_t, sin_t):
    swapped = jnp.concatenate([u[HD // 2:], u[:HD // 2]], axis=0)
    return u * cos_t - swapped * sin_t


def attend(n, q, do, k_ref, b, kt_ref):
    keys = n * TB
    k = k_ref[b, 0:keys, KEY]
    v = k_ref[b, 0:keys, VAL]
    s = dot_nt(k, q)
    row = lax.broadcasted_iota(jnp.int32, (TB, TB), 0)
    col = lax.broadcasted_iota(jnp.int32, (TB, TB), 1)
    last = jnp.where(row <= col, s[keys - TB:], -1e30)
    s = last if n == 1 else jnp.concatenate([s[:keys - TB], last], axis=0)
    e = jnp.exp(s - jnp.max(s, axis=0, keepdims=True))
    p = e * (1.0 / jnp.sum(e, axis=0, keepdims=True))
    p_low = p.astype(BF16)
    dp = dot_nt(v, do)
    ds = (p * (dp - jnp.sum(p * dp, axis=0, keepdims=True))).astype(BF16)
    o_t = dot_nn(kt_ref[b, VAL, 0:keys], p_low)
    dq_t = dot_nn(kt_ref[b, KEY, 0:keys], ds)
    return o_t, dq_t, p_low, ds


def transpose_kv(kv_ref, kt_ref, b, later):
    for j in range(2):
        r = pl.ds(pl.multiple_of((2 * later + j) * TB, TB), TB)
        kt_ref[b, :, r] = kv_ref[b, r, :].astype(F32).T.astype(BF16)


def main_kernel(x_hbm, dout_hbm, wq_own, wo_own, wk_own, wv_own, normw_ref, pos_ref, freq_ref,
                out_hbm, dx_hbm, dw_ref, accq_hbm, acco_hbm, oqt_hbm, dkv_hbm, act_all, dout_all,
                x_ref, dout_ref, io_ref, dkv_ref, oqt, trig_t, dwq_acc,
                act, kv_ref, wkv, cos_s, sin_s, wq_buf, wo_buf, q_s, do_s, o_s, dq_s, out_acc, da_acc, kt_ref,
                dkv_acc, rs_a, rs_c, dw_acc, dw_parts, buf, send, recv, lsem):
    dp = lax.axis_index('dp')
    tp = lax.axis_index('tp')
    sib = (dp, tp ^ 1)
    xp = (dp, tp ^ 2)
    xs = (dp, tp ^ 3)
    yp = (dp ^ 1, tp)
    zp = (dp ^ 2, tp)
    yzp = (dp ^ 3, tp)

    def rc(i, src, dst, dev):
        return pltpu.make_async_remote_copy(src_ref=src, dst_ref=dst, send_sem=send.at[i], recv_sem=recv.at[i],
                                            device_id=dev, device_id_type=MESH)

    def quarter(which, shard, j):
        size = 512 if which == 0 else 128
        r = pl.ds(pl.multiple_of((dp ^ j) * size, size), size)
        if shard is None:
            return (wq_own, wo_own)[which].at[r, :]
        return (wq_buf, wo_buf)[which].at[shard, r, :]

    def rows(blk):
        return pl.ds(pl.multiple_of(blk * TB, TB), TB)

    copies = {}

    def start(i, src, dst, dev):
        copies[i] = rc(i, src, dst, dev)
        copies[i].start()

    def local(i, src, dst):
        cp = pltpu.make_async_copy(src, dst, lsem.at[i])
        cp.start()
        return cp

    def spread(which):
        first = (WQ_X, WO_X)[which]
        mine = quarter(which, 2, 0)
        rc(first, quarter(which, None, 0), mine, xp).wait_recv()
        for j, dev in ((1, yp), (2, zp), (3, yzp)):
            rc(first + j, mine, mine, dev).start()
        rc(first + 4, mine, quarter(which, 3, 0), sib).start()

    def bulk(c):
        r = pl.ds((c // 2) * TB, TB)
        src, dst = (act, act_all) if c % 2 else (dout_hbm, dout_all)
        return rc(BULK_X + c, src.at[r, :], dst.at[2, r, :], xp)

    load_x = local(8, x_hbm, x_ref)
    load_k = local(0, wk_own, wkv.at[:, KEY])
    load_v = local(1, wv_own, wkv.at[:, VAL])
    load_q = local(2, wq_own, wq_buf.at[0])
    load_o = local(3, wo_own, wo_buf.at[0])
    load_d = local(4, dout_hbm, dout_ref)

    barrier = pltpu.get_barrier_semaphore()
    for dev in (sib, xp, xs, yp, zp, yzp):
        pl.semaphore_signal(barrier, inc=1, device_id=dev, device_id_type=MESH)
    pl.semaphore_wait(barrier, 6)

    start(WQ_X, quarter(0, None, 0), quarter(0, 2, 0), xp)
    start(WQ_SIB, wq_own, wq_buf.at[1], sib)
    start(WO_SIB, wo_own, wo_buf.at[1], sib)
    start(DOUT_SIB, dout_hbm, dout_all.at[1], sib)
    load_x.wait()

    def norm_rows(j, carry):
        r = pl.ds(pl.multiple_of(j * 64, 64), 64)
        xf = x_ref[r, :].astype(F32)
        inv = lax.rsqrt(jnp.mean(xf * xf, axis=-1, keepdims=True) + 1e-6)
        act[r, :] = (xf * inv * (1.0 + normw_ref[...])).astype(BF16)
        return carry

    lax.fori_loop(0, TOK // 64, norm_rows, 0)
    lane = lax.broadcasted_iota(jnp.int32, (HD, HD), 1)

    def tables(blk):
        for b in range(NB):
            for h in range(TB // HD):
                pos = pos_ref[b:b + 1, pl.ds(pl.multiple_of(blk * TB + h * HD, HD), HD)].astype(F32)
                angle = jnp.broadcast_to(pos, (HD, HD)).T * freq_ref[...]
                r = pl.ds(pl.multiple_of(blk * TB + h * HD, HD), HD)
                sin_t = jnp.sin(angle)
                cos_s[b, r, :] = jnp.cos(angle)
                sin_s[b, r, :] = jnp.where(lane < HD // 2, -sin_t, sin_t)

    tables(tp)
    load_k.wait()
    load_v.wait()
    kv = dot_nn(act[...], wkv[...])
    for b in range(NB):
        r = slice(b * TB, (b + 1) * TB)
        k_rot = rope(kv[r, KEY].astype(BF16).astype(F32), cos_s[b, rows(tp), :], sin_s[b, rows(tp), :])
        kv_ref[b, rows(tp), KEY] = k_rot.astype(BF16)
        kv_ref[b, rows(tp), VAL] = kv[r, VAL].astype(BF16)
    own_kv = kv_ref.at[:, rows(tp), :]

    @pl.when(tp < 2)
    def _():
        rc(KV_X, own_kv, own_kv, xp).start()

    start(KV_SIB, own_kv, own_kv, sib)
    start(WO_X, quarter(1, None, 0), quarter(1, 2, 0), xp)
    bulk(0).start()
    start(ACT_SIB, act, act_all.at[1], sib)
    own_a = local(5, act, act_all.at[0])

    out_acc[...] = jnp.zeros_like(out_acc)
    da_acc[...] = jnp.zeros_like(da_acc)
    dkv_acc[...] = jnp.zeros_like(dkv_acc)

    def project(n_rows, a_src, slot, table):
        def pair(j, carry):
            cols = pl.ds(pl.multiple_of(j * 2 * HD, 2 * HD), 2 * HD)
            q = dot_nn(a_src[0:n_rows, :], wq_buf[slot, :, cols]).astype(BF16).astype(F32)
            for t in range(n_rows // TB):
                r = slice(t * TB, (t + 1) * TB)
                cos_t, sin_t = table(t)
                for h in range(2):
                    piece = rope(q[r, h * HD:(h + 1) * HD], cos_t, sin_t) * SCALE
                    q_s[r, pl.ds(pl.multiple_of((2 * j + h) * HD, HD), HD)] = piece.astype(BF16)
            return carry
        lax.fori_loop(0, HL // 2, pair, 0)

    def project_back(d_src, slot, dst):
        def pair(j, carry):
            cols = pl.ds(pl.multiple_of(j * 2 * HD, 2 * HD), 2 * HD)
            dst[:, cols] = dot_nt(d_src[...], wo_buf[slot, cols, :]).astype(BF16)
            return carry
        lax.fori_loop(0, HL // 2, pair, 0)

    def project_own(slot):
        project(TOK, act, slot, lambda b: (cos_s[b, rows(tp), :], sin_s[b, rows(tp), :]))
        project_back(dout_ref, slot, do_s)

    def attend_group():
        for n in range(1, 5):
            @pl.when(tp == n - 1)
            def _():
                def step(t, carry):
                    b = t // 2
                    r = pl.ds(pl.multiple_of(b * TB, TB), TB)
                    cos_t = cos_s[b, rows(tp), :]
                    sin_t = sin_s[b, rows(tp), :]
                    for j in range(2):
                        c = pl.ds(pl.multiple_of(((t % 2) * 2 + j) * HD, HD), HD)
                        q = q_s[r, c]
                        do = do_s[r, c]
                        o_t, dq_t, p_low, ds = attend(n, q, do, kv_ref, b, kt_ref)
                        o_s[r, c] = o_t.T.astype(BF16)
                        dq_s[r, c] = rope_back(dq_t.T * SCALE, cos_t, sin_t).astype(BF16)
                        dkv_acc[b, 0:n * TB, KEY] += dot_nn(ds, q)
                        dkv_acc[b, 0:n * TB, VAL] += dot_nn(p_low, do)
                    return carry
                lax.fori_loop(0, 4, step, 0)

    def accumulate(slot):
        def tile(j, carry):
            cols = pl.ds(pl.multiple_of(j * 512, 512), 512)
            out_acc[:, cols] += dot_nn(o_s[...], wo_buf[slot, :, cols])
            da_acc[:, cols] += dot_nt(dq_s[...], wq_buf[slot, cols, :])
            return carry
        lax.fori_loop(0, 4, tile, 0)

    load_q.wait()
    load_o.wait()
    load_d.wait()
    own_d = local(4, dout_ref, dout_all.at[0])
    project_own(0)
    tables(tp ^ 2)
    tables(tp ^ 3)
    spread(0)
    other_kv = kv_ref.at[:, rows(tp ^ 2), :]

    @pl.when(tp >= 2)
    def _():
        rc(KV_X, other_kv, other_kv, xp).wait_recv()
        rc(KV_REL, other_kv, other_kv, sib).start()

    copies[KV_SIB].wait_recv()
    for b in range(NB):
        transpose_kv(kv_ref, kt_ref, b, tp // 2)

    @pl.when(tp >= 2)
    def _():
        sib_kv = kv_ref.at[:, rows(tp ^ 3), :]
        rc(KV_REL, sib_kv, sib_kv, sib).wait_recv()
        for b in range(NB):
            transpose_kv(kv_ref, kt_ref, b, False)

    def group(i, carry):
        @pl.when(i == 1)
        def _():
            rc(WQ_SIB, wq_own, wq_buf.at[1], sib).wait_recv()
            rc(WO_SIB, wo_own, wo_buf.at[1], sib).wait_recv()

        @pl.when(i == 2)
        def _():
            for which, first in ((0, WQ_X), (1, WO_X)):
                for j in (1, 2, 3):
                    piece = quarter(which, 2, j)
                    rc(first + j, piece, piece, sib).wait_recv()
                    rc(first + 4 + j, piece, quarter(which, 3, j), sib).start()

        @pl.when(i == 3)
        def _():
            for which, rel in ((0, WQ_REL), (1, WO_REL)):
                for j in range(4):
                    rc(rel + j, quarter(which, 2, j), quarter(which, 3, j), sib).wait_recv()

        @pl.when(i > 0)
        def _():
            project_own(i)

        attend_group()

        @pl.when(i == 0)
        def _():
            spread(1)
            for c in (1, 2, 3):
                bulk(c).start()

        accumulate(i)

        @pl.when(i == 0)
        def _():
            oqt[0, 0] = o_s[...].astype(F32).T.astype(BF16)
            oqt[0, 1] = dq_s[...].astype(F32).T.astype(BF16)

        @pl.when(i == 1)
        def _():
            rs_c[0] = o_s[...].astype(F32).T.astype(BF16)
            rs_c[1] = dq_s[...].astype(F32).T.astype(BF16)
            rc(OQ_SIB, rs_c, oqt.at[1], sib).start()
        return carry

    lax.fori_loop(0, 4, group, 0)

    start(RS_SIB, dkv_acc.at[:, rows(tp ^ 1), :], rs_a.at[0], sib)
    start(RS_SIB2, dkv_acc.at[:, rows(tp ^ 3), :], rs_a.at[1], sib)
    for r in range(8):
        cols = slice(r * 256, (r + 1) * 256)
        io_ref[:, cols] = (x_ref[:, cols].astype(F32) + out_acc[:, cols]).astype(BF16)
    put_out = local(8, io_ref, out_hbm)
    copies[RS_SIB].wait_recv()
    copies[RS_SIB2].wait_recv()

    def dkv_piece(part, b, blk):
        return dkv_ref.at[part, b, rows(blk), :]

    def reduce_kv(part, blk):
        for b in range(NB):
            total = dkv_acc[b, rows(blk), :] + rs_a[part, b]
            d_k = rope_back(total[:, KEY], cos_s[b, rows(blk), :], sin_s[b, rows(blk), :])
            dkv_ref[part, b, rows(blk), KEY] = d_k.astype(BF16)
            dkv_ref[part, b, rows(blk), VAL] = total[:, VAL].astype(BF16)
        for b in range(NB):
            piece = dkv_piece(part, b, blk)
            rc(DKV_X + 2 * part + b, piece, piece, xp).start()
            rc(DKV_SIB + 2 * part + b, piece, piece, sib).start()

    reduce_kv(0, tp)

    @pl.when(tp >= 2)
    def _():
        reduce_kv(1, tp ^ 2)
        dkv_ref[1, :, rows(tp), :] = jnp.zeros((NB, TB, 2 * HD), BF16)

    def weight_grads(first, o_t, dq_t, a_src, d_src):
        def tile(j, carry):
            cols = pl.ds(pl.multiple_of(j * 512, 512), 512)
            o_part = dot_nn(o_t[...], d_src[:, cols])
            q_part = dot_nn(dq_t[...], a_src[:, cols])
            if first:
                out_acc[:, cols] = o_part
                dwq_acc[:, cols] = q_part
            else:
                out_acc[:, cols] += o_part
                dwq_acc[:, cols] += q_part
            return carry
        lax.fori_loop(0, 4, tile, 0)

    copies[ACT_SIB].wait_recv()
    copies[DOUT_SIB].wait_recv()
    la = local(6, act_all.at[1], buf.at[0])
    ld = local(7, dout_all.at[1], buf.at[1])
    weight_grads(True, oqt.at[0, 0], oqt.at[0, 1], act, dout_ref)
    la.wait()
    ld.wait()
    rc(OQ_SIB, rs_c, oqt.at[1], sib).wait_recv()
    weight_grads(False, oqt.at[1, 0], oqt.at[1, 1], buf.at[0], buf.at[1])

    def head_part(t, carry):
        b = t // 2
        i = 2 + t % 2
        blk = tp ^ i
        r = pl.ds(pl.multiple_of(b * TB, TB), TB)

        def move(c, k):
            whole = (dout_all, act_all)[c]
            return (lambda: rc(BULK_X + 2 * b + c, whole.at[2, r, :], whole.at[2, r, :], xp),
                    lambda: rc(BULK_REL + 2 * b + c, whole.at[2, r, :], whole.at[3, r, :], sib),
                    lambda: pltpu.make_async_copy(whole.at[2 + k, r, :], buf.at[1 - c, pl.ds(k * TB, TB), :], lsem.at[7 - c]))

        def receive(c):
            over_x, relay, load = move(c, 0)
            over_x().wait_recv()
            relay().start()
            load().start()

        def receive_sibling(c):
            _, relay, load = move(c, 1)
            relay().wait_recv()
            load().start()

        half = pl.ds(pl.multiple_of((i - 2) * TB, TB), TB)

        @pl.when(i == 2)
        def _():
            receive(0)
            move(0, 0)[-1]().wait()
            receive_sibling(0)
            project_back(buf.at[1, 0:TB, :], 0, do_s.at[0:TB, :])
            move(0, 1)[-1]().wait()
            project_back(buf.at[1, TB:TOK, :], 0, do_s.at[TB:TOK, :])
            receive(1)

        cos_t = cos_s.at[b, rows(blk), :]
        sin_t = sin_s.at[b, rows(blk), :]
        trig_t[0] = cos_t[...].T
        trig_t[1] = sin_t[...].T
        move(1, 0)[-1]().wait()

        def late_kv(blk):
            piece = kv_ref.at[b, rows(blk), :]
            return rc(KV_LATE + b, piece, piece, sib)

        @pl.when((i == 2) & (tp < 2))
        def _():
            kv = dot_nn(buf[0, 0:TB, :], wkv[...])
            kv_ref[b, rows(blk), KEY] = rope(kv[:, KEY].astype(BF16).astype(F32), cos_t[...], sin_t[...]).astype(BF16)
            kv_ref[b, rows(blk), VAL] = kv[:, VAL].astype(BF16)
            late_kv(tp ^ 2).start()

        project(TB, buf.at[0, half, :], 0, lambda _: (cos_t[...], sin_t[...]))

        @pl.when(i == 2)
        def _():
            receive_sibling(1)

        @pl.when((i == 2) & (tp < 2))
        def _():
            late_kv(tp ^ 3).wait_recv()
            transpose_kv(kv_ref, kt_ref, b, True)

        for n in range(1, 5):
            @pl.when(blk == n - 1)
            def _():
                def step(u, carry):
                    for j in range(2):
                        c = pl.ds(pl.multiple_of((u * 2 + j) * HD, HD), HD)
                        o_t, dq_t, _, _ = attend(n, q_s[0:TB, c], do_s[half, c], kv_ref, b, kt_ref)
                        oqt[0, 0, c, half] = o_t.astype(BF16)
                        oqt[0, 1, c, half] = rope_back_t(dq_t * SCALE, trig_t[0], trig_t[1]).astype(BF16)
                    return carry
                lax.fori_loop(0, 2, step, 0)

        @pl.when(t == 1)
        def _():
            weight_grads(False, oqt.at[0, 0], oqt.at[0, 1], buf.at[0], buf.at[1])
            pltpu.make_async_copy(dwq_acc, accq_hbm, lsem.at[9]).start()
            pltpu.make_async_copy(out_acc, acco_hbm, lsem.at[10]).start()
        return carry

    lax.fori_loop(0, 4, head_part, 0)
    put_oqt = local(0, oqt.at[0], oqt_hbm)
    put_out.wait()

    dw_acc[...] = jnp.zeros_like(dw_acc)
    gain = 1.0 + normw_ref[...]
    put_dkv = []

    for b in range(NB):
        def take(part, blk):
            piece = dkv_piece(part, b, blk)
            rc(DKV_X + 2 * part + b, piece, piece, xp).wait_recv()
            rc(DKV_REL + 2 * part + b, piece, piece, sib).start()

        take(0, tp ^ 2)

        @pl.when(tp < 2)
        def _():
            take(1, tp)

        def dx_rows(j, carry):
            r = pl.ds(pl.multiple_of(b * TB + j * 128, 128), 128)
            own = pl.ds(pl.multiple_of(tp * TB + j * 128, 128), 128)
            da = da_acc[r, :] + dot_nt(dkv_ref[0, b, own, :], wkv[...]) + dot_nt(dkv_ref[1, b, own, :], wkv[...])
            xf = x_ref[r, :].astype(F32)
            inv = lax.rsqrt(jnp.mean(xf * xf, axis=-1, keepdims=True) + 1e-6)
            normed = xf * inv
            prod = da * normed
            dw_acc[...] += jnp.sum(prod.reshape(-1, *dw_acc.shape), axis=0)
            corr = jnp.mean(prod * gain, axis=-1, keepdims=True)
            io_ref[r, :] = (dout_ref[r, :].astype(F32) + inv * (da * gain - normed * corr)).astype(BF16)
            return carry

        lax.fori_loop(0, 2, dx_rows, 0)
        if b == NB - 1:
            dw_parts[0] = jnp.sum(dw_acc[...], axis=0, keepdims=True)
            put_dx = local(8, io_ref, dx_hbm)
            start(DW_SIB, dw_parts.at[0], dw_parts.at[1], sib)
            start(DW_X, dw_parts.at[0], dw_parts.at[2], xp)
            start(DW_XS, dw_parts.at[0], dw_parts.at[3], xs)
        def arrived(first, part, blk):
            piece = dkv_piece(part, b, blk)
            rc(first + 2 * part + b, piece, piece, sib).wait_recv()

        arrived(DKV_SIB, 0, tp ^ 1)
        arrived(DKV_REL, 0, tp ^ 3)

        @pl.when(tp < 2)
        def _():
            arrived(DKV_REL, 1, tp ^ 1)

        @pl.when(tp >= 2)
        def _():
            arrived(DKV_SIB, 1, tp ^ 3)

        put_dkv.append(local(1 + b, dkv_ref.at[0, b], dkv_hbm.at[0, b]))
        put_dkv.append(local(3 + b, dkv_ref.at[1, b, 0:TOK, :], dkv_hbm.at[1, b, 0:TOK, :]))

    for i in (DW_SIB, DW_X, DW_XS):
        copies[i].wait_recv()
    parts = [dw_parts[jnp.bitwise_xor(tp, t)] for t in range(4)]
    dw_ref[...] = sum(parts[1:], parts[0])

    own_a.wait()
    own_d.wait()
    for cp in (put_oqt, put_dx, *put_dkv):
        cp.wait()
    pltpu.make_async_copy(dwq_acc, accq_hbm, lsem.at[9]).wait()
    pltpu.make_async_copy(out_acc, acco_hbm, lsem.at[10]).wait()
    for i in copies:
        copies[i].wait_send()
    rc(OQ_SIB, rs_c, oqt.at[1], sib).wait_send()
    for b in range(NB):
        piece = dkv_piece(0, b, tp)
        for i in (DKV_X, DKV_SIB, DKV_REL):
            rc(i + b, piece, piece, sib).wait_send()

        @pl.when(tp < 2)
        def _():
            rc(DKV_REL + 2 + b, piece, piece, sib).wait_send()
            rc(KV_LATE + b, piece, piece, sib).wait_send()

        @pl.when(tp >= 2)
        def _():
            rc(DKV_X + 2 + b, piece, piece, sib).wait_send()
            rc(DKV_SIB + 2 + b, piece, piece, sib).wait_send()

    @pl.when(tp < 2)
    def _():
        rc(KV_X, own_kv, own_kv, xp).wait_send()

    @pl.when(tp >= 2)
    def _():
        rc(KV_REL, own_kv, own_kv, sib).wait_send()

    for c in range(4):
        bulk(c).wait_send()
        whole = act_all if c % 2 else dout_all
        r = slice((c // 2) * TB, (c // 2 + 1) * TB)
        rc(BULK_REL + c, whole.at[2, r, :], whole.at[3, r, :], sib).wait_send()
    for which, first in ((0, WQ_X), (1, WO_X)):
        for j in range(1, 8):
            rc(first + j, quarter(which, 2, j % 4), quarter(which, 2, j % 4), sib).wait_send()


def grad_kernel(accq_ref, acco_ref, act_ref, dout_ref, oqt_ref, dkv_ref, out_in, dx_in, dw_in,
                dwq_ref, dwo_ref, dwk_ref, dwv_ref, out_ref, dx_ref, dw_ref, dkvt):
    tp = lax.axis_index('tp')
    out_ref[...] = out_in[...]
    dx_ref[...] = dx_in[...]
    dw_ref[...] = dw_in[...]

    @pl.when(pl.program_id(0) == 0)
    def _():
        for t in range(6):
            for b in range(NB):
                piece = dkv_ref[t // 4, b, (t % 4) * TB:(t % 4 + 1) * TB, :]
                dkvt[t, :, b * TB:(b + 1) * TB] = piece.astype(F32).T.astype(BF16)

    a = jnp.concatenate([act_ref[2, TB:TOK, :], act_ref[3, TB:TOK, :]], axis=0)
    d = dout_ref[...].reshape(TOK, -1)
    dwo_ref[...] = acco_ref[...] + dot_nn(oqt_ref[0], d)
    dwq_ref[...] = (accq_ref[...] + dot_nn(oqt_ref[1], a)).T
    total = dot_nn(dkvt[0], act_ref[jnp.bitwise_xor(tp, 0)])
    for t in range(1, 6):
        total += dot_nn(dkvt[t], act_ref[jnp.bitwise_xor(tp, t % 4)])
    dwk_ref[...] = total[KEY].T
    dwv_ref[...] = total[VAL].T


def local_block(hidden, positions, norm_w, w_query, w_key, w_value, w_out, grad_out):
    x = hidden.reshape(TOK, D)
    dout = grad_out.reshape(TOK, D)
    freq = 10000.0 ** (-2.0 * (np.arange(HD) % (HD // 2)) / HD)

    vmem = pl.BlockSpec(memory_space=pltpu.VMEM)
    anym = pl.BlockSpec(memory_space=pl.ANY)
    sds = jax.ShapeDtypeStruct
    out, dx, dw, accq, acco, oqt, dkv, act_all, dout_all = pl.pallas_call(
        main_kernel,
        out_shape=[sds((TOK, D), BF16), sds((TOK, D), BF16), sds((1, D), F32), sds((HW, D), F32), sds((HW, D), F32),
                   sds((2, HW, TOK), BF16), sds((2, NB, SEQ, 2 * HD), BF16), sds((4, TOK, D), BF16), sds((4, TOK, D), BF16)],
        in_specs=[anym, anym, anym, anym, anym, anym, vmem, vmem, vmem],
        out_specs=[anym, anym, vmem, anym, anym, anym, anym, anym, anym],
        scratch_shapes=[
            pltpu.VMEM((TOK, D), BF16), pltpu.VMEM((TOK, D), BF16), pltpu.VMEM((TOK, D), BF16),
            pltpu.VMEM((2, NB, SEQ, 2 * HD), BF16),
            pltpu.VMEM((2, 2, HW, TOK), BF16),
            pltpu.VMEM((2, HD, TB), F32),
            pltpu.VMEM((HW, D), F32),
            pltpu.VMEM((TOK, D), BF16),
            pltpu.VMEM((NB, SEQ, 2 * HD), BF16),
            pltpu.VMEM((D, 2 * HD), BF16),
            pltpu.VMEM((NB, SEQ, HD), F32), pltpu.VMEM((NB, SEQ, HD), F32),
            pltpu.VMEM((4, D, HW), BF16), pltpu.VMEM((4, HW, D), BF16),
            pltpu.VMEM((TOK, HW), BF16), pltpu.VMEM((TOK, HW), BF16),
            pltpu.VMEM((TOK, HW), BF16), pltpu.VMEM((TOK, HW), BF16),
            pltpu.VMEM((TOK, D), F32), pltpu.VMEM((TOK, D), F32),
            pltpu.VMEM((NB, 2 * HD, SEQ), BF16),
            pltpu.VMEM((NB, SEQ, 2 * HD), F32),
            pltpu.VMEM((2, NB, TB, 2 * HD), F32),
            pltpu.VMEM((2, HW, TOK), BF16),
            pltpu.VMEM((8, D), F32), pltpu.VMEM((4, 1, D), F32),
            pltpu.VMEM((2, TOK, D), BF16),
            pltpu.SemaphoreType.DMA((N_SEM,)), pltpu.SemaphoreType.DMA((N_SEM,)), pltpu.SemaphoreType.DMA((11,)),
        ],
        compiler_params=pltpu.CompilerParams(collective_id=0, has_side_effects=True, vmem_limit_bytes=67_000_000),
        name='main',
    )(x, dout, w_query, w_out, w_key, w_value, norm_w[None, :], positions, jnp.asarray(freq[None, :], F32))

    whole = lambda s: pl.BlockSpec(s, lambda t: (0,) * len(s))
    steps = 2
    cols = D // steps
    by_row = lambda r, c: pl.BlockSpec((r, c), lambda t: (t, 0))
    by_col = pl.BlockSpec((HW, cols), lambda t: (0, t))
    dwq, dwo, dwk, dwv, out, dx, dw = pl.pallas_call(
        grad_kernel,
        grid=(steps,),
        out_shape=[sds((D, HW), F32), sds((HW, D), F32), sds((D, HD), F32), sds((D, HD), F32), sds((TOK, D), BF16), sds((TOK, D), BF16), sds((1, D), F32)],
        in_specs=[by_col, by_col, pl.BlockSpec((4, TOK, cols), lambda t: (0, 0, t)), pl.BlockSpec((2, TB, cols), lambda t: (1, 1, t)),
                  whole((2, HW, TOK)), whole((2, NB, SEQ, 2 * HD)), by_row(TOK // steps, D), by_row(TOK // steps, D), whole((1, D))],
        out_specs=[by_row(cols, HW), by_col, by_row(cols, HD), by_row(cols, HD), by_row(TOK // steps, D), by_row(TOK // steps, D), whole((1, D))],
        scratch_shapes=[pltpu.VMEM((6, 2 * HD, TOK), BF16)],
        compiler_params=pltpu.CompilerParams(vmem_limit_bytes=64_000_000),
        name='grads',
    )(accq, acco, act_all, dout_all, oqt, dkv, out, dx, dw)

    return out.reshape(NB, TB, D), dx.reshape(NB, TB, D), dwq, dwo, dwk, dwv, dw.reshape(D)


def solution(mesh):
    specs_in = (P('dp', 'tp'), P('dp'), P(), P(None, 'tp'), P(), P(), P('tp'), P('dp', 'tp'))
    specs_out = (P('dp', 'tp'), P('dp', 'tp'), P('dp', 'tp'), P(('dp', 'tp')), P('dp'), P('dp'), P('dp'))
    return jax.shard_map(local_block, mesh=mesh, in_specs=specs_in, out_specs=specs_out, check_vma=False)
```

```python
import jax
import jax.numpy as jnp
import numpy as np
from jax import lax
from jax.experimental import pallas as pl
from jax.experimental.pallas import tpu as pltpu
from jax.sharding import PartitionSpec as P

F32 = jnp.float32
BF16 = jnp.bfloat16
MESH = pl.DeviceIdType.MESH

TB = 256
NB = 2
TOK = TB * NB
SEQ = 1024
D = 2048
HD = 128
HL = 4
HW = HD * HL
SCALE = HD ** -0.5

N_SEM = 52
(WQ_X, _, _, _, WQ_REL, _, _, _, WQ_SIB,
 WO_X, _, _, _, WO_REL, _, _, _, WO_SIB,
 KV_X, KV_SIB, KV_REL, KV_LATE, _, BULK_END,
 BULK_X, _, _, _, BULK_REL, _, _, _,
 DOUT_SIB, ACT_SIB, RS_SIB, RS_SIB2, OQ_SIB, DW_SIB, DW_X, DW_XS,
 DKV_X, _, _, _, DKV_SIB, _, _, _, DKV_REL, _, _, _) = range(N_SEM)
KEY = slice(HD)
VAL = slice(HD, 2 * HD)


def dot_nn(a, b):
    return jnp.dot(a, b, preferred_element_type=F32)


def dot_nt(a, b):
    return lax.dot_general(a, b, (((1,), (1,)), ((), ())), preferred_element_type=F32)


def dot_tn(a, b):
    return lax.dot_general(a, b, (((0,), (0,)), ((), ())), preferred_element_type=F32)


def rope(u, cos_t, sin_t):
    return u * cos_t + pltpu.roll(u, HD // 2, 1) * sin_t


def rope_back(u, cos_t, sin_t):
    return u * cos_t - pltpu.roll(u, HD // 2, 1) * sin_t


def rope_back_t(u, cos_t, sin_t):
    swapped = jnp.concatenate([u[HD // 2:], u[:HD // 2]], axis=0)
    return u * cos_t - swapped * sin_t


def attend(n, q, do, k_ref, b, kt_ref):
    keys = n * TB
    k = k_ref[b, 0:keys, KEY]
    v = k_ref[b, 0:keys, VAL]
    s = dot_nt(k, q)
    row = lax.broadcasted_iota(jnp.int32, (TB, TB), 0)
    col = lax.broadcasted_iota(jnp.int32, (TB, TB), 1)
    last = jnp.where(row <= col, s[keys - TB:], -1e30)
    s = last if n == 1 else jnp.concatenate([s[:keys - TB], last], axis=0)
    e = jnp.exp(s - jnp.max(s, axis=0, keepdims=True))
    p = e * (1.0 / jnp.sum(e, axis=0, keepdims=True))
    p_low = p.astype(BF16)
    dp = dot_nt(v, do)
    ds = (p * (dp - jnp.sum(p * dp, axis=0, keepdims=True))).astype(BF16)
    o_t = dot_nn(kt_ref[b, VAL, 0:keys], p_low)
    dq_t = dot_nn(kt_ref[b, KEY, 0:keys], ds)
    return o_t, dq_t, p_low, ds


def transpose_kv(kv_ref, kt_ref, b, later):
    for j in range(2):
        r = pl.ds(pl.multiple_of((2 * later + j) * TB, TB), TB)
        kt_ref[b, :, r] = kv_ref[b, r, :].astype(F32).T.astype(BF16)


def main_kernel(x_hbm, dout_hbm, wq_own, wo_own, wk_own, wv_own, normw_ref, pos_ref, freq_ref,
                out_hbm, dx_hbm, dw_ref, accq_hbm, acco_hbm, oqt_hbm, dkv_hbm, act_all, dout_all,
                x_ref, dout_ref, io_ref, dkv_ref, oqt, trig_t, dwq_acc,
                act, kv_ref, wkv, cos_s, sin_s, wq_buf, wo_buf, q_s, do_s, o_s, dq_s, out_acc, da_acc, kt_ref,
                dkv_acc, rs_a, rs_c, dw_acc, dw_parts, buf, send, recv, lsem):
    dp = lax.axis_index('dp')
    tp = lax.axis_index('tp')
    sib = (dp, tp ^ 1)
    xp = (dp, tp ^ 2)
    xs = (dp, tp ^ 3)
    yp = (dp ^ 1, tp)
    zp = (dp ^ 2, tp)
    yzp = (dp ^ 3, tp)

    def rc(i, src, dst, dev):
        return pltpu.make_async_remote_copy(src_ref=src, dst_ref=dst, send_sem=send.at[i], recv_sem=recv.at[i],
                                            device_id=dev, device_id_type=MESH)

    def quarter(which, shard, j):
        size = 512 if which == 0 else 128
        r = pl.ds(pl.multiple_of((dp ^ j) * size, size), size)
        if shard is None:
            return (wq_own, wo_own)[which].at[r, :]
        return (wq_buf, wo_buf)[which].at[shard, r, :]

    def rows(blk):
        return pl.ds(pl.multiple_of(blk * TB, TB), TB)

    copies = {}

    def start(i, src, dst, dev):
        copies[i] = rc(i, src, dst, dev)
        copies[i].start()

    def first_quarter(which, i):
        start(i, quarter(which, None, 0), quarter(which, 2, 0), xp)

    def local(i, src, dst):
        cp = pltpu.make_async_copy(src, dst, lsem.at[i])
        cp.start()
        return cp

    def spread(which):
        first = (WQ_X, WO_X)[which]
        mine = quarter(which, 2, 0)
        rc(first, quarter(which, None, 0), mine, xp).wait_recv()
        for j, dev in ((1, yp), (2, zp), (3, yzp)):
            rc(first + j, mine, mine, dev).start()
        rc(first + 4, mine, quarter(which, 3, 0), sib).start()

    def bulk(c):
        r = pl.ds((c // 2) * TB, HD if c == 3 else TB)
        src, dst = (act, act_all) if c % 2 else (dout_hbm, dout_all)
        return rc(BULK_X + c, src.at[r, :], dst.at[2, r, :], xp)

    def bulk_end():
        r = pl.ds(TOK - HD, HD)
        return rc(BULK_END, act.at[r, :], act_all.at[2, r, :], xp)

    def receive(c):
        whole = act_all if c % 2 else dout_all
        r = pl.ds((c // 2) * TB, TB)
        bulk(c).wait_recv()
        if c == 3:
            bulk_end().wait_recv()
        rc(BULK_REL + c, whole.at[2, r, :], whole.at[3, r, :], sib).start()

    load_x = local(8, x_hbm, x_ref)
    load_k = local(0, wk_own, wkv.at[:, KEY])
    load_v = local(1, wv_own, wkv.at[:, VAL])
    load_q = local(2, wq_own, wq_buf.at[0])
    load_o = local(3, wo_own, wo_buf.at[0])
    load_d = local(4, dout_hbm, dout_ref)

    barrier = pltpu.get_barrier_semaphore()
    for dev in (sib, xp, xs, yp, zp, yzp):
        pl.semaphore_signal(barrier, inc=1, device_id=dev, device_id_type=MESH)
    pl.semaphore_wait(barrier, 6)

    first_quarter(0, WQ_X)
    start(WQ_SIB, wq_own, wq_buf.at[1], sib)
    start(WO_SIB, wo_own, wo_buf.at[1], sib)
    start(DOUT_SIB, dout_hbm, dout_all.at[1], sib)
    load_x.wait()

    def norm_rows(j, carry):
        r = pl.ds(pl.multiple_of(j * 64, 64), 64)
        xf = x_ref[r, :].astype(F32)
        inv = lax.rsqrt(jnp.mean(xf * xf, axis=-1, keepdims=True) + 1e-6)
        act[r, :] = (xf * inv * (1.0 + normw_ref[...])).astype(BF16)
        return carry

    lax.fori_loop(0, TOK // 64, norm_rows, 0)
    lane = lax.broadcasted_iota(jnp.int32, (HD, HD), 1)

    def tables(blk):
        for b in range(NB):
            for h in range(TB // HD):
                pos = pos_ref[b:b + 1, pl.ds(pl.multiple_of(blk * TB + h * HD, HD), HD)].astype(F32)
                angle = jnp.broadcast_to(pos, (HD, HD)).T * freq_ref[...]
                r = pl.ds(pl.multiple_of(blk * TB + h * HD, HD), HD)
                sin_t = jnp.sin(angle)
                cos_s[b, r, :] = jnp.cos(angle)
                sin_s[b, r, :] = jnp.where(lane < HD // 2, -sin_t, sin_t)

    tables(tp)
    load_k.wait()
    load_v.wait()
    kv = dot_nn(act[...], wkv[...])
    for b in range(NB):
        r = slice(b * TB, (b + 1) * TB)
        k_rot = rope(kv[r, KEY].astype(BF16).astype(F32), cos_s[b, rows(tp), :], sin_s[b, rows(tp), :])
        kv_ref[b, rows(tp), KEY] = k_rot.astype(BF16)
        kv_ref[b, rows(tp), VAL] = kv[r, VAL].astype(BF16)
    own_kv = kv_ref.at[:, rows(tp), :]

    @pl.when(tp < 2)
    def _():
        rc(KV_X, own_kv, own_kv, xp).start()

    start(KV_SIB, own_kv, own_kv, sib)
    first_quarter(1, WO_X)
    bulk(0).start()
    start(ACT_SIB, act, act_all.at[1], sib)
    own_a = local(5, act, act_all.at[0])

    out_acc[...] = jnp.zeros_like(out_acc)
    da_acc[...] = jnp.zeros_like(da_acc)
    dkv_acc[...] = jnp.zeros_like(dkv_acc)

    def project(n_rows, a_src, slot, table):
        def pair(j, carry):
            cols = pl.ds(pl.multiple_of(j * TB, TB), TB)
            q = dot_nn(a_src[0:n_rows, :], wq_buf[slot, :, cols]).astype(BF16).astype(F32)
            for t in range(n_rows // TB):
                r = slice(t * TB, (t + 1) * TB)
                cos_t, sin_t = table(t)
                for h in range(2):
                    piece = rope(q[r, h * HD:(h + 1) * HD], cos_t, sin_t) * SCALE
                    q_s[r, pl.ds(pl.multiple_of((2 * j + h) * HD, HD), HD)] = piece.astype(BF16)
            return carry
        lax.fori_loop(0, HL // 2, pair, 0)

    def project_back(d_src, slot, dst):
        def pair(j, carry):
            cols = pl.ds(pl.multiple_of(j * TB, TB), TB)
            dst[:, cols] = dot_nt(d_src[...], wo_buf[slot, cols, :]).astype(BF16)
            return carry
        lax.fori_loop(0, HL // 2, pair, 0)

    def project_own(slot):
        project(TOK, act, slot, lambda b: (cos_s[b, rows(tp), :], sin_s[b, rows(tp), :]))
        project_back(dout_ref, slot, do_s)

    def attend_group():
        for n in range(1, 5):
            @pl.when(tp == n - 1)
            def _():
                def step(t, carry):
                    b = t // 2
                    r = pl.ds(pl.multiple_of(b * TB, TB), TB)
                    cos_t = cos_s[b, rows(tp), :]
                    sin_t = sin_s[b, rows(tp), :]
                    for j in range(2):
                        c = pl.ds(pl.multiple_of(((t % 2) * 2 + j) * HD, HD), HD)
                        q = q_s[r, c]
                        do = do_s[r, c]
                        o_t, dq_t, p_low, ds = attend(n, q, do, kv_ref, b, kt_ref)
                        o_s[r, c] = o_t.T.astype(BF16)
                        dq_s[r, c] = rope_back(dq_t.T * SCALE, cos_t, sin_t).astype(BF16)
                        dkv_acc[b, 0:n * TB, KEY] += dot_nn(ds, q)
                        dkv_acc[b, 0:n * TB, VAL] += dot_nn(p_low, do)
                    return carry
                lax.fori_loop(0, 4, step, 0)

    def accumulate(slot):
        def tile(j, carry):
            cols = pl.ds(pl.multiple_of(j * HW, HW), HW)
            out_acc[:, cols] += dot_nn(o_s[...], wo_buf[slot, :, cols])
            da_acc[:, cols] += dot_nt(dq_s[...], wq_buf[slot, cols, :])
            return carry
        lax.fori_loop(0, 4, tile, 0)

    load_q.wait()
    load_o.wait()
    load_d.wait()
    own_d = local(4, dout_ref, dout_all.at[0])
    project_own(0)
    tables(tp ^ 2)
    tables(tp ^ 3)
    spread(0)
    other_kv = kv_ref.at[:, rows(tp ^ 2), :]

    @pl.when(tp >= 2)
    def _():
        rc(KV_X, other_kv, other_kv, xp).wait_recv()
        rc(KV_REL, other_kv, other_kv, sib).start()

    copies[KV_SIB].wait_recv()
    for b in range(NB):
        transpose_kv(kv_ref, kt_ref, b, tp // 2)

    @pl.when(tp >= 2)
    def _():
        sib_kv = kv_ref.at[:, rows(tp ^ 3), :]
        rc(KV_REL, sib_kv, sib_kv, sib).wait_recv()
        for b in range(NB):
            transpose_kv(kv_ref, kt_ref, b, False)

    def weight_grad(acc, first, left, src):
        def tile(j, carry):
            cols = pl.ds(pl.multiple_of(j * HW, HW), HW)
            part = dot_nn(left[...], src[:, cols])
            acc[:, cols] = part if first else acc[:, cols] + part
            return carry
        lax.fori_loop(0, 4, tile, 0)

    def group(i, carry):
        @pl.when(i == 1)
        def _():
            rc(WQ_SIB, wq_own, wq_buf.at[1], sib).wait_recv()
            rc(WO_SIB, wo_own, wo_buf.at[1], sib).wait_recv()

        @pl.when(i == 2)
        def _():
            copies[ACT_SIB].wait_recv()
            load = local(6, act_all.at[1], buf.at[0])
            weight_grad(dwq_acc, True, oqt.at[0, 1], act)
            load.wait()
            rc(OQ_SIB, rs_c, oqt.at[1], sib).wait_recv()
            weight_grad(dwq_acc, False, oqt.at[1, 1], buf.at[0])
            for which, first in ((0, WQ_X), (1, WO_X)):
                for j in (1, 2, 3):
                    piece = quarter(which, 2, j)
                    rc(first + j, piece, piece, sib).wait_recv()
                    rc(first + 4 + j, piece, quarter(which, 3, j), sib).start()

        @pl.when(i == 3)
        def _():
            for which, rel in ((0, WQ_REL), (1, WO_REL)):
                for j in range(4):
                    rc(rel + j, quarter(which, 2, j), quarter(which, 3, j), sib).wait_recv()

        @pl.when(i > 0)
        def _():
            project_own(i)

        attend_group()

        @pl.when(i == 0)
        def _():
            spread(1)
            for c in (1, 2, 3):
                bulk(c).start()

        accumulate(i)

        @pl.when(i == 0)
        def _():
            oqt[0, 0] = o_s[...].astype(F32).T.astype(BF16)
            oqt[0, 1] = dq_s[...].astype(F32).T.astype(BF16)

        @pl.when(i == 1)
        def _():
            rs_c[0] = o_s[...].astype(F32).T.astype(BF16)
            rs_c[1] = dq_s[...].astype(F32).T.astype(BF16)
            rc(OQ_SIB, rs_c, oqt.at[1], sib).start()
        return carry

    lax.fori_loop(0, 4, group, 0)
    copies[DOUT_SIB].wait_recv()
    load_sib = local(7, dout_all.at[1], buf.at[1])

    start(RS_SIB, dkv_acc.at[:, rows(tp ^ 1), :], rs_a.at[0], sib)
    start(RS_SIB2, dkv_acc.at[:, rows(tp ^ 3), :], rs_a.at[1], sib)
    for r in range(8):
        cols = slice(r * 256, (r + 1) * 256)
        io_ref[:, cols] = (x_ref[:, cols].astype(F32) + out_acc[:, cols]).astype(BF16)
    put_out = local(8, io_ref, out_hbm)
    copies[RS_SIB].wait_recv()
    copies[RS_SIB2].wait_recv()

    def dkv_piece(part, b, blk):
        return dkv_ref.at[part, b, rows(blk), :]

    def reduce_kv(part, blk):
        for b in range(NB):
            total = dkv_acc[b, rows(blk), :] + rs_a[part, b]
            d_k = rope_back(total[:, KEY], cos_s[b, rows(blk), :], sin_s[b, rows(blk), :])
            dkv_ref[part, b, rows(blk), KEY] = d_k.astype(BF16)
            dkv_ref[part, b, rows(blk), VAL] = total[:, VAL].astype(BF16)
        for b in range(NB):
            piece = dkv_piece(part, b, blk)
            rc(DKV_X + 2 * part + b, piece, piece, xp).start()
            rc(DKV_SIB + 2 * part + b, piece, piece, sib).start()

    @pl.when(tp >= 2)
    def _():
        reduce_kv(1, tp ^ 2)
        dkv_ref[1, :, rows(tp), :] = jnp.zeros((NB, TB, 2 * HD), BF16)

    bulk_end().start()
    reduce_kv(0, tp)

    for c in range(2):
        receive(c)
    weight_grad(out_acc, True, oqt.at[0, 0], dout_ref)
    load_sib.wait()
    weight_grad(out_acc, False, oqt.at[1, 0], buf.at[1])
    own_a.wait()
    own_d.wait()
    put_out.wait()

    def take(part, b, blk):
        piece = dkv_piece(part, b, blk)
        rc(DKV_X + NB * part + b, piece, piece, xp).wait_recv()
        rc(DKV_REL + NB * part + b, piece, piece, sib).start()

    def dw_copies():
        return [rc(DW_SIB + k, dw_parts.at[0], dw_parts.at[k + 1], dev) for k, dev in enumerate((sib, xp, xs))]

    def finish_dx():
        @pl.when(tp < 2)
        def _():
            for b in range(NB):
                take(1, b, tp)

        dw_acc[...] = jnp.zeros_like(dw_acc)
        gain = 1.0 + normw_ref[...]

        def dx_rows(j, carry):
            b = j // 2
            r = pl.ds(pl.multiple_of(j * HD, HD), HD)
            own = pl.ds(pl.multiple_of(tp * TB + (j % 2) * HD, HD), HD)
            da = da_acc[r, :] + dot_nt(dkv_ref[0, b, own, :], wkv[...]) + dot_nt(dkv_ref[1, b, own, :], wkv[...])
            xf = x_ref[r, :].astype(F32)
            inv = lax.rsqrt(jnp.mean(xf * xf, axis=-1, keepdims=True) + 1e-6)
            normed = xf * inv
            prod = da * normed
            dw_acc[...] += jnp.sum(prod.reshape(-1, *dw_acc.shape), axis=0)
            corr = jnp.mean(prod * gain, axis=-1, keepdims=True)
            io_ref[r, :] = (dout_ref[r, :].astype(F32) + inv * (da * gain - normed * corr)).astype(BF16)
            return carry

        lax.fori_loop(0, TOK // HD, dx_rows, 0)
        dw_parts[0] = jnp.sum(dw_acc[...], axis=0, keepdims=True)
        pltpu.make_async_copy(io_ref, dx_hbm, lsem.at[8]).start()
        for cp in dw_copies():
            cp.start()

    def head_part(t, carry):
        b = t // 2
        i = 2 + t % 2
        blk = tp ^ i
        r = pl.ds(pl.multiple_of(b * TB, TB), TB)

        def load(c, k):
            whole = (dout_all, act_all)[c]
            return pltpu.make_async_copy(whole.at[2 + k, r, :], buf.at[1 - c, pl.ds(k * TB, TB), :], lsem.at[7 - c + 5 * k])

        def load_relayed(c):
            whole = (dout_all, act_all)[c]
            rc(BULK_REL + 2 * b + c, whole.at[2, r, :], whole.at[3, r, :], sib).wait_recv()
            load(c, 1).start()

        half = pl.ds(pl.multiple_of((i - 2) * TB, TB), TB)

        @pl.when(i == 2)
        def _():
            load(0, 0).start()
            load_relayed(0)

            @pl.when(b == 0)
            def _():
                load(1, 0).start()

            for k in range(2):
                load(0, k).wait()
                part = slice(k * TB, (k + 1) * TB)
                project_back(buf.at[1, part, :], 0, do_s.at[part, :])

            @pl.when(b == 1)
            def _():
                receive(3)
                load(1, 0).start()

            load(1, 0).wait()

        @pl.when(i == 3)
        def _():
            load(1, 1).wait()

        cos_t = cos_s.at[b, rows(blk), :]
        sin_t = sin_s.at[b, rows(blk), :]
        trig_t[0] = cos_t[...].T
        trig_t[1] = sin_t[...].T

        def late_kv(blk):
            piece = kv_ref.at[b, rows(blk), :]
            return rc(KV_LATE + b, piece, piece, sib)

        @pl.when((i == 2) & (tp < 2))
        def _():
            kv = dot_nn(buf[0, 0:TB, :], wkv[...])
            kv_ref[b, rows(blk), KEY] = rope(kv[:, KEY].astype(BF16).astype(F32), cos_t[...], sin_t[...]).astype(BF16)
            kv_ref[b, rows(blk), VAL] = kv[:, VAL].astype(BF16)
            late_kv(tp ^ 2).start()

        project(TB, buf.at[0, half, :], 0, lambda _: (cos_t[...], sin_t[...]))

        @pl.when(i == 2)
        def _():
            load_relayed(1)

        @pl.when((i == 2) & (tp < 2))
        def _():
            late_kv(tp ^ 3).wait_recv()
            transpose_kv(kv_ref, kt_ref, b, True)

        @pl.when(t == 3)
        def _():
            for seq in range(NB):
                take(0, seq, tp ^ 2)

        for n in range(1, 5):
            @pl.when(blk == n - 1)
            def _():
                def step(u, carry):
                    for j in range(2):
                        c = pl.ds(pl.multiple_of((u * 2 + j) * HD, HD), HD)
                        o_t, dq_t, _, _ = attend(n, q_s[0:TB, c], do_s[half, c], kv_ref, b, kt_ref)
                        oqt[0, 0, c, half] = o_t.astype(BF16)
                        oqt[0, 1, c, half] = rope_back_t(dq_t * SCALE, trig_t[0], trig_t[1]).astype(BF16)
                    return carry
                lax.fori_loop(0, 2, step, 0)

        @pl.when(t == 1)
        def _():
            receive(2)
            weight_grad(out_acc, False, oqt.at[0, 0], buf.at[1])
            weight_grad(dwq_acc, False, oqt.at[0, 1], buf.at[0])
            pltpu.make_async_copy(dwq_acc, accq_hbm, lsem.at[9]).start()
            pltpu.make_async_copy(out_acc, acco_hbm, lsem.at[10]).start()
            finish_dx()
        return carry

    lax.fori_loop(0, 4, head_part, 0)
    put_oqt = local(0, oqt.at[0], oqt_hbm)
    put_dkv = []
    for b in range(NB):
        def arrived(first, part, blk):
            piece = dkv_piece(part, b, blk)
            rc(first + NB * part + b, piece, piece, sib).wait_recv()

        arrived(DKV_SIB, 0, tp ^ 1)
        arrived(DKV_REL, 0, tp ^ 3)

        @pl.when(tp < 2)
        def _():
            arrived(DKV_REL, 1, tp ^ 1)

        @pl.when(tp >= 2)
        def _():
            arrived(DKV_SIB, 1, tp ^ 3)

        put_dkv.append(local(1 + b, dkv_ref.at[0, b], dkv_hbm.at[0, b]))
        put_dkv.append(local(3 + b, dkv_ref.at[1, b, 0:TOK, :], dkv_hbm.at[1, b, 0:TOK, :]))

    for cp in dw_copies():
        cp.wait_recv()
    parts = [dw_parts[jnp.bitwise_xor(tp, t)] for t in range(4)]
    dw_ref[...] = sum(parts[1:], parts[0])

    for cp in (put_oqt, *put_dkv):
        cp.wait()
    pltpu.make_async_copy(io_ref, dx_hbm, lsem.at[8]).wait()
    for cp in dw_copies():
        cp.wait_send()
    bulk_end().wait_send()
    pltpu.make_async_copy(dwq_acc, accq_hbm, lsem.at[9]).wait()
    pltpu.make_async_copy(out_acc, acco_hbm, lsem.at[10]).wait()
    for i in copies:
        copies[i].wait_send()
    rc(OQ_SIB, rs_c, oqt.at[1], sib).wait_send()
    for b in range(NB):
        piece = dkv_piece(0, b, tp)
        for i in (DKV_X, DKV_SIB, DKV_REL):
            rc(i + b, piece, piece, sib).wait_send()

        @pl.when(tp < 2)
        def _():
            rc(DKV_REL + 2 + b, piece, piece, sib).wait_send()
            rc(KV_LATE + b, piece, piece, sib).wait_send()

        @pl.when(tp >= 2)
        def _():
            rc(DKV_X + 2 + b, piece, piece, sib).wait_send()
            rc(DKV_SIB + 2 + b, piece, piece, sib).wait_send()

    @pl.when(tp < 2)
    def _():
        rc(KV_X, own_kv, own_kv, xp).wait_send()

    @pl.when(tp >= 2)
    def _():
        rc(KV_REL, own_kv, own_kv, sib).wait_send()

    for c in range(4):
        bulk(c).wait_send()
        whole = act_all if c % 2 else dout_all
        r = slice((c // 2) * TB, (c // 2 + 1) * TB)
        rc(BULK_REL + c, whole.at[2, r, :], whole.at[3, r, :], sib).wait_send()
    for which, first in ((0, WQ_X), (1, WO_X)):
        for j in range(1, 8):
            rc(first + j, quarter(which, 2, j % 4), quarter(which, 2, j % 4), sib).wait_send()


def grad_kernel(accq_ref, acco_ref, act_ref, dout_ref, oqt_ref, dkv_ref, out_in, dx_in, dw_in,
                dwq_ref, dwo_ref, dwk_ref, dwv_ref, out_ref, dx_ref, dw_ref, dkvt):
    tp = lax.axis_index('tp')
    out_ref[...] = out_in[...]
    dx_ref[...] = dx_in[...]
    dw_ref[...] = dw_in[...]

    @pl.when(pl.program_id(0) == 0)
    def _():
        for t in range(6):
            for b in range(NB):
                piece = dkv_ref[t // 4, b, (t % 4) * TB:(t % 4 + 1) * TB, :]
                dkvt[t, :, b * TB:(b + 1) * TB] = piece.astype(F32).T.astype(BF16)

    a = jnp.concatenate([act_ref[2, TB:TOK, :], act_ref[3, TB:TOK, :]], axis=0)
    d = dout_ref[...].reshape(TOK, -1)
    dwo_ref[...] = acco_ref[...] + dot_nn(oqt_ref[0], d)
    dwq_ref[...] = (accq_ref[...] + dot_nn(oqt_ref[1], a)).T
    total = dot_nn(dkvt[0], act_ref[jnp.bitwise_xor(tp, 0)])
    for t in range(1, 6):
        total += dot_nn(dkvt[t], act_ref[jnp.bitwise_xor(tp, t % 4)])
    dwk_ref[...] = total[KEY].T
    dwv_ref[...] = total[VAL].T


def local_block(hidden, positions, norm_w, w_query, w_key, w_value, w_out, grad_out):
    x = hidden.reshape(TOK, D)
    dout = grad_out.reshape(TOK, D)
    freq = 10000.0 ** (-2.0 * (np.arange(HD) % (HD // 2)) / HD)

    vmem = pl.BlockSpec(memory_space=pltpu.VMEM)
    anym = pl.BlockSpec(memory_space=pl.ANY)
    sds = jax.ShapeDtypeStruct
    out, dx, dw, accq, acco, oqt, dkv, act_all, dout_all = pl.pallas_call(
        main_kernel,
        out_shape=[sds((TOK, D), BF16), sds((TOK, D), BF16), sds((1, D), F32), sds((HW, D), F32), sds((HW, D), F32),
                   sds((2, HW, TOK), BF16), sds((2, NB, SEQ, 2 * HD), BF16), sds((4, TOK, D), BF16), sds((4, TOK, D), BF16)],
        in_specs=[anym, anym, anym, anym, anym, anym, vmem, vmem, vmem],
        out_specs=[anym, anym, vmem, anym, anym, anym, anym, anym, anym],
        scratch_shapes=[
            pltpu.VMEM((TOK, D), BF16), pltpu.VMEM((TOK, D), BF16), pltpu.VMEM((TOK, D), BF16),
            pltpu.VMEM((2, NB, SEQ, 2 * HD), BF16),
            pltpu.VMEM((2, 2, HW, TOK), BF16),
            pltpu.VMEM((2, HD, TB), F32),
            pltpu.VMEM((HW, D), F32),
            pltpu.VMEM((TOK, D), BF16),
            pltpu.VMEM((NB, SEQ, 2 * HD), BF16),
            pltpu.VMEM((D, 2 * HD), BF16),
            pltpu.VMEM((NB, SEQ, HD), F32), pltpu.VMEM((NB, SEQ, HD), F32),
            pltpu.VMEM((4, D, HW), BF16), pltpu.VMEM((4, HW, D), BF16),
            pltpu.VMEM((TOK, HW), BF16), pltpu.VMEM((TOK, HW), BF16),
            pltpu.VMEM((TOK, HW), BF16), pltpu.VMEM((TOK, HW), BF16),
            pltpu.VMEM((TOK, D), F32), pltpu.VMEM((TOK, D), F32),
            pltpu.VMEM((NB, 2 * HD, SEQ), BF16),
            pltpu.VMEM((NB, SEQ, 2 * HD), F32),
            pltpu.VMEM((2, NB, TB, 2 * HD), F32),
            pltpu.VMEM((2, HW, TOK), BF16),
            pltpu.VMEM((8, D), F32), pltpu.VMEM((4, 1, D), F32),
            pltpu.VMEM((2, TOK, D), BF16),
            pltpu.SemaphoreType.DMA((N_SEM,)), pltpu.SemaphoreType.DMA((N_SEM,)), pltpu.SemaphoreType.DMA((13,)),
        ],
        compiler_params=pltpu.CompilerParams(collective_id=0, has_side_effects=True, vmem_limit_bytes=67_000_000),
        name='main',
    )(x, dout, w_query, w_out, w_key, w_value, norm_w[None, :], positions, jnp.asarray(freq[None, :], F32))

    whole = lambda s: pl.BlockSpec(s, lambda t: (0,) * len(s))
    steps = 2
    cols = D // steps
    by_row = lambda r, c: pl.BlockSpec((r, c), lambda t: (t, 0))
    by_col = pl.BlockSpec((HW, cols), lambda t: (0, t))
    dwq, dwo, dwk, dwv, out, dx, dw = pl.pallas_call(
        grad_kernel,
        grid=(steps,),
        out_shape=[sds((D, HW), F32), sds((HW, D), F32), sds((D, HD), F32), sds((D, HD), F32), sds((TOK, D), BF16), sds((TOK, D), BF16), sds((1, D), F32)],
        in_specs=[by_col, by_col, pl.BlockSpec((4, TOK, cols), lambda t: (0, 0, t)), pl.BlockSpec((2, TB, cols), lambda t: (1, 1, t)),
                  whole((2, HW, TOK)), whole((2, NB, SEQ, 2 * HD)), by_row(TOK // steps, D), by_row(TOK // steps, D), whole((1, D))],
        out_specs=[by_row(cols, HW), by_col, by_row(cols, HD), by_row(cols, HD), by_row(TOK // steps, D), by_row(TOK // steps, D), whole((1, D))],
        scratch_shapes=[pltpu.VMEM((6, 2 * HD, TOK), BF16)],
        compiler_params=pltpu.CompilerParams(vmem_limit_bytes=64_000_000),
        name='grads',
    )(accq, acco, act_all, dout_all, oqt, dkv, out, dx, dw)

    return out.reshape(NB, TB, D), dx.reshape(NB, TB, D), dwq, dwo, dwk, dwv, dw.reshape(D)


def solution(mesh):
    specs_in = (P('dp', 'tp'), P('dp'), P(), P(None, 'tp'), P(), P(), P('tp'), P('dp', 'tp'))
    specs_out = (P('dp', 'tp'), P('dp', 'tp'), P('dp', 'tp'), P(('dp', 'tp')), P('dp'), P('dp'), P('dp'))
    return jax.shard_map(local_block, mesh=mesh, in_specs=specs_in, out_specs=specs_out, check_vma=False)
```

```python
import jax
import jax.numpy as jnp
import numpy as np
from jax import lax
from jax.experimental import pallas as pl
from jax.experimental.pallas import tpu as pltpu
from jax.sharding import PartitionSpec as P

F32 = jnp.float32
BF16 = jnp.bfloat16
MESH = pl.DeviceIdType.MESH

TB = 256
NB = 2
TOK = TB * NB
SEQ = 1024
D = 2048
HD = 128
HL = 4
HW = HD * HL
SCALE = HD ** -0.5

N_SEM = 52
(WQ_X, _, _, _, WQ_REL, _, _, _, WQ_SIB,
 WO_X, _, _, _, WO_REL, _, _, _, WO_SIB,
 KV_X, KV_SIB, KV_REL, KV_LATE, _, BULK_END,
 BULK_X, _, _, _, BULK_REL, _, _, _,
 DOUT_SIB, ACT_SIB, RS_SIB, RS_SIB2, OQ_SIB, DW_SIB, DW_X, DW_XS,
 DKV_X, _, _, _, DKV_SIB, _, _, _, DKV_REL, _, _, _) = range(N_SEM)
KEY = slice(HD)
VAL = slice(HD, 2 * HD)


def dot_nn(a, b):
    return jnp.dot(a, b, preferred_element_type=F32)


def dot_nt(a, b):
    return lax.dot_general(a, b, (((1,), (1,)), ((), ())), preferred_element_type=F32)


def dot_tn(a, b):
    return lax.dot_general(a, b, (((0,), (0,)), ((), ())), preferred_element_type=F32)


def rope(u, cos_t, sin_t):
    return u * cos_t + pltpu.roll(u, HD // 2, 1) * sin_t


def rope_back(u, cos_t, sin_t):
    return u * cos_t - pltpu.roll(u, HD // 2, 1) * sin_t


def rope_back_t(u, cos_t, sin_t):
    swapped = jnp.concatenate([u[HD // 2:], u[:HD // 2]], axis=0)
    return u * cos_t - swapped * sin_t


def attend(n, q, do, k_ref, b, kt_ref):
    keys = n * TB
    k = k_ref[b, 0:keys, KEY]
    v = k_ref[b, 0:keys, VAL]
    s = dot_nt(k, q)
    row = lax.broadcasted_iota(jnp.int32, (TB, TB), 0)
    col = lax.broadcasted_iota(jnp.int32, (TB, TB), 1)
    last = jnp.where(row <= col, s[keys - TB:], -1e30)
    s = last if n == 1 else jnp.concatenate([s[:keys - TB], last], axis=0)
    e = jnp.exp(s - jnp.max(s, axis=0, keepdims=True))
    p = e * (1.0 / jnp.sum(e, axis=0, keepdims=True))
    p_low = p.astype(BF16)
    dp = dot_nt(v, do)
    ds = (p * (dp - jnp.sum(p * dp, axis=0, keepdims=True))).astype(BF16)
    o_t = dot_nn(kt_ref[b, VAL, 0:keys], p_low)
    dq_t = dot_nn(kt_ref[b, KEY, 0:keys], ds)
    return o_t, dq_t, p_low, ds


def transpose_kv(kv_ref, kt_ref, b, later):
    for j in range(2):
        r = pl.ds(pl.multiple_of((2 * later + j) * TB, TB), TB)
        kt_ref[b, :, r] = kv_ref[b, r, :].astype(F32).T.astype(BF16)


def main_kernel(x_hbm, dout_hbm, wq_own, wo_own, wk_own, wv_own, normw_ref, pos_ref, freq_ref,
                out_hbm, dx_hbm, dw_hbm, accq_hbm, acco_hbm, oqt_hbm, dkv_hbm, act_all, dout_all,
                x_ref, dout_ref, io_ref, dkv_ref, oqt, trig_t, dwq_acc,
                act, kv_ref, wkv, cos_s, sin_s, wq_buf, wo_buf, q_s, do_s, o_s, dq_s, out_acc, da_acc, kt_ref,
                dkv_acc, rs_a, rs_c, dw_acc, dw_parts, dw_row, buf, send, recv, lsem):
    dp = lax.axis_index('dp')
    tp = lax.axis_index('tp')
    sib = (dp, tp ^ 1)
    xp = (dp, tp ^ 2)
    xs = (dp, tp ^ 3)
    yp = (dp ^ 1, tp)
    zp = (dp ^ 2, tp)
    yzp = (dp ^ 3, tp)

    def rc(i, src, dst, dev):
        return pltpu.make_async_remote_copy(src_ref=src, dst_ref=dst, send_sem=send.at[i], recv_sem=recv.at[i],
                                            device_id=dev, device_id_type=MESH)

    def quarter(which, shard, j):
        size = 512 if which == 0 else 128
        r = pl.ds(pl.multiple_of((dp ^ j) * size, size), size)
        if shard is None:
            return (wq_own, wo_own)[which].at[r, :]
        return (wq_buf, wo_buf)[which].at[shard, r, :]

    def rows(blk):
        return pl.ds(pl.multiple_of(blk * TB, TB), TB)

    copies = {}

    def start(i, src, dst, dev):
        copies[i] = rc(i, src, dst, dev)
        copies[i].start()

    def first_quarter(which, i):
        start(i, quarter(which, None, 0), quarter(which, 2, 0), xp)

    def local(i, src, dst):
        cp = pltpu.make_async_copy(src, dst, lsem.at[i])
        cp.start()
        return cp

    def spread(which):
        first = (WQ_X, WO_X)[which]
        mine = quarter(which, 2, 0)
        rc(first, quarter(which, None, 0), mine, xp).wait_recv()
        for j, dev in ((1, yp), (2, zp), (3, yzp)):
            rc(first + j, mine, mine, dev).start()
        rc(first + 4, mine, quarter(which, 3, 0), sib).start()

    def bulk(c):
        r = pl.ds((c // 2) * TB, HD if c == 3 else TB)
        src, dst = (act, act_all) if c % 2 else (dout_hbm, dout_all)
        return rc(BULK_X + c, src.at[r, :], dst.at[2, r, :], xp)

    def bulk_end():
        r = pl.ds(TOK - HD, HD)
        return rc(BULK_END, act.at[r, :], act_all.at[2, r, :], xp)

    def receive(c):
        whole = act_all if c % 2 else dout_all
        r = pl.ds((c // 2) * TB, TB)
        bulk(c).wait_recv()
        if c == 3:
            bulk_end().wait_recv()
        rc(BULK_REL + c, whole.at[2, r, :], whole.at[3, r, :], sib).start()

    load_x = local(8, x_hbm, x_ref)
    load_k = local(0, wk_own, wkv.at[:, KEY])
    load_v = local(1, wv_own, wkv.at[:, VAL])
    load_q = local(2, wq_own, wq_buf.at[0])
    load_o = local(3, wo_own, wo_buf.at[0])
    load_d = local(4, dout_hbm, dout_ref)

    barrier = pltpu.get_barrier_semaphore()
    for dev in (sib, xp, xs, yp, zp, yzp):
        pl.semaphore_signal(barrier, inc=1, device_id=dev, device_id_type=MESH)
    pl.semaphore_wait(barrier, 6)

    first_quarter(0, WQ_X)
    start(WQ_SIB, wq_own, wq_buf.at[1], sib)
    start(WO_SIB, wo_own, wo_buf.at[1], sib)
    start(DOUT_SIB, dout_hbm, dout_all.at[1], sib)
    load_x.wait()

    def norm_rows(j, carry):
        r = pl.ds(pl.multiple_of(j * 64, 64), 64)
        xf = x_ref[r, :].astype(F32)
        inv = lax.rsqrt(jnp.mean(xf * xf, axis=-1, keepdims=True) + 1e-6)
        act[r, :] = (xf * inv * (1.0 + normw_ref[...])).astype(BF16)
        return carry

    lax.fori_loop(0, TOK // 64, norm_rows, 0)
    lane = lax.broadcasted_iota(jnp.int32, (HD, HD), 1)

    def tables(blk):
        for b in range(NB):
            for h in range(TB // HD):
                pos = pos_ref[b:b + 1, pl.ds(pl.multiple_of(blk * TB + h * HD, HD), HD)].astype(F32)
                angle = jnp.broadcast_to(pos, (HD, HD)).T * freq_ref[...]
                r = pl.ds(pl.multiple_of(blk * TB + h * HD, HD), HD)
                sin_t = jnp.sin(angle)
                cos_s[b, r, :] = jnp.cos(angle)
                sin_s[b, r, :] = jnp.where(lane < HD // 2, -sin_t, sin_t)

    tables(tp)
    load_k.wait()
    load_v.wait()
    kv = dot_nn(act[...], wkv[...])
    for b in range(NB):
        r = slice(b * TB, (b + 1) * TB)
        k_rot = rope(kv[r, KEY].astype(BF16).astype(F32), cos_s[b, rows(tp), :], sin_s[b, rows(tp), :])
        kv_ref[b, rows(tp), KEY] = k_rot.astype(BF16)
        kv_ref[b, rows(tp), VAL] = kv[r, VAL].astype(BF16)
    own_kv = kv_ref.at[:, rows(tp), :]

    @pl.when(tp < 2)
    def _():
        rc(KV_X, own_kv, own_kv, xp).start()

    start(KV_SIB, own_kv, own_kv, sib)
    first_quarter(1, WO_X)
    bulk(0).start()
    start(ACT_SIB, act, act_all.at[1], sib)
    own_a = local(5, act, act_all.at[0])

    out_acc[...] = jnp.zeros_like(out_acc)
    da_acc[...] = jnp.zeros_like(da_acc)
    dkv_acc[...] = jnp.zeros_like(dkv_acc)

    def project(n_rows, a_src, slot, table):
        def pair(j, carry):
            cols = pl.ds(pl.multiple_of(j * TB, TB), TB)
            q = dot_nn(a_src[0:n_rows, :], wq_buf[slot, :, cols]).astype(BF16).astype(F32)
            for t in range(n_rows // TB):
                r = slice(t * TB, (t + 1) * TB)
                cos_t, sin_t = table(t)
                for h in range(2):
                    piece = rope(q[r, h * HD:(h + 1) * HD], cos_t, sin_t) * SCALE
                    q_s[r, pl.ds(pl.multiple_of((2 * j + h) * HD, HD), HD)] = piece.astype(BF16)
            return carry
        lax.fori_loop(0, HL // 2, pair, 0)

    def project_back(d_src, slot, dst):
        def pair(j, carry):
            cols = pl.ds(pl.multiple_of(j * TB, TB), TB)
            dst[:, cols] = dot_nt(d_src[...], wo_buf[slot, cols, :]).astype(BF16)
            return carry
        lax.fori_loop(0, HL // 2, pair, 0)

    def project_own(slot):
        project(TOK, act, slot, lambda b: (cos_s[b, rows(tp), :], sin_s[b, rows(tp), :]))
        project_back(dout_ref, slot, do_s)

    def attend_group():
        for n in range(1, 5):
            @pl.when(tp == n - 1)
            def _():
                def step(t, carry):
                    b = t // 2
                    r = pl.ds(pl.multiple_of(b * TB, TB), TB)
                    cos_t = cos_s[b, rows(tp), :]
                    sin_t = sin_s[b, rows(tp), :]
                    for j in range(2):
                        c = pl.ds(pl.multiple_of(((t % 2) * 2 + j) * HD, HD), HD)
                        q = q_s[r, c]
                        do = do_s[r, c]
                        o_t, dq_t, p_low, ds = attend(n, q, do, kv_ref, b, kt_ref)
                        o_s[r, c] = o_t.T.astype(BF16)
                        dq_s[r, c] = rope_back(dq_t.T * SCALE, cos_t, sin_t).astype(BF16)
                        dkv_acc[b, 0:n * TB, KEY] += dot_nn(ds, q)
                        dkv_acc[b, 0:n * TB, VAL] += dot_nn(p_low, do)
                    return carry
                lax.fori_loop(0, 4, step, 0)

    def accumulate(slot):
        def tile(j, carry):
            cols = pl.ds(pl.multiple_of(j * HW, HW), HW)
            out_acc[:, cols] += dot_nn(o_s[...], wo_buf[slot, :, cols])
            da_acc[:, cols] += dot_nt(dq_s[...], wq_buf[slot, cols, :])
            return carry
        lax.fori_loop(0, 4, tile, 0)

    load_q.wait()
    load_o.wait()
    load_d.wait()
    own_d = local(4, dout_ref, dout_all.at[0])
    project_own(0)
    tables(tp ^ 2)
    tables(tp ^ 3)
    spread(0)
    other_kv = kv_ref.at[:, rows(tp ^ 2), :]

    @pl.when(tp >= 2)
    def _():
        rc(KV_X, other_kv, other_kv, xp).wait_recv()
        rc(KV_REL, other_kv, other_kv, sib).start()

    copies[KV_SIB].wait_recv()
    for b in range(NB):
        transpose_kv(kv_ref, kt_ref, b, tp // 2)

    @pl.when(tp >= 2)
    def _():
        sib_kv = kv_ref.at[:, rows(tp ^ 3), :]
        rc(KV_REL, sib_kv, sib_kv, sib).wait_recv()
        for b in range(NB):
            transpose_kv(kv_ref, kt_ref, b, False)

    def weight_grad(acc, first, left, src):
        def tile(j, carry):
            cols = pl.ds(pl.multiple_of(j * HW, HW), HW)
            part = dot_nn(left[...], src[:, cols])
            acc[:, cols] = part if first else acc[:, cols] + part
            return carry
        lax.fori_loop(0, 4, tile, 0)

    def group(i, carry):
        @pl.when(i == 1)
        def _():
            rc(WQ_SIB, wq_own, wq_buf.at[1], sib).wait_recv()
            rc(WO_SIB, wo_own, wo_buf.at[1], sib).wait_recv()

        @pl.when(i == 2)
        def _():
            copies[ACT_SIB].wait_recv()
            load = local(6, act_all.at[1], buf.at[0])
            weight_grad(dwq_acc, True, oqt.at[0, 1], act)
            load.wait()
            rc(OQ_SIB, rs_c, oqt.at[1], sib).wait_recv()
            weight_grad(dwq_acc, False, oqt.at[1, 1], buf.at[0])
            for which, first in ((0, WQ_X), (1, WO_X)):
                for j in (1, 2, 3):
                    piece = quarter(which, 2, j)
                    rc(first + j, piece, piece, sib).wait_recv()
                    rc(first + 4 + j, piece, quarter(which, 3, j), sib).start()

        @pl.when(i == 3)
        def _():
            for which, rel in ((0, WQ_REL), (1, WO_REL)):
                for j in range(4):
                    rc(rel + j, quarter(which, 2, j), quarter(which, 3, j), sib).wait_recv()

        @pl.when(i > 0)
        def _():
            project_own(i)

        attend_group()

        @pl.when(i == 0)
        def _():
            spread(1)
            for c in (1, 2, 3):
                bulk(c).start()

        accumulate(i)

        @pl.when(i == 0)
        def _():
            oqt[0, 0] = o_s[...].astype(F32).T.astype(BF16)
            oqt[0, 1] = dq_s[...].astype(F32).T.astype(BF16)

        @pl.when(i == 1)
        def _():
            rs_c[0] = o_s[...].astype(F32).T.astype(BF16)
            rs_c[1] = dq_s[...].astype(F32).T.astype(BF16)
            rc(OQ_SIB, rs_c, oqt.at[1], sib).start()
        return carry

    lax.fori_loop(0, 4, group, 0)
    copies[DOUT_SIB].wait_recv()
    load_sib = local(7, dout_all.at[1], buf.at[1])

    start(RS_SIB, dkv_acc.at[:, rows(tp ^ 1), :], rs_a.at[0], sib)
    start(RS_SIB2, dkv_acc.at[:, rows(tp ^ 3), :], rs_a.at[1], sib)
    for r in range(8):
        cols = slice(r * 256, (r + 1) * 256)
        io_ref[:, cols] = (x_ref[:, cols].astype(F32) + out_acc[:, cols]).astype(BF16)
    put_out = local(8, io_ref, out_hbm)
    copies[RS_SIB].wait_recv()
    copies[RS_SIB2].wait_recv()

    def dkv_piece(part, b, blk):
        return dkv_ref.at[part, b, rows(blk), :]

    def reduce_kv(part, blk):
        for b in range(NB):
            total = dkv_acc[b, rows(blk), :] + rs_a[part, b]
            d_k = rope_back(total[:, KEY], cos_s[b, rows(blk), :], sin_s[b, rows(blk), :])
            dkv_ref[part, b, rows(blk), KEY] = d_k.astype(BF16)
            dkv_ref[part, b, rows(blk), VAL] = total[:, VAL].astype(BF16)
        for b in range(NB):
            piece = dkv_piece(part, b, blk)
            rc(DKV_X + 2 * part + b, piece, piece, xp).start()
            rc(DKV_SIB + 2 * part + b, piece, piece, sib).start()

    @pl.when(tp >= 2)
    def _():
        reduce_kv(1, tp ^ 2)
        dkv_ref[1, :, rows(tp), :] = jnp.zeros((NB, TB, 2 * HD), BF16)

    bulk_end().start()
    reduce_kv(0, tp)

    for c in range(2):
        receive(c)
    weight_grad(out_acc, True, oqt.at[0, 0], dout_ref)
    load_sib.wait()
    weight_grad(out_acc, False, oqt.at[1, 0], buf.at[1])
    own_a.wait()
    own_d.wait()
    put_out.wait()

    def take(part, b, blk):
        piece = dkv_piece(part, b, blk)
        rc(DKV_X + NB * part + b, piece, piece, xp).wait_recv()
        rc(DKV_REL + NB * part + b, piece, piece, sib).start()

    def dw_copies():
        return [rc(DW_SIB + k, dw_parts.at[0], dw_parts.at[k + 1], dev) for k, dev in enumerate((sib, xp, xs))]

    def finish_dx():
        @pl.when(tp < 2)
        def _():
            for b in range(NB):
                take(1, b, tp)

        dw_acc[...] = jnp.zeros_like(dw_acc)
        gain = 1.0 + normw_ref[...]

        def dx_rows(j, carry):
            b = j // 2
            r = pl.ds(pl.multiple_of(j * HD, HD), HD)
            own = pl.ds(pl.multiple_of(tp * TB + (j % 2) * HD, HD), HD)
            da = da_acc[r, :] + dot_nt(dkv_ref[0, b, own, :], wkv[...]) + dot_nt(dkv_ref[1, b, own, :], wkv[...])
            xf = x_ref[r, :].astype(F32)
            inv = lax.rsqrt(jnp.mean(xf * xf, axis=-1, keepdims=True) + 1e-6)
            normed = xf * inv
            prod = da * normed
            dw_acc[...] += jnp.sum(prod.reshape(-1, *dw_acc.shape), axis=0)
            corr = jnp.mean(prod * gain, axis=-1, keepdims=True)
            io_ref[r, :] = (dout_ref[r, :].astype(F32) + inv * (da * gain - normed * corr)).astype(BF16)
            return carry

        lax.fori_loop(0, TOK // HD, dx_rows, 0)
        dw_parts[0] = jnp.sum(dw_acc[...], axis=0, keepdims=True)
        pltpu.make_async_copy(io_ref, dx_hbm, lsem.at[8]).start()
        for cp in dw_copies():
            cp.start()

    def head_part(t, carry):
        b = t // 2
        i = 2 + t % 2
        blk = tp ^ i
        r = pl.ds(pl.multiple_of(b * TB, TB), TB)

        def load(c, k):
            whole = (dout_all, act_all)[c]
            return pltpu.make_async_copy(whole.at[2 + k, r, :], buf.at[1 - c, pl.ds(k * TB, TB), :], lsem.at[7 - c + 5 * k])

        def load_relayed(c):
            whole = (dout_all, act_all)[c]
            rc(BULK_REL + 2 * b + c, whole.at[2, r, :], whole.at[3, r, :], sib).wait_recv()
            load(c, 1).start()

        half = pl.ds(pl.multiple_of((i - 2) * TB, TB), TB)

        @pl.when(i == 2)
        def _():
            load(0, 0).start()
            load_relayed(0)

            @pl.when(b == 0)
            def _():
                load(1, 0).start()

            for k in range(2):
                load(0, k).wait()
                part = slice(k * TB, (k + 1) * TB)
                project_back(buf.at[1, part, :], 0, do_s.at[part, :])

            @pl.when(b == 1)
            def _():
                receive(3)
                load(1, 0).start()

            load(1, 0).wait()

        @pl.when(i == 3)
        def _():
            load(1, 1).wait()

        cos_t = cos_s.at[b, rows(blk), :]
        sin_t = sin_s.at[b, rows(blk), :]
        trig_t[0] = cos_t[...].T
        trig_t[1] = sin_t[...].T

        def late_kv(blk):
            piece = kv_ref.at[b, rows(blk), :]
            return rc(KV_LATE + b, piece, piece, sib)

        @pl.when((i == 2) & (tp < 2))
        def _():
            kv = dot_nn(buf[0, 0:TB, :], wkv[...])
            kv_ref[b, rows(blk), KEY] = rope(kv[:, KEY].astype(BF16).astype(F32), cos_t[...], sin_t[...]).astype(BF16)
            kv_ref[b, rows(blk), VAL] = kv[:, VAL].astype(BF16)
            late_kv(tp ^ 2).start()

        project(TB, buf.at[0, half, :], 0, lambda _: (cos_t[...], sin_t[...]))

        @pl.when(i == 2)
        def _():
            load_relayed(1)

        @pl.when((i == 2) & (tp < 2))
        def _():
            late_kv(tp ^ 3).wait_recv()
            transpose_kv(kv_ref, kt_ref, b, True)

        @pl.when(t == 3)
        def _():
            for seq in range(NB):
                take(0, seq, tp ^ 2)
            for cp in dw_copies():
                cp.wait_recv()
            parts = [dw_parts[jnp.bitwise_xor(tp, d)] for d in range(4)]
            dw_row[...] = sum(parts[1:], parts[0])
            pltpu.make_async_copy(dw_row, dw_hbm, lsem.at[5]).start()

        for n in range(1, 5):
            @pl.when(blk == n - 1)
            def _():
                def step(u, carry):
                    for j in range(2):
                        c = pl.ds(pl.multiple_of((u * 2 + j) * HD, HD), HD)
                        o_t, dq_t, _, _ = attend(n, q_s[0:TB, c], do_s[half, c], kv_ref, b, kt_ref)
                        oqt[0, 0, c, half] = o_t.astype(BF16)
                        oqt[0, 1, c, half] = rope_back_t(dq_t * SCALE, trig_t[0], trig_t[1]).astype(BF16)
                    return carry
                lax.fori_loop(0, 2, step, 0)

        @pl.when(t == 1)
        def _():
            receive(2)
            weight_grad(out_acc, False, oqt.at[0, 0], buf.at[1])
            weight_grad(dwq_acc, False, oqt.at[0, 1], buf.at[0])
            pltpu.make_async_copy(dwq_acc, accq_hbm, lsem.at[9]).start()
            pltpu.make_async_copy(out_acc, acco_hbm, lsem.at[10]).start()
            finish_dx()
        return carry

    lax.fori_loop(0, 4, head_part, 0)
    put_oqt = local(0, oqt.at[0], oqt_hbm)
    put_dkv = []
    for b in range(NB):
        def arrived(first, part, blk):
            piece = dkv_piece(part, b, blk)
            rc(first + NB * part + b, piece, piece, sib).wait_recv()

        arrived(DKV_SIB, 0, tp ^ 1)
        arrived(DKV_REL, 0, tp ^ 3)

        @pl.when(tp < 2)
        def _():
            arrived(DKV_REL, 1, tp ^ 1)

        @pl.when(tp >= 2)
        def _():
            arrived(DKV_SIB, 1, tp ^ 3)

        put_dkv.append(local(1 + b, dkv_ref.at[0, b], dkv_hbm.at[0, b]))
        put_dkv.append(local(3 + b, dkv_ref.at[1, b, 0:TOK, :], dkv_hbm.at[1, b, 0:TOK, :]))

    for cp in (put_oqt, *put_dkv):
        cp.wait()
    pltpu.make_async_copy(io_ref, dx_hbm, lsem.at[8]).wait()
    pltpu.make_async_copy(dw_row, dw_hbm, lsem.at[5]).wait()
    for cp in dw_copies():
        cp.wait_send()
    bulk_end().wait_send()
    pltpu.make_async_copy(dwq_acc, accq_hbm, lsem.at[9]).wait()
    pltpu.make_async_copy(out_acc, acco_hbm, lsem.at[10]).wait()
    for i in copies:
        copies[i].wait_send()
    rc(OQ_SIB, rs_c, oqt.at[1], sib).wait_send()
    for b in range(NB):
        piece = dkv_piece(0, b, tp)
        for i in (DKV_X, DKV_SIB, DKV_REL):
            rc(i + b, piece, piece, sib).wait_send()

        @pl.when(tp < 2)
        def _():
            rc(DKV_REL + 2 + b, piece, piece, sib).wait_send()
            rc(KV_LATE + b, piece, piece, sib).wait_send()

        @pl.when(tp >= 2)
        def _():
            rc(DKV_X + 2 + b, piece, piece, sib).wait_send()
            rc(DKV_SIB + 2 + b, piece, piece, sib).wait_send()

    @pl.when(tp < 2)
    def _():
        rc(KV_X, own_kv, own_kv, xp).wait_send()

    @pl.when(tp >= 2)
    def _():
        rc(KV_REL, own_kv, own_kv, sib).wait_send()

    for c in range(4):
        bulk(c).wait_send()
        whole = act_all if c % 2 else dout_all
        r = slice((c // 2) * TB, (c // 2 + 1) * TB)
        rc(BULK_REL + c, whole.at[2, r, :], whole.at[3, r, :], sib).wait_send()
    for which, first in ((0, WQ_X), (1, WO_X)):
        for j in range(1, 8):
            rc(first + j, quarter(which, 2, j % 4), quarter(which, 2, j % 4), sib).wait_send()


def grad_kernel(accq_ref, acco_ref, act_ref, dout_ref, oqt_ref, dkv_ref, out_in, dx_in, dw_in,
                dwq_ref, dwo_ref, dwk_ref, dwv_ref, out_ref, dx_ref, dw_ref, dkvt):
    tp = lax.axis_index('tp')
    out_ref[...] = out_in[...]
    dx_ref[...] = dx_in[...]
    dw_ref[...] = dw_in[...]

    @pl.when(pl.program_id(0) == 0)
    def _():
        for t in range(6):
            for b in range(NB):
                piece = dkv_ref[t // 4, b, (t % 4) * TB:(t % 4 + 1) * TB, :]
                dkvt[t, :, b * TB:(b + 1) * TB] = piece.astype(F32).T.astype(BF16)

    a = jnp.concatenate([act_ref[2, TB:TOK, :], act_ref[3, TB:TOK, :]], axis=0)
    d = dout_ref[...].reshape(TOK, -1)
    dwo_ref[...] = acco_ref[...] + dot_nn(oqt_ref[0], d)
    dwq_ref[...] = (accq_ref[...] + dot_nn(oqt_ref[1], a)).T
    total = dot_nn(dkvt[0], act_ref[jnp.bitwise_xor(tp, 0)])
    for t in range(1, 6):
        total += dot_nn(dkvt[t], act_ref[jnp.bitwise_xor(tp, t % 4)])
    dwk_ref[...] = total[KEY].T
    dwv_ref[...] = total[VAL].T


def local_block(hidden, positions, norm_w, w_query, w_key, w_value, w_out, grad_out):
    x = hidden.reshape(TOK, D)
    dout = grad_out.reshape(TOK, D)
    freq = 10000.0 ** (-2.0 * (np.arange(HD) % (HD // 2)) / HD)

    vmem = pl.BlockSpec(memory_space=pltpu.VMEM)
    anym = pl.BlockSpec(memory_space=pl.ANY)
    sds = jax.ShapeDtypeStruct
    out, dx, dw, accq, acco, oqt, dkv, act_all, dout_all = pl.pallas_call(
        main_kernel,
        out_shape=[sds((TOK, D), BF16), sds((TOK, D), BF16), sds((1, D), F32), sds((HW, D), F32), sds((HW, D), F32),
                   sds((2, HW, TOK), BF16), sds((2, NB, SEQ, 2 * HD), BF16), sds((4, TOK, D), BF16), sds((4, TOK, D), BF16)],
        in_specs=[anym, anym, anym, anym, anym, anym, vmem, vmem, vmem],
        out_specs=[anym] * 9,
        scratch_shapes=[
            pltpu.VMEM((TOK, D), BF16), pltpu.VMEM((TOK, D), BF16), pltpu.VMEM((TOK, D), BF16),
            pltpu.VMEM((2, NB, SEQ, 2 * HD), BF16),
            pltpu.VMEM((2, 2, HW, TOK), BF16),
            pltpu.VMEM((2, HD, TB), F32),
            pltpu.VMEM((HW, D), F32),
            pltpu.VMEM((TOK, D), BF16),
            pltpu.VMEM((NB, SEQ, 2 * HD), BF16),
            pltpu.VMEM((D, 2 * HD), BF16),
            pltpu.VMEM((NB, SEQ, HD), F32), pltpu.VMEM((NB, SEQ, HD), F32),
            pltpu.VMEM((4, D, HW), BF16), pltpu.VMEM((4, HW, D), BF16),
            pltpu.VMEM((TOK, HW), BF16), pltpu.VMEM((TOK, HW), BF16),
            pltpu.VMEM((TOK, HW), BF16), pltpu.VMEM((TOK, HW), BF16),
            pltpu.VMEM((TOK, D), F32), pltpu.VMEM((TOK, D), F32),
            pltpu.VMEM((NB, 2 * HD, SEQ), BF16),
            pltpu.VMEM((NB, SEQ, 2 * HD), F32),
            pltpu.VMEM((2, NB, TB, 2 * HD), F32),
            pltpu.VMEM((2, HW, TOK), BF16),
            pltpu.VMEM((8, D), F32), pltpu.VMEM((4, 1, D), F32), pltpu.VMEM((1, D), F32),
            pltpu.VMEM((2, TOK, D), BF16),
            pltpu.SemaphoreType.DMA((N_SEM,)), pltpu.SemaphoreType.DMA((N_SEM,)), pltpu.SemaphoreType.DMA((13,)),
        ],
        compiler_params=pltpu.CompilerParams(collective_id=0, has_side_effects=True, vmem_limit_bytes=67_000_000),
        name='main',
    )(x, dout, w_query, w_out, w_key, w_value, norm_w[None, :], positions, jnp.asarray(freq[None, :], F32))

    whole = lambda s: pl.BlockSpec(s, lambda t: (0,) * len(s))
    steps = 2
    cols = D // steps
    by_row = lambda r, c: pl.BlockSpec((r, c), lambda t: (t, 0))
    by_col = pl.BlockSpec((HW, cols), lambda t: (0, t))
    dwq, dwo, dwk, dwv, out, dx, dw = pl.pallas_call(
        grad_kernel,
        grid=(steps,),
        out_shape=[sds((D, HW), F32), sds((HW, D), F32), sds((D, HD), F32), sds((D, HD), F32), sds((TOK, D), BF16), sds((TOK, D), BF16), sds((1, D), F32)],
        in_specs=[by_col, by_col, pl.BlockSpec((4, TOK, cols), lambda t: (0, 0, t)), pl.BlockSpec((2, TB, cols), lambda t: (1, 1, t)),
                  whole((2, HW, TOK)), whole((2, NB, SEQ, 2 * HD)), by_row(TOK // steps, D), by_row(TOK // steps, D), whole((1, D))],
        out_specs=[by_row(cols, HW), by_col, by_row(cols, HD), by_row(cols, HD), by_row(TOK // steps, D), by_row(TOK // steps, D), whole((1, D))],
        scratch_shapes=[pltpu.VMEM((6, 2 * HD, TOK), BF16)],
        compiler_params=pltpu.CompilerParams(vmem_limit_bytes=64_000_000),
        name='grads',
    )(accq, acco, act_all, dout_all, oqt, dkv, out, dx, dw)

    return out.reshape(NB, TB, D), dx.reshape(NB, TB, D), dwq, dwo, dwk, dwv, dw.reshape(D)


def solution(mesh):
    specs_in = (P('dp', 'tp'), P('dp'), P(), P(None, 'tp'), P(), P(), P('tp'), P('dp', 'tp'))
    specs_out = (P('dp', 'tp'), P('dp', 'tp'), P('dp', 'tp'), P(('dp', 'tp')), P('dp'), P('dp'), P('dp'))
    return jax.shard_map(local_block, mesh=mesh, in_specs=specs_in, out_specs=specs_out, check_vma=False)
```
